8 devices in a mesh: dp: 1 (over z), tp: 2 (over y), cp: 4 (over x, core).
Axes of the slice: x: 2, y: 2, z: 1, core: 2. Of those that a mesh axis runs over, the one named last changes fastest.
Arguments:
- tokens: bfloat16 [8192, 1536], P(('dp', 'cp', 'tp'))
- norm_attn: bfloat16 [1536], replicated
- norm_mlp: bfloat16 [1536], replicated
- w_query: bfloat16 [1536, 12, 128], P(None, 'tp')
- w_key: bfloat16 [1536, 2, 128], P(None, 'tp')
- w_value: bfloat16 [1536, 2, 128], P(None, 'tp')
- w_out: bfloat16 [12, 128, 1536], P('tp')
- w_gate: bfloat16 [1536, 8960], P(None, 'tp')
- w_up: bfloat16 [1536, 8960], P(None, 'tp')
- w_down: bfloat16 [8960, 1536], P('tp')
Outputs:
- output 1: bfloat16 [8192, 1536], P(('dp', 'cp', 'tp'))
- output 2: bfloat16 [8192, 256], P(('dp', 'cp'), 'tp')
- output 3: bfloat16 [8192, 256], P(('dp', 'cp'), 'tp')
All inputs are finite; a program needn't handle non-finite values.
Results may differ from the reference program's by a relative error of at most 0.0117268.
Values are sent between devices in bfloat16 or wider.
A program may use at most 1 GiB of HBM per device.

```python
import math
import jax
import jax.numpy as jnp
from jax import lax

MODEL_DIM = 1536
Q_HEADS = 12
KV_HEADS = 2
HEAD_DIM = 128
FFN_DIM = 8960
CP_SIZE = 4
SEQ_LEN = 8192

ROPE_BASE = 500000.0
NORM_EPS = 1e-5
QUERY_BLOCK = min(64, SEQ_LEN)
CHUNK_LEN = SEQ_LEN // (2 * CP_SIZE)
GROUP_SIZE = Q_HEADS // KV_HEADS


def folded_positions():
    row_ids = jnp.arange(SEQ_LEN, dtype=jnp.int32)
    shard_ids = row_ids // (2 * CHUNK_LEN)
    within = row_ids % (2 * CHUNK_LEN)
    piece_ids = jnp.where(within < CHUNK_LEN, shard_ids, 2 * CP_SIZE - 1 - shard_ids)
    return piece_ids * CHUNK_LEN + within % CHUNK_LEN


def rms_norm(tensor, gain_vec):
    widened = tensor.astype(jnp.float32)
    inv_rms = lax.rsqrt(jnp.mean(widened * widened, axis=-1, keepdims=True) + NORM_EPS)
    return (widened * inv_rms * gain_vec.astype(jnp.float32)).astype(jnp.bfloat16)


def rope_rotate(tensor, positions):
    half_dim = HEAD_DIM // 2
    inv_freq = ROPE_BASE ** (-2.0 * jnp.arange(half_dim, dtype=jnp.float32) / HEAD_DIM)
    angles = positions.astype(jnp.float32)[:, None] * inv_freq[None, :]
    cosine = jnp.cos(angles)[:, None, :]
    sine_tab = jnp.sin(angles)[:, None, :]
    first_half = tensor[..., :half_dim]
    second_half = tensor[..., half_dim:]
    return jnp.concatenate([first_half * cosine - second_half * sine_tab, second_half * cosine + first_half * sine_tab], axis=-1)


def natural_order(tensor):
    folded = tensor.reshape(CP_SIZE, 2, CHUNK_LEN, KV_HEADS * HEAD_DIM)
    return jnp.concatenate([folded[:, 0], folded[::-1, 1]], axis=0).reshape(SEQ_LEN, KV_HEADS * HEAD_DIM)


def setup_inputs(seed: int = 0, part: int = 0) -> dict:
    key_list = jax.random.split(jax.random.key(seed), 9)
    part_key = jax.random.fold_in(jax.random.key(seed + 1), part)
    score_std = math.sqrt(0.75 * math.log(SEQ_LEN))
    qk_scale = math.sqrt(score_std) * MODEL_DIM ** -0.5
    q_width = Q_HEADS * HEAD_DIM

    def normal(rng_key, out_shape, std_dev):
        return (jax.random.normal(rng_key, out_shape, jnp.float32) * std_dev).astype(jnp.bfloat16)

    return {
        "tokens": normal(part_key, (SEQ_LEN, MODEL_DIM), 1.0),
        "norm_attn": jax.random.uniform(key_list[0], (MODEL_DIM,), jnp.float32, 0.5, 1.5).astype(jnp.bfloat16),
        "norm_mlp": jax.random.uniform(key_list[1], (MODEL_DIM,), jnp.float32, 0.5, 1.5).astype(jnp.bfloat16),
        "w_query": normal(key_list[2], (MODEL_DIM, Q_HEADS, HEAD_DIM), qk_scale),
        "w_key": normal(key_list[3], (MODEL_DIM, KV_HEADS, HEAD_DIM), qk_scale),
        "w_value": normal(key_list[4], (MODEL_DIM, KV_HEADS, HEAD_DIM), MODEL_DIM ** -0.5),
        "w_out": normal(key_list[5], (Q_HEADS, HEAD_DIM, MODEL_DIM), 2.0 * q_width ** -0.5),
        "w_gate": normal(key_list[6], (MODEL_DIM, FFN_DIM), MODEL_DIM ** -0.5),
        "w_up": normal(key_list[7], (MODEL_DIM, FFN_DIM), MODEL_DIM ** -0.5),
        "w_down": normal(key_list[8], (FFN_DIM, MODEL_DIM), 1.5 * FFN_DIM ** -0.5),
    }


def reference(tokens, norm_attn, norm_mlp, w_query, w_key, w_value, w_out, w_gate, w_up, w_down):
    positions = folded_positions()
    normed = rms_norm(tokens, norm_attn)
    q_proj = jnp.dot(normed, w_query.reshape(MODEL_DIM, Q_HEADS * HEAD_DIM), preferred_element_type=jnp.float32)
    k_proj = jnp.dot(normed, w_key.reshape(MODEL_DIM, KV_HEADS * HEAD_DIM), preferred_element_type=jnp.float32)
    v_proj = jnp.dot(normed, w_value.reshape(MODEL_DIM, KV_HEADS * HEAD_DIM), preferred_element_type=jnp.float32)
    queries = rope_rotate(q_proj.reshape(SEQ_LEN, Q_HEADS, HEAD_DIM), positions).astype(jnp.bfloat16)
    keys_rot = rope_rotate(k_proj.reshape(SEQ_LEN, KV_HEADS, HEAD_DIM), positions).astype(jnp.bfloat16)
    values = v_proj.astype(jnp.bfloat16).reshape(SEQ_LEN, KV_HEADS, HEAD_DIM)
    keys_wide = keys_rot.astype(jnp.float32)
    values_wide = values.astype(jnp.float32)
    q_blocks = queries.reshape(SEQ_LEN // QUERY_BLOCK, QUERY_BLOCK, KV_HEADS, GROUP_SIZE, HEAD_DIM)
    pos_blocks = positions.reshape(SEQ_LEN // QUERY_BLOCK, QUERY_BLOCK)

    def attend_block(block_args):
        q_blk, q_pos = block_args
        scores = jnp.einsum("qkgd,tkd->qkgt", q_blk.astype(jnp.float32), keys_wide) * (HEAD_DIM ** -0.5)
        visible = (positions[None, :] <= q_pos[:, None])[:, None, None, :]
        probs = jax.nn.softmax(jnp.where(visible, scores, -jnp.inf), axis=-1)
        return jnp.einsum("qkgt,tkd->qkgd", probs, values_wide).astype(jnp.bfloat16)

    attn_heads = lax.map(attend_block, (q_blocks, pos_blocks)).reshape(SEQ_LEN, Q_HEADS * HEAD_DIM)
    attn_proj = jnp.dot(attn_heads, w_out.reshape(Q_HEADS * HEAD_DIM, MODEL_DIM), preferred_element_type=jnp.float32)
    residual = (tokens.astype(jnp.float32) + attn_proj).astype(jnp.bfloat16)
    normed_mlp = rms_norm(residual, norm_mlp)
    gate_val = jnp.dot(normed_mlp, w_gate, preferred_element_type=jnp.float32)
    up_val = jnp.dot(normed_mlp, w_up, preferred_element_type=jnp.float32)
    hidden = (jax.nn.silu(gate_val) * up_val).astype(jnp.bfloat16)
    layer_out = (residual.astype(jnp.float32) + jnp.dot(hidden, w_down, preferred_element_type=jnp.float32)).astype(jnp.bfloat16)
    return layer_out, natural_order(keys_rot), natural_order(values)
```

```python
import functools

import jax
import jax.numpy as jnp
from jax import lax
from jax.experimental import pallas as pl
from jax.experimental.pallas import tpu as pltpu
from jax.sharding import PartitionSpec as P

ROPE_BASE = 500000.0
NORM_EPS = 1e-5
MASK_VALUE = -1e30
LOG2E = 1.4426950408889634
VMEM_LIMIT = 60 * 1024 * 1024
Q_ROWS = 256
K_ROWS = 512


def rms_norm(tensor, gain_vec):
    widened = tensor.astype(jnp.float32)
    inv_rms = lax.rsqrt(jnp.mean(widened * widened, axis=-1, keepdims=True) + NORM_EPS)
    return (widened * inv_rms * gain_vec.astype(jnp.float32)).astype(jnp.bfloat16)


def rope_tables(positions, head_dim):
    half_dim = head_dim // 2
    inv_freq = ROPE_BASE ** (-2.0 * jnp.arange(half_dim, dtype=jnp.float32) / head_dim)
    angles = positions.astype(jnp.float32)[:, None] * inv_freq[None, :]
    return jnp.cos(angles), jnp.sin(angles)


def rope_rotate(proj, tables, head_dim):
    cosine, sine_tab = tables
    half_dim = head_dim // 2
    parts = []
    for h in range(proj.shape[1] // head_dim):
        first_half = proj[:, h * head_dim:h * head_dim + half_dim]
        second_half = proj[:, h * head_dim + half_dim:(h + 1) * head_dim]
        parts += [first_half * cosine - second_half * sine_tab, second_half * cosine + first_half * sine_tab]
    return jnp.concatenate(parts, axis=1).astype(jnp.bfloat16)


def attention_kernel(table, q_ref, k_ref, v_ref, o_ref, m_sc, l_sc, acc_sc, *, heads, chains, chunk_len):
    head_dim = 128
    piece = table[8]
    start = pl.program_id(0) * Q_ROWS
    per_chain = heads // chains
    rows = per_chain * Q_ROWS
    coef = head_dim ** -0.5 * LOG2E
    q_parts = []
    for a in range(chains):
        q_parts.append(jnp.concatenate([q_ref[:, (a * per_chain + h) * head_dim:(a * per_chain + h + 1) * head_dim] for h in range(per_chain)], axis=0))
    m_sc[...] = jnp.full_like(m_sc, MASK_VALUE)
    l_sc[...] = jnp.zeros_like(l_sc)
    acc_sc[...] = jnp.zeros_like(acc_sc)
    per_piece = chunk_len // K_ROWS

    def block(i, masked):
        slot = table[i // per_piece]
        off = pl.multiple_of((i % per_piece) * K_ROWS, K_ROWS)
        k_blk = k_ref[slot, pl.ds(off, K_ROWS), :]
        v_blk = v_ref[slot, pl.ds(off, K_ROWS), :]
        for a in range(chains):
            s = lax.dot_general(q_parts[a], k_blk, (((1,), (1,)), ((), ())), preferred_element_type=jnp.float32)
            if masked:
                q_pos = start + lax.rem(lax.broadcasted_iota(jnp.int32, (rows, K_ROWS), 0), Q_ROWS)
                k_pos = off + lax.broadcasted_iota(jnp.int32, (rows, K_ROWS), 1)
                s = jnp.where(k_pos <= q_pos, s, MASK_VALUE)
            m_prev = m_sc[a]
            m_new = jnp.maximum(m_prev, jnp.max(s, axis=1, keepdims=True))
            alpha = jnp.exp2((m_prev - m_new) * coef)
            mc = m_new * coef
            sums = l_sc[a] * alpha
            p_tiles = []
            for j in range(K_ROWS // 128):
                p = jnp.exp2(s[:, j * 128:(j + 1) * 128] * coef - mc)
                sums = sums + p
                p_tiles.append(p.astype(jnp.bfloat16))
            l_sc[a] = sums
            m_sc[a] = m_new
            p_all = jnp.concatenate(p_tiles, axis=1)
            acc_sc[a] = acc_sc[a] * alpha + jnp.dot(p_all, v_blk, preferred_element_type=jnp.float32)

    n_full = piece * per_piece + start // K_ROWS

    def step(i, carry):
        block(i, False)
        return carry

    lax.fori_loop(0, n_full, step, 0)
    block(n_full, True)
    for a in range(chains):
        total = jnp.sum(l_sc[a], axis=1, keepdims=True)
        out = (acc_sc[a] / total).astype(jnp.bfloat16)
        for h in range(per_chain):
            o_ref[:, (a * per_chain + h) * head_dim:(a * per_chain + h + 1) * head_dim] = out[h * Q_ROWS:(h + 1) * Q_ROWS]


def attention(table, q, k, v, name):
    rows, width = q.shape
    heads = width // 128
    chains = 2
    m_rows = heads // chains * Q_ROWS
    slots, chunk_len, head_dim = k.shape
    return pl.pallas_call(
        functools.partial(attention_kernel, heads=heads, chains=chains, chunk_len=chunk_len),
        grid_spec=pltpu.PrefetchScalarGridSpec(
            num_scalar_prefetch=1,
            grid=(rows // Q_ROWS,),
            in_specs=[
                pl.BlockSpec((Q_ROWS, width), lambda i, t: (i, 0)),
                pl.BlockSpec((slots, chunk_len, head_dim), lambda i, t: (0, 0, 0)),
                pl.BlockSpec((slots, chunk_len, head_dim), lambda i, t: (0, 0, 0)),
            ],
            out_specs=pl.BlockSpec((Q_ROWS, width), lambda i, t: (i, 0)),
            scratch_shapes=[pltpu.VMEM((chains, m_rows, 128), jnp.float32)] * 3,
        ),
        out_shape=jax.ShapeDtypeStruct((rows, width), jnp.bfloat16),
        compiler_params=pltpu.CompilerParams(vmem_limit_bytes=VMEM_LIMIT),
        cost_estimate=pl.CostEstimate(flops=4 * rows * 4096 * width, bytes_accessed=8 * 2**20, transcendentals=rows * 4096 * heads),
        name=name,
    )(table, q, k, v)


M_BLOCK = 512


def mlp_half_kernel(b_ref, w1_ref, w3_ref, w2_ref, acc_ref):
    step = pl.program_id(0)

    @pl.when(step == 0)
    def _():
        acc_ref[...] = jnp.zeros_like(acc_ref)

    def rows_step(m, carry):
        sl = pl.ds(pl.multiple_of(m * M_BLOCK, M_BLOCK), M_BLOCK)
        b = b_ref[sl, :]
        gate = jnp.dot(b, w1_ref[...], preferred_element_type=jnp.float32)
        up = jnp.dot(b, w3_ref[...], preferred_element_type=jnp.float32)
        hidden = (jax.nn.silu(gate) * up).astype(jnp.bfloat16)
        acc_ref[sl, :] += jnp.dot(hidden, w2_ref[...], preferred_element_type=jnp.float32)
        return carry

    lax.fori_loop(0, b_ref.shape[0] // M_BLOCK, rows_step, 0)


def mlp_half(b, w1, w3, w2, tile, n_tiles, name):
    rows, dim = b.shape
    return pl.pallas_call(
        mlp_half_kernel,
        grid=(n_tiles,),
        in_specs=[
            pl.BlockSpec((rows, dim), lambda i: (0, 0)),
            pl.BlockSpec((dim, tile), lambda i: (0, i)),
            pl.BlockSpec((dim, tile), lambda i: (0, i)),
            pl.BlockSpec((tile, dim), lambda i: (i, 0)),
        ],
        out_specs=pl.BlockSpec((rows, dim), lambda i: (0, 0)),
        out_shape=jax.ShapeDtypeStruct((rows, dim), jnp.float32),
        compiler_params=pltpu.CompilerParams(vmem_limit_bytes=VMEM_LIMIT),
        cost_estimate=pl.CostEstimate(flops=6 * rows * dim * tile * n_tiles, bytes_accessed=6 * dim * tile * n_tiles, transcendentals=rows * tile * n_tiles),
        name=name,
    )(b, w1, w3, w2)


def mlp_pieces_kernel(b_ref, base_ref, *refs, n_pieces):
    out_ref = refs[-1]
    b = b_ref[...]
    total = base_ref[...].astype(jnp.float32)
    for n in range(n_pieces):
        w1_ref, w3_ref, w2_ref = refs[3 * n:3 * n + 3]
        gate = jnp.dot(b, w1_ref[...], preferred_element_type=jnp.float32)
        up = jnp.dot(b, w3_ref[...], preferred_element_type=jnp.float32)
        hidden = (jax.nn.silu(gate) * up).astype(jnp.bfloat16)
        total = total + jnp.dot(hidden, w2_ref[...], preferred_element_type=jnp.float32)
    out_ref[...] = total.astype(out_ref.dtype)


def mlp_pieces(b, base, pieces, out_dtype, name):
    rows, dim = b.shape
    flat = [w for piece in pieces for w in piece]
    width = pieces[0][0].shape[1] * len(pieces)
    mb = 256
    return pl.pallas_call(
        functools.partial(mlp_pieces_kernel, n_pieces=len(pieces)),
        grid=(rows // mb,),
        in_specs=[pl.BlockSpec((mb, dim), lambda i: (i, 0))] * 2 + [pl.BlockSpec(w.shape, lambda i: (0, 0)) for w in flat],
        out_specs=pl.BlockSpec((mb, dim), lambda i: (i, 0)),
        out_shape=jax.ShapeDtypeStruct((rows, dim), out_dtype),
        input_output_aliases={1: 0} if base.dtype == out_dtype else {},
        compiler_params=pltpu.CompilerParams(vmem_limit_bytes=VMEM_LIMIT),
        cost_estimate=pl.CostEstimate(flops=6 * rows * dim * width, bytes_accessed=6 * dim * width, transcendentals=rows * width),
        name=name,
    )(b, base, *flat)


def solution(mesh):
    cp_size = mesh.shape["cp"]
    tp_swap = [(0, 1), (1, 0)]
    chip_swap = [(0, 2), (2, 0), (1, 3), (3, 1)]
    core_swap = [(0, 1), (1, 0), (2, 3), (3, 2)]

    def swap_tp(a):
        return lax.ppermute(a, "tp", tp_swap)

    def swap_chip(a):
        return lax.ppermute(a, "cp", chip_swap)

    def swap_core(a):
        return lax.ppermute(a, "cp", core_swap)

    def spread(a):
        b = swap_chip(a)
        return [a, b, swap_core(a), swap_core(b)]

    def layer_shard(x_loc, norm_attn, norm_mlp, w_query, w_key, w_value, w_out, w_gate, w_up, w_down):
        tok_dev, dim = x_loc.shape
        local_q, head_dim = w_query.shape[1], w_query.shape[2]
        cp_index = lax.axis_index("cp")
        tp_index = lax.axis_index("tp")
        n_pieces = 2 * cp_size
        piece = jnp.where(tp_index == 0, cp_index, n_pieces - 1 - cp_index)
        tables = rope_tables(piece * tok_dev + jnp.arange(tok_dev, dtype=jnp.int32), head_dim)

        peers = jnp.arange(cp_size, dtype=jnp.int32) ^ cp_index
        rel_slot = jnp.where(peers == 1, 2, jnp.where(peers == 2, 1, peers))
        ids = jnp.arange(n_pieces, dtype=jnp.int32)
        owner_cp = jnp.where(ids < cp_size, ids, n_pieces - 1 - ids)
        same_side = (ids < cp_size) == (tp_index == 0)
        piece_slot = jnp.where(same_side, 0, cp_size) + rel_slot[owner_cp]
        table = jnp.concatenate([piece_slot, piece[None]]).astype(jnp.int32)

        wq = w_query.reshape(dim, local_q * head_dim)
        wkv = jnp.concatenate([w_key.reshape(dim, -1), w_value.reshape(dim, -1)], axis=1)
        wo = w_out.reshape(local_q * head_dim, dim)

        def other_half_rows(w):
            quarter = w.shape[0] // cp_size
            own = lax.dynamic_slice_in_dim(w, cp_index * quarter, quarter, axis=0)
            stack = jnp.stack(spread(swap_tp(own)))
            return jnp.take(stack, rel_slot, axis=0).reshape(w.shape)

        wkv_other = other_half_rows(wkv)
        wq_other = other_half_rows(wq)
        wo_other = other_half_rows(wo)

        normed = rms_norm(x_loc, norm_attn)
        dot = functools.partial(jnp.dot, preferred_element_type=jnp.float32)

        def kv_pair(w):
            proj = dot(normed, w)
            return jnp.stack([rope_rotate(proj[:, :head_dim], tables, head_dim), proj[:, head_dim:].astype(jnp.bfloat16)])

        kv_own = kv_pair(wkv)
        kv_other = kv_pair(wkv_other)
        same_own, same_other = spread(kv_own), spread(kv_other)
        cross_other, cross_own = spread(swap_tp(kv_own)), spread(swap_tp(kv_other))
        keys_own = jnp.stack([a[0] for a in same_own + cross_own])
        values_own = jnp.stack([a[1] for a in same_own + cross_own])
        keys_other = jnp.stack([a[0] for a in same_other + cross_other])
        values_other = jnp.stack([a[1] for a in same_other + cross_other])

        q_own = rope_rotate(dot(normed, wq), tables, head_dim)
        q_other = rope_rotate(dot(normed, wq_other), tables, head_dim)
        o_own = attention(table, q_own, keys_own, values_own, "attn_own")
        o_other = attention(table, q_other, keys_other, values_other, "attn_other")
        residual = (x_loc.astype(jnp.float32) + (dot(o_own, wo) + dot(o_other, wo_other))).astype(jnp.bfloat16)
        b = rms_norm(residual, norm_mlp)

        ffn = w_gate.shape[1]
        tile = 640
        acc = mlp_half(b, w_gate, w_up, w_down, tile, ffn // tile, "mlp_own")

        quarter = ffn // cp_size
        chunks = (256, 256, 256, 256, 128)
        padded = sum(chunks)
        base = cp_index * quarter
        pad_cols = ((0, 0), (0, padded - quarter))
        w1_q = jnp.pad(lax.dynamic_slice_in_dim(w_gate, base, quarter, axis=1), pad_cols)
        w3_q = jnp.pad(lax.dynamic_slice_in_dim(w_up, base, quarter, axis=1), pad_cols)
        w2_q = jnp.pad(lax.dynamic_slice_in_dim(w_down, base, quarter, axis=0), pad_cols[::-1])
        off = 0
        acc = acc + residual.astype(jnp.float32)
        for n, width in enumerate(chunks):
            parts = [spread(swap_tp(a)) for a in (w1_q[:, off:off + width], w3_q[:, off:off + width], w2_q[off:off + width])]
            off += width
            last = n == len(chunks) - 1
            acc = mlp_pieces(b, acc, list(zip(*parts)), jnp.bfloat16 if last else jnp.float32, f"mlp_other{n}")
        layer_out = acc

        cache_slots = lax.dynamic_slice_in_dim(piece_slot, 2 * cp_index, 2)
        k_cache = jnp.take(keys_own, cache_slots, axis=0).reshape(2 * tok_dev, head_dim)
        v_cache = jnp.take(values_own, cache_slots, axis=0).reshape(2 * tok_dev, head_dim)
        return layer_out, k_cache, v_cache

    row_spec = P(("dp", "cp", "tp"), None)
    cache_spec = P(("dp", "cp"), "tp")
    head_spec = P(None, "tp", None)
    return jax.shard_map(
        layer_shard,
        mesh=mesh,
        in_specs=(row_spec, P(None), P(None), head_spec, head_spec, head_spec, P("tp", None, None), P(None, "tp"), P(None, "tp"), P("tp", None)),
        out_specs=(row_spec, cache_spec, cache_spec),
        check_vma=False,
    )
```

```python
import functools

import jax
import jax.numpy as jnp
from jax import lax
from jax.experimental import pallas as pl
from jax.experimental.pallas import tpu as pltpu
from jax.sharding import PartitionSpec as P

ROPE_BASE = 500000.0
NORM_EPS = 1e-5
MASK_VALUE = -1e30
LOG2E = 1.4426950408889634
VMEM_LIMIT = 60 * 1024 * 1024
Q_ROWS = 256
K_ROWS = 512
MESH = pl.DeviceIdType.MESH
TILE = 128
N_CHUNKS = 9
N_EARLY = 4


def rms_norm(tensor, gain_vec):
    widened = tensor.astype(jnp.float32)
    inv_rms = lax.rsqrt(jnp.mean(widened * widened, axis=-1, keepdims=True) + NORM_EPS)
    return (widened * inv_rms * gain_vec.astype(jnp.float32)).astype(jnp.bfloat16)


def rope_tables(positions, head_dim):
    half_dim = head_dim // 2
    inv_freq = ROPE_BASE ** (-2.0 * jnp.arange(half_dim, dtype=jnp.float32) / head_dim)
    angles = positions.astype(jnp.float32)[:, None] * inv_freq[None, :]
    return jnp.cos(angles), jnp.sin(angles)


def rope_rotate(proj, tables, head_dim):
    cosine, sine_tab = tables
    half_dim = head_dim // 2
    parts = []
    for h in range(proj.shape[1] // head_dim):
        first_half = proj[:, h * head_dim:h * head_dim + half_dim]
        second_half = proj[:, h * head_dim + half_dim:(h + 1) * head_dim]
        parts += [first_half * cosine - second_half * sine_tab, second_half * cosine + first_half * sine_tab]
    return jnp.concatenate(parts, axis=1).astype(jnp.bfloat16)


class Links:
    def __init__(self, weights, recv, send_sems, recv_sems, n_tiles):
        self.y, self.c = lax.axis_index("tp"), lax.axis_index("cp")
        self.peer = {
            "y": {"tp": 1 - self.y},
            "x": {"cp": lax.rem(self.c + 2, 4)},
            "d": {"cp": self.c + 1 - 2 * lax.rem(self.c, 2)},
        }
        self.weights, self.recv, self.send_sems, self.recv_sems = weights, recv, send_sems, recv_sems
        self.n_tiles = n_tiles
        self.started = []

    def barrier(self):
        sem = pltpu.get_barrier_semaphore()
        for name in "yxd":
            pl.semaphore_signal(sem, inc=1, device_id=self.peer[name], device_id_type=MESH)
        pl.semaphore_wait(sem, 3)

    def remote(self, src, dst, ssem, rsem, to):
        return pltpu.make_async_remote_copy(src_ref=src, dst_ref=dst, send_sem=ssem, recv_sem=rsem, device_id=self.peer[to], device_id_type=MESH)

    def chunk(self, stage, j):
        to = "yxdd"[stage]
        copies = []
        for a in range(3):
            if stage == 0:
                tile = jnp.minimum(4 * j + self.c, self.n_tiles - 1)
                sl = pl.ds(pl.multiple_of(tile * TILE, TILE), TILE)
                src = self.weights[a].at[sl, :] if a == 2 else self.weights[a].at[:, sl]
            else:
                src = self.recv[a].at[j, (0, 0, 0, 1)[stage]]
            copies.append(self.remote(src, self.recv[a].at[j, stage], self.send_sems.at[j, stage, a], self.recv_sems.at[j, stage, a], to))
        return copies

    def start(self, stage, j):
        for copy in self.chunk(stage, j):
            copy.start()

    def arrived(self, stage, j):
        for copy in self.chunk(stage, j):
            copy.wait_recv()

    def sent(self, stage, j):
        for copy in self.chunk(stage, j):
            copy.wait_send()


EARLY_FORWARD = ((0, 16), (1, 20), (2, 23))
EARLY_SECOND = ((0, 20), (1, 23))


def attention_kernel(q_ref, kv_ref, wo_ref, w1_ref, w3_ref, w2_ref, o_ref, kc_ref, vc_ref, ro_ref, r1_ref, r3_ref, r2_ref,
                     kv_buf, m_sc, l_sc, acc_sc, send_sems, recv_sems, kv_send, kv_recv, wo_send, wo_recv):
    head_dim = 128
    chunk_len = kv_ref.shape[2]
    heads = q_ref.shape[2] // head_dim
    chains = 2
    per_chain = heads // chains
    rows = per_chain * Q_ROWS
    q_blocks = chunk_len // Q_ROWS
    coef = head_dim ** -0.5 * LOG2E
    net = Links((w1_ref, w3_ref, w2_ref), (r1_ref, r3_ref, r2_ref), send_sems, recv_sems, w1_ref.shape[1] // TILE)
    y, c = net.y, net.c
    core_lower = lax.rem(c + y, 2)
    chip_lower = lax.rem(c // 2 + y, 2)

    def kv_copy(n):
        src, dst, to = ((None, 1, "x"), (None, 2, "d"), (1, 3, "d"), (None, 4, "y"), (4, 5, "x"), (4, 6, "d"), (5, 7, "d"))[n]
        return net.remote(kv_ref if src is None else kv_buf.at[src], kv_buf.at[dst], kv_send.at[n], kv_recv.at[n], to)

    def wo_copy(stage):
        quarter = wo_ref.shape[0] // 4
        src = wo_ref.at[pl.ds(pl.multiple_of(c * quarter, 64), quarter), :] if stage == 0 else ro_ref.at[(0, 0, 0, 1)[stage]]
        return net.remote(src, ro_ref.at[stage], wo_send.at[stage], wo_recv.at[stage], "yxdd"[stage])

    net.barrier()
    kv_copy(3).start()
    kv_copy(0).start()
    kv_copy(1).start()
    wo_copy(0).start()
    net.start(0, 0)
    net.start(0, 1)
    m_sc[...] = jnp.full_like(m_sc, MASK_VALUE)
    l_sc[...] = jnp.zeros_like(l_sc)
    acc_sc[...] = jnp.zeros_like(acc_sc)
    kv_buf[0] = kv_ref[...]
    kv_copy(1).wait_recv()

    def block(q_parts, state, start, slot, head, off, masked):
        k_blk = kv_buf[slot, head, 0, pl.ds(off, K_ROWS), :]
        v_blk = kv_buf[slot, head, 1, pl.ds(off, K_ROWS), :]
        for a in range(chains):
            s = lax.dot_general(q_parts[a], k_blk, (((1,), (1,)), ((), ())), preferred_element_type=jnp.float32)
            if masked:
                q_pos = start + lax.rem(lax.broadcasted_iota(jnp.int32, (rows, K_ROWS), 0), Q_ROWS)
                k_pos = off + lax.broadcasted_iota(jnp.int32, (rows, K_ROWS), 1)
                s = jnp.where(k_pos <= q_pos, s, MASK_VALUE)
            m_prev = m_sc[state, a]
            m_new = jnp.maximum(m_prev, jnp.max(s, axis=1, keepdims=True))
            alpha = jnp.exp2((m_prev - m_new) * coef)
            mc = m_new * coef
            sums = l_sc[state, a] * alpha
            p_tiles = []
            for j in range(K_ROWS // 128):
                p = jnp.exp2(s[:, j * 128:(j + 1) * 128] * coef - mc)
                sums = sums + p
                p_tiles.append(p.astype(jnp.bfloat16))
            l_sc[state, a] = sums
            m_sc[state, a] = m_new
            p_all = jnp.concatenate(p_tiles, axis=1)
            acc_sc[state, a] = acc_sc[state, a] * alpha + jnp.dot(p_all, v_blk, preferred_element_type=jnp.float32)

    def load_q(head, qb):
        sl = pl.ds(pl.multiple_of(qb * Q_ROWS, Q_ROWS), Q_ROWS)
        return [jnp.concatenate([q_ref[head, sl, (a * per_chain + h) * head_dim:(a * per_chain + h + 1) * head_dim] for h in range(per_chain)], axis=0) for a in range(chains)]

    per_pass = 2 * q_blocks
    per_piece = chunk_len // K_ROWS

    def step(s, carry):
        phase = s // per_pass
        head = lax.rem(s, per_pass) // q_blocks
        qb = lax.rem(s, q_blocks)
        state = lax.rem(s, per_pass)

        def at(k, fn):
            pl.when(s == k)(fn)

        @pl.when(s == 5)
        def _():
            kv_copy(0).wait_recv()
            kv_copy(2).start()

        @pl.when(s == 7)
        def _():
            kv_copy(3).wait_recv()
            kv_copy(4).start()
            kv_copy(5).start()

        @pl.when(s == 8)
        def _():
            kv_copy(2).wait_recv()

        @pl.when(s == 11)
        def _():
            wo_copy(0).wait_recv()
            wo_copy(1).start()
            wo_copy(2).start()

        @pl.when(s == 14)
        def _():
            kv_copy(4).wait_recv()
            kv_copy(6).start()

        @pl.when(s == 16)
        def _():
            kv_copy(5).wait_recv()
            kv_copy(6).wait_recv()
            wo_copy(1).wait_recv()
            wo_copy(3).start()

        for j, when in EARLY_FORWARD:
            @pl.when(s == when)
            def _(j=j):
                net.arrived(0, j)
                net.start(1, j)
                net.start(2, j)
                if j + 2 < N_EARLY:
                    net.start(0, j + 2)

        for j, when in EARLY_SECOND:
            @pl.when(s == when)
            def _(j=j):
                net.arrived(1, j)
                net.start(3, j)

        q_parts = load_q(head, qb)
        start = qb * Q_ROWS
        diag = start // K_ROWS
        is_first = (phase == 0).astype(jnp.int32)
        is_last = (phase == 2).astype(jnp.int32)
        is_mid = 1 - is_first - is_last
        count = is_first * (diag + per_piece * core_lower) + is_mid * 2 * per_piece * chip_lower + is_last * 4 * per_piece * y
        kv_head = head + is_last * (1 - 2 * head)

        def inner(i, carry):
            in_core = (i >= diag).astype(jnp.int32)
            idx = i - is_first * in_core * diag
            slot = is_first * 2 * in_core + is_mid * (1 + 2 * (i // per_piece)) + is_last * (4 + i // per_piece)
            off = (is_first * (in_core * lax.rem(idx, per_piece) + (1 - in_core) * i) + (1 - is_first) * lax.rem(i, per_piece)) * K_ROWS
            block(q_parts, state, start, slot, kv_head, pl.multiple_of(off, K_ROWS), False)
            return carry

        lax.fori_loop(0, count, inner, 0)

        @pl.when(phase == 0)
        def _():
            block(q_parts, state, start, 0, head, pl.multiple_of(diag * K_ROWS, K_ROWS), True)

        return carry

    lax.fori_loop(0, 3 * per_pass, step, 0)

    def finish(state, carry):
        head = state // q_blocks
        sl = pl.ds(pl.multiple_of(lax.rem(state, q_blocks) * Q_ROWS, Q_ROWS), Q_ROWS)
        for a in range(chains):
            total = jnp.sum(l_sc[state, a], axis=1, keepdims=True)
            out = (acc_sc[state, a] / total).astype(jnp.bfloat16)
            for h in range(per_chain):
                o_ref[head, sl, (a * per_chain + h) * head_dim:(a * per_chain + h + 1) * head_dim] = out[h * Q_ROWS:(h + 1) * Q_ROWS]
        return carry

    lax.fori_loop(0, per_pass, finish, 0)

    for e in range(2):
        late = c // 2
        owner = (1 - late) * (2 * c + e) + late * (7 - 2 * c - e)
        cross = lax.rem(late + y, 2)
        slot = 4 * cross + 2 * lax.rem(owner + c, 2) + lax.rem(owner // 2 + c // 2, 2)
        kc_ref[e * chunk_len:(e + 1) * chunk_len] = kv_buf[slot, cross, 0]
        vc_ref[e * chunk_len:(e + 1) * chunk_len] = kv_buf[slot, cross, 1]

    wo_copy(2).wait_recv()
    wo_copy(3).wait_recv()
    for n in range(7):
        kv_copy(n).wait_send()
    for n in range(4):
        wo_copy(n).wait_send()
    forwarded = [j for j, _ in EARLY_FORWARD]
    second = [j for j, _ in EARLY_SECOND]
    for j in range(N_EARLY):
        if j not in forwarded:
            net.arrived(0, j)
        net.sent(0, j)
    for j in forwarded:
        if j not in second:
            net.arrived(1, j)
        net.arrived(2, j)
        net.sent(1, j)
        net.sent(2, j)
    for j in second:
        net.arrived(3, j)
        net.sent(3, j)


def attention(q, kv, wo, w1, w3, w2):
    _, rows, width = q.shape
    dim = w1.shape[0]
    states = 2 * rows // Q_ROWS
    m_rows = width // 128 // 2 * Q_ROWS
    vm = pl.BlockSpec(memory_space=pltpu.VMEM)
    hbm = pl.BlockSpec(memory_space=pl.ANY)
    bf16 = jnp.bfloat16
    n = N_EARLY
    return pl.pallas_call(
        attention_kernel,
        in_specs=[vm, vm, hbm, hbm, hbm, hbm],
        out_specs=[vm, vm, vm, hbm, hbm, hbm, hbm],
        out_shape=[
            jax.ShapeDtypeStruct(q.shape, bf16),
            jax.ShapeDtypeStruct((2 * rows, 128), bf16),
            jax.ShapeDtypeStruct((2 * rows, 128), bf16),
            jax.ShapeDtypeStruct((4, wo.shape[0] // 4, dim), bf16),
            jax.ShapeDtypeStruct((N_CHUNKS, 4, dim, TILE), bf16),
            jax.ShapeDtypeStruct((N_CHUNKS, 4, dim, TILE), bf16),
            jax.ShapeDtypeStruct((N_CHUNKS, 4, TILE, dim), bf16),
        ],
        scratch_shapes=[
            pltpu.VMEM((8,) + kv.shape, bf16),
            pltpu.VMEM((states, 2, m_rows, 128), jnp.float32),
            pltpu.VMEM((states, 2, m_rows, 128), jnp.float32),
            pltpu.VMEM((states, 2, m_rows, 128), jnp.float32),
            pltpu.SemaphoreType.DMA((n, 4, 3)),
            pltpu.SemaphoreType.DMA((n, 4, 3)),
            pltpu.SemaphoreType.DMA((7,)),
            pltpu.SemaphoreType.DMA((7,)),
            pltpu.SemaphoreType.DMA((4,)),
            pltpu.SemaphoreType.DMA((4,)),
        ],
        compiler_params=pltpu.CompilerParams(collective_id=0, has_side_effects=True, vmem_limit_bytes=VMEM_LIMIT),
        cost_estimate=pl.CostEstimate(flops=16 * rows * 4096 * width, bytes_accessed=32 * 2**20, transcendentals=rows * 4096 * 12),
        name="attention",
    )(q, kv, wo, w1, w3, w2)


M_BLOCK = 512
LATE_FORWARD = {0: (3,), 4: (4,), 9: (5,)}
LATE_SECOND = {0: (2,), 5: (3,), 10: (4,)}
END_FORWARD = {12: (6,), 14: (7,), 15: (8,)}
END_SECOND = {12: (5,), 14: (6,), 15: (7,), 16: (8,)}
LOAD_AFTER = 12


def mlp_kernel(b_ref, res_ref, w1_ref, w3_ref, w2_ref, a1_ref, a3_ref, a2_ref, out_ref, r1_ref, r3_ref, r2_ref,
               w1_sc, w3_sc, w2_sc, acc_sc, load_sems, send_sems, recv_sems):
    dim = b_ref.shape[1]
    width = 4 * TILE
    n_tiles = w1_ref.shape[1] // TILE
    net = Links((w1_ref, w3_ref, w2_ref), (r1_ref, r3_ref, r2_ref), send_sems, recv_sems, n_tiles)
    own_last = (n_tiles - 4) * TILE

    def own_loads(j, slot):
        off = min(j * width, own_last) if isinstance(j, int) else pl.multiple_of(jnp.minimum(j * width, own_last), TILE)
        sl = pl.ds(off, width)
        return [
            pltpu.make_async_copy(w1_ref.at[:, sl], w1_sc.at[slot], load_sems.at[slot, 0]),
            pltpu.make_async_copy(w3_ref.at[:, sl], w3_sc.at[slot], load_sems.at[slot, 1]),
            pltpu.make_async_copy(w2_ref.at[sl, :], w2_sc.at[slot], load_sems.at[slot, 2]),
        ]

    def other_loads(j, slot):
        copies = []
        for p in range(4):
            sl = pl.ds(p * TILE, TILE)
            copies.append(pltpu.make_async_copy(r1_ref.at[j, p], w1_sc.at[slot, :, sl], load_sems.at[slot, 0]))
            copies.append(pltpu.make_async_copy(r3_ref.at[j, p], w3_sc.at[slot, :, sl], load_sems.at[slot, 1]))
            copies.append(pltpu.make_async_copy(r2_ref.at[j, p], w2_sc.at[slot, sl, :], load_sems.at[slot, 2]))
        return copies

    def compute(slot, lane_keep):
        def rows_step(m, carry):
            sl = pl.ds(pl.multiple_of(m * M_BLOCK, M_BLOCK), M_BLOCK)
            b = b_ref[sl, :]
            gate = jnp.dot(b, w1_sc[slot], preferred_element_type=jnp.float32)
            up = jnp.dot(b, w3_sc[slot], preferred_element_type=jnp.float32)
            hidden = jax.nn.silu(gate) * up
            hidden = jnp.where(lane_keep > 0.5, hidden, 0.0).astype(jnp.bfloat16)
            acc_sc[sl, :] += jnp.dot(hidden, w2_sc[slot], preferred_element_type=jnp.float32)
            return carry

        lax.fori_loop(0, b_ref.shape[0] // M_BLOCK, rows_step, 0)

    net.barrier()
    net.start(0, 4)
    net.start(0, 5)
    for copy in own_loads(0, 0):
        copy.start()
    acc_sc[...] = res_ref[...].astype(jnp.float32)
    lane_tile = lax.broadcasted_iota(jnp.int32, (1, width), 1) // TILE
    source = 2 * lax.rem(lane_tile + net.c // 2, 2) + lax.rem(lane_tile // 2 + lax.rem(net.c, 2), 2)

    def pass_on(s, forward, second):
        for when, chunks in forward.items():
            @pl.when(s == when)
            def _(chunks=chunks):
                for j in chunks:
                    if j >= N_EARLY:
                        net.arrived(0, j)
                    net.start(1, j)
                    net.start(2, j)
                    if 6 <= j + 2 < N_CHUNKS:
                        net.start(0, j + 2)
        for when, chunks in second.items():
            @pl.when(s == when)
            def _(chunks=chunks):
                for j in chunks:
                    if j >= 3:
                        net.arrived(1, j)
                    net.start(3, j)

    def load_next(s, slot, after):
        for j in range(2, N_CHUNKS):
            if (N_CHUNKS - 1 + j >= LOAD_AFTER) == after:
                @pl.when(s == N_CHUNKS - 1 + j)
                def _(j=j):
                    if j >= 3:
                        net.arrived(2, j)
                    net.arrived(3, j)

        if not after:
            @pl.when(s + 1 < N_CHUNKS)
            def _():
                for copy in own_loads(s + 1, 1 - slot):
                    copy.start()

        first, last = (LOAD_AFTER, 2 * N_CHUNKS - 1) if after else (N_CHUNKS - 1, LOAD_AFTER)

        @pl.when((s >= first) & (s < last))
        def _():
            for copy in other_loads(s + 1 - N_CHUNKS, 1 - slot):
                copy.start()

    def step(s, carry):
        slot = lax.rem(s, 2)
        pass_on(s, LATE_FORWARD, LATE_SECOND)
        load_next(s, slot, False)
        for copy in own_loads(0, slot):
            copy.wait()
        own_end = (s == N_CHUNKS - 1).astype(jnp.float32)
        other_end = (s == 2 * N_CHUNKS - 1).astype(jnp.float32)
        keep = 1.0 - own_end * (lane_tile == 0).astype(jnp.float32) - other_end * (source == 3).astype(jnp.float32)
        compute(slot, keep)
        pass_on(s, END_FORWARD, END_SECOND)
        load_next(s, slot, True)
        return carry

    lax.fori_loop(0, 2 * N_CHUNKS, step, 0)
    out_ref[...] = acc_sc[...].astype(out_ref.dtype)
    for j in range(4, N_CHUNKS):
        net.sent(0, j)
    for j in range(3, N_CHUNKS):
        net.sent(1, j)
        net.sent(2, j)
    for j in range(2, N_CHUNKS):
        net.sent(3, j)


def mlp(b, res, w1, w3, w2, early):
    rows, dim = b.shape
    vm = pl.BlockSpec(memory_space=pltpu.VMEM)
    hbm = pl.BlockSpec(memory_space=pl.ANY)
    bf16 = jnp.bfloat16
    width = 4 * TILE
    n = N_CHUNKS
    return pl.pallas_call(
        mlp_kernel,
        in_specs=[vm, vm] + [hbm] * 6,
        out_specs=[vm, hbm, hbm, hbm],
        out_shape=[jax.ShapeDtypeStruct((rows, dim), bf16)] + [jax.ShapeDtypeStruct(a.shape, bf16) for a in early],
        input_output_aliases={5: 1, 6: 2, 7: 3},
        scratch_shapes=[
            pltpu.VMEM((2, dim, width), bf16),
            pltpu.VMEM((2, dim, width), bf16),
            pltpu.VMEM((2, width, dim), bf16),
            pltpu.VMEM((rows, dim), jnp.float32),
            pltpu.SemaphoreType.DMA((2, 3)),
            pltpu.SemaphoreType.DMA((n, 4, 3)),
            pltpu.SemaphoreType.DMA((n, 4, 3)),
        ],
        compiler_params=pltpu.CompilerParams(collective_id=1, has_side_effects=True, vmem_limit_bytes=VMEM_LIMIT),
        cost_estimate=pl.CostEstimate(flops=12 * rows * dim * w1.shape[1], bytes_accessed=12 * dim * w1.shape[1], transcendentals=2 * rows * w1.shape[1]),
        name="mlp",
    )(b, res, w1, w3, w2, *early)[0]

def solution(mesh):
    cp_size = mesh.shape["cp"]
    tp_swap = [(0, 1), (1, 0)]
    chip_swap = [(0, 2), (2, 0), (1, 3), (3, 1)]
    core_swap = [(0, 1), (1, 0), (2, 3), (3, 2)]

    def swap_tp(a):
        return lax.ppermute(a, "tp", tp_swap)

    def swap_chip(a):
        return lax.ppermute(a, "cp", chip_swap)

    def swap_core(a):
        return lax.ppermute(a, "cp", core_swap)

    def spread(a):
        b = swap_chip(a)
        return [a, b, swap_core(a), swap_core(b)]

    def layer_shard(x_loc, norm_attn, norm_mlp, w_query, w_key, w_value, w_out, w_gate, w_up, w_down):
        tok_dev, dim = x_loc.shape
        local_q, head_dim = w_query.shape[1], w_query.shape[2]
        cp_index = lax.axis_index("cp")
        tp_index = lax.axis_index("tp")
        n_pieces = 2 * cp_size
        piece = jnp.where(tp_index == 0, cp_index, n_pieces - 1 - cp_index)
        tables = rope_tables(piece * tok_dev + jnp.arange(tok_dev, dtype=jnp.int32), head_dim)

        peers = jnp.arange(cp_size, dtype=jnp.int32) ^ cp_index
        rel_slot = jnp.where(peers == 1, 2, jnp.where(peers == 2, 1, peers))

        wq = w_query.reshape(dim, local_q * head_dim)
        wkv = jnp.concatenate([w_key.reshape(dim, -1), w_value.reshape(dim, -1)], axis=1)
        wo = w_out.reshape(local_q * head_dim, dim)

        def other_half_rows(w):
            quarter = w.shape[0] // cp_size
            own = lax.dynamic_slice_in_dim(w, cp_index * quarter, quarter, axis=0)
            stack = jnp.stack(spread(swap_tp(own)))
            return jnp.take(stack, rel_slot, axis=0).reshape(w.shape)

        wkv_other = other_half_rows(wkv)
        wq_other = other_half_rows(wq)

        normed = rms_norm(x_loc, norm_attn)
        dot = functools.partial(jnp.dot, preferred_element_type=jnp.float32)

        def kv_pair(w):
            proj = dot(normed, w)
            return jnp.stack([rope_rotate(proj[:, :head_dim], tables, head_dim), proj[:, head_dim:].astype(jnp.bfloat16)])

        kv = jnp.stack([kv_pair(wkv), kv_pair(wkv_other)])
        q = jnp.stack([rope_rotate(dot(normed, wq), tables, head_dim), rope_rotate(dot(normed, wq_other), tables, head_dim)])
        o, k_cache, v_cache, wo_parts, *early = attention(q, kv, wo, w_gate, w_up, w_down)
        wo_other = jnp.take(wo_parts, rel_slot, axis=0).reshape(wo.shape)
        residual = (x_loc.astype(jnp.float32) + (dot(o[0], wo) + dot(o[1], wo_other))).astype(jnp.bfloat16)
        layer_out = mlp(rms_norm(residual, norm_mlp), residual, w_gate, w_up, w_down, early)
        return layer_out, k_cache, v_cache

    row_spec = P(("dp", "cp", "tp"), None)
    cache_spec = P(("dp", "cp"), "tp")
    head_spec = P(None, "tp", None)
    return jax.shard_map(
        layer_shard,
        mesh=mesh,
        in_specs=(row_spec, P(None), P(None), head_spec, head_spec, head_spec, P("tp", None, None), P(None, "tp"), P(None, "tp"), P("tp", None)),
        out_specs=(row_spec, cache_spec, cache_spec),
        check_vma=False,
    )
```

```python
import functools

import jax
import jax.numpy as jnp
from jax import lax
from jax.experimental import pallas as pl
from jax.experimental.pallas import tpu as pltpu
from jax.sharding import PartitionSpec as P

ROPE_BASE = 500000.0
NORM_EPS = 1e-5
MASK_VALUE = -1e30
LOG2E = 1.4426950408889634
VMEM_LIMIT = 60 * 1024 * 1024
Q_ROWS = 256
K_ROWS = 512
MESH = pl.DeviceIdType.MESH
TILE = 128
N_CHUNKS = 9
N_EARLY = 5


def rope_tables(positions, head_dim):
    half_dim = head_dim // 2
    inv_freq = ROPE_BASE ** (-2.0 * jnp.arange(half_dim, dtype=jnp.float32) / head_dim)
    angles = positions.astype(jnp.float32)[:, None] * inv_freq[None, :]
    return jnp.cos(angles), jnp.sin(angles)


class Links:
    def __init__(self, weights, recv, send_sems, recv_sems, n_tiles):
        self.y, self.c = lax.axis_index("tp"), lax.axis_index("cp")
        self.peer = {
            "y": {"tp": 1 - self.y},
            "x": {"cp": lax.rem(self.c + 2, 4)},
            "d": {"cp": self.c + 1 - 2 * lax.rem(self.c, 2)},
        }
        self.weights, self.recv, self.send_sems, self.recv_sems = weights, recv, send_sems, recv_sems
        self.n_tiles = n_tiles
        self.started = []

    def barrier(self):
        sem = pltpu.get_barrier_semaphore()
        for name in "yxd":
            pl.semaphore_signal(sem, inc=1, device_id=self.peer[name], device_id_type=MESH)
        pl.semaphore_wait(sem, 3)

    def remote(self, src, dst, ssem, rsem, to):
        return pltpu.make_async_remote_copy(src_ref=src, dst_ref=dst, send_sem=ssem, recv_sem=rsem, device_id=self.peer[to], device_id_type=MESH)

    def chunk(self, stage, j):
        to = "yxdd"[stage]
        copies = []
        for a in range(3):
            if stage == 0:
                tile = jnp.minimum(4 * j + self.c, self.n_tiles - 1)
                sl = pl.ds(pl.multiple_of(tile * TILE, TILE), TILE)
                src = self.weights[a].at[sl, :] if a == 2 else self.weights[a].at[:, sl]
            else:
                src = self.recv[a].at[j, (0, 0, 0, 1)[stage]]
            copies.append(self.remote(src, self.recv[a].at[j, stage], self.send_sems.at[j, stage, a], self.recv_sems.at[j, stage, a], to))
        return copies

    def start(self, stage, j):
        for copy in self.chunk(stage, j):
            copy.start()

    def arrived(self, stage, j):
        for copy in self.chunk(stage, j):
            copy.wait_recv()

    def sent(self, stage, j):
        for copy in self.chunk(stage, j):
            copy.wait_send()


EARLY_FORWARD = ((0, 14), (1, 17), (2, 19), (3, 21))
EARLY_SECOND = ((0, 18), (1, 20), (2, 22))
SLOT_SOURCE = (0, 0, 0, 1)


def normed_rows(wide, gain):
    inv_rms = lax.rsqrt(jnp.mean(wide * wide, axis=-1, keepdims=True) + NORM_EPS)
    return (wide * inv_rms * gain).astype(jnp.bfloat16)


def attention_kernel(x_ref, gain_ref, cos_ref, sin_ref, wq_ref, wkv_ref, wo_ref, w1_ref, w3_ref, w2_ref,
                     o_ref, kc_ref, vc_ref, ro_ref, r1_ref, r3_ref, r2_ref,
                     a_sc, q_sc, wq_sc, wkv_sc, kv_buf, m_sc, l_sc, acc_sc, send_sems, recv_sems, kv_send, kv_recv, wt_send, wt_recv):
    head_dim = 128
    half_dim = head_dim // 2
    chunk_len = x_ref.shape[0]
    width = wq_ref.shape[1]
    heads = width // head_dim
    chains = 2
    per_chain = heads // chains
    rows = per_chain * Q_ROWS
    q_blocks = chunk_len // Q_ROWS
    coef = head_dim ** -0.5 * LOG2E
    net = Links((w1_ref, w3_ref, w2_ref), (r1_ref, r3_ref, r2_ref), send_sems, recv_sems, w1_ref.shape[1] // TILE)
    y, c = net.y, net.c
    core_lower = lax.rem(c + y, 2)
    chip_lower = lax.rem(c // 2 + y, 2)
    other_chip = lax.rem(c + 2, 4)

    def kv_copy(n, hd):
        src, dst, to = ((0, 1, "x"), (0, 2, "d"), (1, 3, "d"), (0, 4, "y"), (4, 5, "x"), (4, 6, "d"), (5, 7, "d"))[n]
        return net.remote(kv_buf.at[src, hd], kv_buf.at[dst, hd], kv_send.at[n, hd], kv_recv.at[n, hd], to)

    def weight_copy(kind, stage):
        own, held = ((wkv_ref, wkv_sc), (wq_ref, wq_sc), (wo_ref, ro_ref))[kind]
        quarter = own.shape[0] // 4
        sl = pl.ds(pl.multiple_of((other_chip if stage == 3 else c) * quarter, 64), quarter)
        src = own if stage == 0 else held
        return net.remote(src.at[sl, :], held.at[sl, :], wt_send.at[kind, stage], wt_recv.at[kind, stage], "yxdd"[stage])

    def row_slice(i):
        return pl.ds(pl.multiple_of(i * Q_ROWS, Q_ROWS), Q_ROWS)

    def rope(t, sl):
        return (t * cos_ref[sl, :] + pltpu.roll(t, half_dim, 1) * sin_ref[sl, :]).astype(jnp.bfloat16)

    def norm_x():
        def body(i, carry):
            sl = row_slice(i)
            a_sc[sl, :] = normed_rows(x_ref[sl, :].astype(jnp.float32), gain_ref[...].astype(jnp.float32))
            return carry
        lax.fori_loop(0, q_blocks, body, 0)

    def make_kv(w_ref, hd):
        def body(i, carry):
            sl = row_slice(i)
            proj = jnp.dot(a_sc[sl, :], w_ref[...], preferred_element_type=jnp.float32)
            kv_buf[0, hd, 0, sl, :] = rope(proj[:, :head_dim], sl)
            kv_buf[0, hd, 1, sl, :] = proj[:, head_dim:].astype(jnp.bfloat16)
            return carry
        lax.fori_loop(0, q_blocks, body, 0)

    def make_q(w_ref, hd):
        def body(i, carry):
            sl = row_slice(i)
            proj = jnp.dot(a_sc[sl, :], w_ref[...], preferred_element_type=jnp.float32)
            for h in range(heads):
                cols = slice(h * head_dim, (h + 1) * head_dim)
                q_sc[hd, sl, cols] = rope(proj[:, cols], sl)
            return carry
        lax.fori_loop(0, q_blocks, body, 0)

    net.barrier()
    weight_copy(0, 0).start()
    weight_copy(1, 0).start()
    norm_x()
    make_kv(wkv_ref, 0)
    m_sc[...] = jnp.full_like(m_sc, MASK_VALUE)
    l_sc[...] = jnp.zeros_like(l_sc)
    acc_sc[...] = jnp.zeros_like(acc_sc)
    weight_copy(0, 0).wait_recv()
    weight_copy(0, 1).start()
    weight_copy(0, 2).start()
    kv_copy(1, 0).start()
    kv_copy(0, 0).start()
    kv_copy(3, 0).start()
    make_q(wq_ref, 0)

    def block(q_parts, state, start, slot, head, off, masked):
        k_blk = kv_buf[slot, head, 0, pl.ds(off, K_ROWS), :]
        v_blk = kv_buf[slot, head, 1, pl.ds(off, K_ROWS), :]
        for a in range(chains):
            s = lax.dot_general(q_parts[a], k_blk, (((1,), (1,)), ((), ())), preferred_element_type=jnp.float32)
            if masked:
                q_pos = start + lax.rem(lax.broadcasted_iota(jnp.int32, (rows, K_ROWS), 0), Q_ROWS)
                k_pos = off + lax.broadcasted_iota(jnp.int32, (rows, K_ROWS), 1)
                s = jnp.where(k_pos <= q_pos, s, MASK_VALUE)
            m_prev = m_sc[state, a]
            m_new = jnp.maximum(m_prev, jnp.max(s, axis=1, keepdims=True))
            alpha = jnp.exp2((m_prev - m_new) * coef)
            mc = m_new * coef
            sums = l_sc[state, a] * alpha
            p_tiles = []
            for j in range(K_ROWS // 128):
                p = jnp.exp2(s[:, j * 128:(j + 1) * 128] * coef - mc)
                sums = sums + p
                p_tiles.append(p.astype(jnp.bfloat16))
            l_sc[state, a] = sums
            m_sc[state, a] = m_new
            p_all = jnp.concatenate(p_tiles, axis=1)
            acc_sc[state, a] = acc_sc[state, a] * alpha + jnp.dot(p_all, v_blk, preferred_element_type=jnp.float32)

    def load_q(head, qb):
        sl = row_slice(qb)
        return [jnp.concatenate([q_sc[head, sl, (a * per_chain + h) * head_dim:(a * per_chain + h + 1) * head_dim] for h in range(per_chain)], axis=0) for a in range(chains)]

    per_piece = chunk_len // K_ROWS

    def step(s, carry):
        phase = s // q_blocks
        qb = lax.rem(s, q_blocks)
        is_last = phase // 4
        is_mid = (1 - is_last) * lax.rem(phase, 2)
        is_first = 1 - is_last - is_mid
        head = (1 - is_last) * (phase // 2) + is_last * (phase - 4)
        state = head * q_blocks + qb

        @pl.when(s == 0)
        def _():
            kv_copy(1, 0).wait_recv()

        @pl.when(s == 1)
        def _():
            weight_copy(0, 1).wait_recv()
            weight_copy(0, 3).start()

        @pl.when(s == 2)
        def _():
            weight_copy(0, 2).wait_recv()
            weight_copy(0, 3).wait_recv()
            make_kv(wkv_sc, 1)
            weight_copy(1, 0).wait_recv()
            weight_copy(1, 1).start()
            weight_copy(1, 2).start()

        @pl.when(s == 3)
        def _():
            kv_copy(1, 1).start()
            kv_copy(0, 1).start()
            kv_copy(3, 1).start()
            weight_copy(2, 0).start()
            net.start(0, 0)
            net.start(0, 1)
            kv_copy(0, 0).wait_recv()
            kv_copy(2, 0).start()

        @pl.when(s == 4)
        def _():
            kv_copy(2, 0).wait_recv()

        @pl.when(s == 6)
        def _():
            weight_copy(1, 1).wait_recv()
            weight_copy(1, 3).start()
            kv_copy(3, 0).wait_recv()
            kv_copy(4, 0).start()
            kv_copy(5, 0).start()

        @pl.when(s == 7)
        def _():
            weight_copy(1, 2).wait_recv()
            weight_copy(1, 3).wait_recv()
            make_q(wq_sc, 1)

        @pl.when(s == 8)
        def _():
            kv_copy(1, 1).wait_recv()

        @pl.when(s == 9)
        def _():
            kv_copy(0, 1).wait_recv()
            kv_copy(2, 1).start()

        @pl.when(s == 10)
        def _():
            kv_copy(3, 1).wait_recv()
            kv_copy(4, 1).start()
            kv_copy(5, 1).start()

        @pl.when(s == 12)
        def _():
            kv_copy(2, 1).wait_recv()
            weight_copy(2, 0).wait_recv()
            weight_copy(2, 1).start()
            weight_copy(2, 2).start()

        @pl.when(s == 13)
        def _():
            kv_copy(4, 0).wait_recv()
            kv_copy(6, 0).start()

        @pl.when(s == 14)
        def _():
            kv_copy(4, 1).wait_recv()
            kv_copy(6, 1).start()

        @pl.when(s == 16)
        def _():
            for hd in range(2):
                kv_copy(5, hd).wait_recv()
                kv_copy(6, hd).wait_recv()
            weight_copy(2, 1).wait_recv()
            weight_copy(2, 3).start()

        for j, when in EARLY_FORWARD:
            @pl.when(s == when)
            def _(j=j):
                net.arrived(0, j)
                net.start(1, j)
                net.start(2, j)
                if j + 2 < N_EARLY:
                    net.start(0, j + 2)

        for j, when in EARLY_SECOND:
            @pl.when(s == when)
            def _(j=j):
                net.arrived(1, j)
                net.start(3, j)

        q_parts = load_q(head, qb)
        start = qb * Q_ROWS
        diag = start // K_ROWS
        count = is_first * (diag + per_piece * core_lower) + is_mid * 2 * per_piece * chip_lower + is_last * 4 * per_piece * y
        kv_head = head + is_last * (1 - 2 * head)

        def inner(i, carry):
            in_core = (i >= diag).astype(jnp.int32)
            idx = i - is_first * in_core * diag
            slot = is_first * 2 * in_core + is_mid * (1 + 2 * (i // per_piece)) + is_last * (4 + i // per_piece)
            off = (is_first * (in_core * lax.rem(idx, per_piece) + (1 - in_core) * i) + (1 - is_first) * lax.rem(i, per_piece)) * K_ROWS
            block(q_parts, state, start, slot, kv_head, pl.multiple_of(off, K_ROWS), False)
            return carry

        lax.fori_loop(0, count, inner, 0)

        @pl.when(is_first == 1)
        def _():
            block(q_parts, state, start, 0, head, pl.multiple_of(diag * K_ROWS, K_ROWS), True)

        return carry

    lax.fori_loop(0, 6 * q_blocks, step, 0)

    def finish(state, carry):
        head = state // q_blocks
        sl = row_slice(lax.rem(state, q_blocks))
        for a in range(chains):
            total = jnp.sum(l_sc[state, a], axis=1, keepdims=True)
            out = (acc_sc[state, a] / total).astype(jnp.bfloat16)
            for h in range(per_chain):
                o_ref[head, sl, (a * per_chain + h) * head_dim:(a * per_chain + h + 1) * head_dim] = out[h * Q_ROWS:(h + 1) * Q_ROWS]
        return carry

    lax.fori_loop(0, 2 * q_blocks, finish, 0)

    for e in range(2):
        late = c // 2
        owner = (1 - late) * (2 * c + e) + late * (7 - 2 * c - e)
        cross = lax.rem(late + y, 2)
        slot = 4 * cross + 2 * lax.rem(owner + c, 2) + lax.rem(owner // 2 + c // 2, 2)
        kc_ref[e * chunk_len:(e + 1) * chunk_len] = kv_buf[slot, cross, 0]
        vc_ref[e * chunk_len:(e + 1) * chunk_len] = kv_buf[slot, cross, 1]

    weight_copy(2, 2).wait_recv()
    weight_copy(2, 3).wait_recv()
    for hd in range(2):
        for n in range(7):
            kv_copy(n, hd).wait_send()
    for kind in range(3):
        for stage in range(4):
            weight_copy(kind, stage).wait_send()
    forwarded = [j for j, _ in EARLY_FORWARD]
    second = [j for j, _ in EARLY_SECOND]
    for j in range(N_EARLY):
        if j not in forwarded:
            net.arrived(0, j)
        net.sent(0, j)
    for j in forwarded:
        if j not in second:
            net.arrived(1, j)
        net.arrived(2, j)
        net.sent(1, j)
        net.sent(2, j)
    for j in second:
        net.arrived(3, j)
        net.sent(3, j)


def attention(x, gain, cos2, sin2, wq, wkv, wo, w1, w3, w2):
    rows, dim = x.shape
    width = wq.shape[1]
    states = 2 * rows // Q_ROWS
    m_rows = width // 128 // 2 * Q_ROWS
    vm = pl.BlockSpec(memory_space=pltpu.VMEM)
    hbm = pl.BlockSpec(memory_space=pl.ANY)
    bf16 = jnp.bfloat16
    n = N_EARLY
    return pl.pallas_call(
        attention_kernel,
        in_specs=[vm] * 6 + [hbm] * 4,
        out_specs=[vm, vm, vm, hbm, hbm, hbm, hbm],
        out_shape=[
            jax.ShapeDtypeStruct((2, rows, width), bf16),
            jax.ShapeDtypeStruct((2 * rows, 128), bf16),
            jax.ShapeDtypeStruct((2 * rows, 128), bf16),
            jax.ShapeDtypeStruct(wo.shape, bf16),
            jax.ShapeDtypeStruct((N_CHUNKS, 4, dim, TILE), bf16),
            jax.ShapeDtypeStruct((N_CHUNKS, 4, dim, TILE), bf16),
            jax.ShapeDtypeStruct((N_CHUNKS, 4, TILE, dim), bf16),
        ],
        scratch_shapes=[
            pltpu.VMEM((rows, dim), bf16),
            pltpu.VMEM((2, rows, width), bf16),
            pltpu.VMEM(wq.shape, bf16),
            pltpu.VMEM(wkv.shape, bf16),
            pltpu.VMEM((8, 2, 2, rows, 128), bf16),
            pltpu.VMEM((states, 2, m_rows, 128), jnp.float32),
            pltpu.VMEM((states, 2, m_rows, 128), jnp.float32),
            pltpu.VMEM((states, 2, m_rows, 128), jnp.float32),
            pltpu.SemaphoreType.DMA((n, 4, 3)),
            pltpu.SemaphoreType.DMA((n, 4, 3)),
            pltpu.SemaphoreType.DMA((7, 2)),
            pltpu.SemaphoreType.DMA((7, 2)),
            pltpu.SemaphoreType.DMA((3, 4)),
            pltpu.SemaphoreType.DMA((3, 4)),
        ],
        compiler_params=pltpu.CompilerParams(collective_id=0, has_side_effects=True, vmem_limit_bytes=VMEM_LIMIT),
        cost_estimate=pl.CostEstimate(flops=16 * rows * 4096 * width, bytes_accessed=32 * 2**20, transcendentals=rows * 4096 * 12),
        name="attention",
    )(x, gain, cos2, sin2, wq, wkv, wo, w1, w3, w2)


M_BLOCK = 512
LATE_FORWARD = {0: (4,), 4: (5,), 8: (6,)}
LATE_SECOND = {0: (3,), 4: (4,), 8: (5,)}
END_FORWARD = {12: (7,), 15: (8,)}
END_SECOND = {12: (6,), 15: (7,), 16: (8,)}
LOAD_AFTER = 12


def mlp_kernel(x_ref, gain_ref, o_ref, wo_ref, ro_ref, w1_ref, w3_ref, w2_ref, a1_ref, a3_ref, a2_ref, out_ref, r1_ref, r3_ref, r2_ref,
               w1_sc, w3_sc, w2_sc, b_ref, acc_sc, load_sems, send_sems, recv_sems):
    dim = x_ref.shape[1]
    width = 4 * TILE
    n_tiles = w1_ref.shape[1] // TILE
    net = Links((w1_ref, w3_ref, w2_ref), (r1_ref, r3_ref, r2_ref), send_sems, recv_sems, n_tiles)
    own_last = (n_tiles - 4) * TILE

    def own_loads(j, slot):
        off = min(j * width, own_last) if isinstance(j, int) else pl.multiple_of(jnp.minimum(j * width, own_last), TILE)
        sl = pl.ds(off, width)
        return [
            pltpu.make_async_copy(w1_ref.at[:, sl], w1_sc.at[slot], load_sems.at[slot, 0]),
            pltpu.make_async_copy(w3_ref.at[:, sl], w3_sc.at[slot], load_sems.at[slot, 1]),
            pltpu.make_async_copy(w2_ref.at[sl, :], w2_sc.at[slot], load_sems.at[slot, 2]),
        ]

    def other_loads(j, slot):
        copies = []
        for p in range(4):
            sl = pl.ds(p * TILE, TILE)
            copies.append(pltpu.make_async_copy(r1_ref.at[j, p], w1_sc.at[slot, :, sl], load_sems.at[slot, 0]))
            copies.append(pltpu.make_async_copy(r3_ref.at[j, p], w3_sc.at[slot, :, sl], load_sems.at[slot, 1]))
            copies.append(pltpu.make_async_copy(r2_ref.at[j, p], w2_sc.at[slot, sl, :], load_sems.at[slot, 2]))
        return copies

    def compute(slot, lane_keep):
        def rows_step(m, carry):
            sl = pl.ds(pl.multiple_of(m * M_BLOCK, M_BLOCK), M_BLOCK)
            b = b_ref[sl, :]
            gate = jnp.dot(b, w1_sc[slot], preferred_element_type=jnp.float32)
            up = jnp.dot(b, w3_sc[slot], preferred_element_type=jnp.float32)
            hidden = jax.nn.silu(gate) * up
            hidden = jnp.where(lane_keep > 0.5, hidden, 0.0).astype(jnp.bfloat16)
            acc_sc[sl, :] += jnp.dot(hidden, w2_sc[slot], preferred_element_type=jnp.float32)
            return carry

        lax.fori_loop(0, b_ref.shape[0] // M_BLOCK, rows_step, 0)

    net.barrier()
    net.start(0, N_EARLY)
    net.start(0, N_EARLY + 1)
    for copy in own_loads(0, 0):
        copy.start()

    def residual_rows(i, carry):
        sl = pl.ds(pl.multiple_of(i * Q_ROWS, Q_ROWS), Q_ROWS)
        attn = jnp.dot(o_ref[0, sl, :], wo_ref[...], preferred_element_type=jnp.float32)
        attn = attn + jnp.dot(o_ref[1, sl, :], ro_ref[...], preferred_element_type=jnp.float32)
        residual = (x_ref[sl, :].astype(jnp.float32) + attn).astype(jnp.bfloat16).astype(jnp.float32)
        acc_sc[sl, :] = residual
        b_ref[sl, :] = normed_rows(residual, gain_ref[...].astype(jnp.float32))
        return carry

    lax.fori_loop(0, x_ref.shape[0] // Q_ROWS, residual_rows, 0)
    lane_tile = lax.broadcasted_iota(jnp.int32, (1, width), 1) // TILE
    source = 2 * lax.rem(lane_tile + net.c // 2, 2) + lax.rem(lane_tile // 2 + lax.rem(net.c, 2), 2)

    def pass_on(s, forward, second):
        for when, chunks in forward.items():
            @pl.when(s == when)
            def _(chunks=chunks):
                for j in chunks:
                    if j >= N_EARLY:
                        net.arrived(0, j)
                    net.start(1, j)
                    net.start(2, j)
                    if N_EARLY + 2 <= j + 2 < N_CHUNKS:
                        net.start(0, j + 2)
        for when, chunks in second.items():
            @pl.when(s == when)
            def _(chunks=chunks):
                for j in chunks:
                    if j >= 4:
                        net.arrived(1, j)
                    net.start(3, j)

    def load_next(s, slot, after):
        for j in range(3, N_CHUNKS):
            if (N_CHUNKS - 1 + j >= LOAD_AFTER) == after:
                @pl.when(s == N_CHUNKS - 1 + j)
                def _(j=j):
                    if j >= 4:
                        net.arrived(2, j)
                    net.arrived(3, j)

        if not after:
            @pl.when(s + 1 < N_CHUNKS)
            def _():
                for copy in own_loads(s + 1, 1 - slot):
                    copy.start()

        first, last = (LOAD_AFTER, 2 * N_CHUNKS - 1) if after else (N_CHUNKS - 1, LOAD_AFTER)

        @pl.when((s >= first) & (s < last))
        def _():
            for copy in other_loads(s + 1 - N_CHUNKS, 1 - slot):
                copy.start()

    def step(s, carry):
        slot = lax.rem(s, 2)
        pass_on(s, LATE_FORWARD, LATE_SECOND)
        load_next(s, slot, False)
        for copy in own_loads(0, slot):
            copy.wait()
        own_end = (s == N_CHUNKS - 1).astype(jnp.float32)
        other_end = (s == 2 * N_CHUNKS - 1).astype(jnp.float32)
        keep = 1.0 - own_end * (lane_tile == 0).astype(jnp.float32) - other_end * (source == 3).astype(jnp.float32)
        compute(slot, keep)
        pass_on(s, END_FORWARD, END_SECOND)
        load_next(s, slot, True)
        return carry

    lax.fori_loop(0, 2 * N_CHUNKS, step, 0)
    out_ref[...] = acc_sc[...].astype(out_ref.dtype)
    for j in range(N_EARLY, N_CHUNKS):
        net.sent(0, j)
    for j in range(4, N_CHUNKS):
        net.sent(1, j)
        net.sent(2, j)
    for j in range(3, N_CHUNKS):
        net.sent(3, j)


def mlp(x, gain, o, wo, ro, w1, w3, w2, early):
    rows, dim = x.shape
    vm = pl.BlockSpec(memory_space=pltpu.VMEM)
    hbm = pl.BlockSpec(memory_space=pl.ANY)
    bf16 = jnp.bfloat16
    width = 4 * TILE
    n = N_CHUNKS
    return pl.pallas_call(
        mlp_kernel,
        in_specs=[vm] * 5 + [hbm] * 6,
        out_specs=[vm, hbm, hbm, hbm],
        out_shape=[jax.ShapeDtypeStruct((rows, dim), bf16)] + [jax.ShapeDtypeStruct(a.shape, bf16) for a in early],
        input_output_aliases={8: 1, 9: 2, 10: 3},
        scratch_shapes=[
            pltpu.VMEM((2, dim, width), bf16),
            pltpu.VMEM((2, dim, width), bf16),
            pltpu.VMEM((2, width, dim), bf16),
            pltpu.VMEM((rows, dim), bf16),
            pltpu.VMEM((rows, dim), jnp.float32),
            pltpu.SemaphoreType.DMA((2, 3)),
            pltpu.SemaphoreType.DMA((n, 4, 3)),
            pltpu.SemaphoreType.DMA((n, 4, 3)),
        ],
        compiler_params=pltpu.CompilerParams(collective_id=1, has_side_effects=True, vmem_limit_bytes=VMEM_LIMIT),
        cost_estimate=pl.CostEstimate(flops=12 * rows * dim * w1.shape[1], bytes_accessed=12 * dim * w1.shape[1], transcendentals=2 * rows * w1.shape[1]),
        name="mlp",
    )(x, gain, o, wo, ro, w1, w3, w2, *early)[0]

def solution(mesh):
    n_pieces = 2 * mesh.shape["cp"]

    def layer_shard(x_loc, norm_attn, norm_mlp, w_query, w_key, w_value, w_out, w_gate, w_up, w_down):
        tok_dev, dim = x_loc.shape
        local_q, head_dim = w_query.shape[1], w_query.shape[2]
        cp_index = lax.axis_index("cp")
        piece = jnp.where(lax.axis_index("tp") == 0, cp_index, n_pieces - 1 - cp_index)
        cosine, sine_tab = rope_tables(piece * tok_dev + jnp.arange(tok_dev, dtype=jnp.int32), head_dim)
        cos2 = jnp.concatenate([cosine, cosine], axis=1)
        sin2 = jnp.concatenate([-sine_tab, sine_tab], axis=1)
        wq = w_query.reshape(dim, local_q * head_dim)
        wkv = jnp.concatenate([w_key.reshape(dim, -1), w_value.reshape(dim, -1)], axis=1)
        wo = w_out.reshape(local_q * head_dim, dim)
        o, k_cache, v_cache, wo_other, *early = attention(x_loc, norm_attn[None], cos2, sin2, wq, wkv, wo, w_gate, w_up, w_down)
        layer_out = mlp(x_loc, norm_mlp[None], o, wo, wo_other, w_gate, w_up, w_down, early)
        return layer_out, k_cache, v_cache

    row_spec = P(("dp", "cp", "tp"), None)
    cache_spec = P(("dp", "cp"), "tp")
    head_spec = P(None, "tp", None)
    return jax.shard_map(
        layer_shard,
        mesh=mesh,
        in_specs=(row_spec, P(None), P(None), head_spec, head_spec, head_spec, P("tp", None, None), P(None, "tp"), P(None, "tp"), P("tp", None)),
        out_specs=(row_spec, cache_spec, cache_spec),
        check_vma=False,
    )
```

```python
import functools

import jax
import jax.numpy as jnp
from jax import lax
from jax.experimental import pallas as pl
from jax.experimental.pallas import tpu as pltpu
from jax.sharding import PartitionSpec as P

ROPE_BASE = 500000.0
NORM_EPS = 1e-5
MASK_VALUE = -1e30
LOG2E = 1.4426950408889634
VMEM_LIMIT = 60 * 1024 * 1024
Q_ROWS = 256
K_ROWS = 512
MESH = pl.DeviceIdType.MESH
TILE = 128
N_CHUNKS = 9
N_EARLY = 9


def rope_tables(positions, head_dim):
    half_dim = head_dim // 2
    inv_freq = ROPE_BASE ** (-2.0 * jnp.arange(half_dim, dtype=jnp.float32) / head_dim)
    angles = positions.astype(jnp.float32)[:, None] * inv_freq[None, :]
    return jnp.cos(angles), jnp.sin(angles)


class Links:
    def __init__(self, weights, recv, send_sems, recv_sems, n_tiles):
        self.y, self.c = lax.axis_index("tp"), lax.axis_index("cp")
        self.peer = {
            "y": {"tp": 1 - self.y},
            "x": {"cp": lax.rem(self.c + 2, 4)},
            "d": {"cp": self.c + 1 - 2 * lax.rem(self.c, 2)},
        }
        self.weights, self.recv, self.send_sems, self.recv_sems = weights, recv, send_sems, recv_sems
        self.n_tiles = n_tiles
        self.started = []

    def barrier(self):
        sem = pltpu.get_barrier_semaphore()
        for name in "yxd":
            pl.semaphore_signal(sem, inc=1, device_id=self.peer[name], device_id_type=MESH)
        pl.semaphore_wait(sem, 3)

    def remote(self, src, dst, ssem, rsem, to):
        return pltpu.make_async_remote_copy(src_ref=src, dst_ref=dst, send_sem=ssem, recv_sem=rsem, device_id=self.peer[to], device_id_type=MESH)

    def chunk(self, stage, j):
        to = "yxdd"[stage]
        copies = []
        for a in range(3):
            if stage == 0:
                tile = jnp.minimum(4 * j + self.c, self.n_tiles - 1)
                sl = pl.ds(pl.multiple_of(tile * TILE, TILE), TILE)
                src = self.weights[a].at[sl, :] if a == 2 else self.weights[a].at[:, sl]
            else:
                src = self.recv[a].at[j, (0, 0, 0, 1)[stage]]
            copies.append(self.remote(src, self.recv[a].at[j, stage], self.send_sems.at[j, stage, a], self.recv_sems.at[j, stage, a], to))
        return copies

    def start(self, stage, j):
        for copy in self.chunk(stage, j):
            copy.start()

    def arrived(self, stage, j):
        for copy in self.chunk(stage, j):
            copy.wait_recv()

    def sent(self, stage, j):
        for copy in self.chunk(stage, j):
            copy.wait_send()


EARLY_FORWARD = ((0, 14), (1, 17), (2, 19), (3, 21))
EARLY_SECOND = ((0, 18), (1, 20), (2, 22))
SLOT_SOURCE = (0, 0, 0, 1)


def normed_rows(wide, gain):
    inv_rms = lax.rsqrt(jnp.mean(wide * wide, axis=-1, keepdims=True) + NORM_EPS)
    return (wide * inv_rms * gain).astype(jnp.bfloat16)


def attention_kernel(x_ref, gain_ref, cos_ref, sin_ref, wq_ref, wkv_ref, wo_ref, w1_ref, w3_ref, w2_ref,
                     o_ref, kc_ref, vc_ref, ro_ref, r1_ref, r3_ref, r2_ref,
                     a_sc, q_sc, wq_sc, wkv_sc, kv_buf, m_sc, l_sc, acc_sc, send_sems, recv_sems, kv_send, kv_recv, wt_send, wt_recv):
    head_dim = 128
    half_dim = head_dim // 2
    chunk_len = x_ref.shape[0]
    width = wq_ref.shape[1]
    heads = width // head_dim
    chains = 2
    per_chain = heads // chains
    rows = per_chain * Q_ROWS
    q_blocks = chunk_len // Q_ROWS
    coef = head_dim ** -0.5 * LOG2E
    net = Links((w1_ref, w3_ref, w2_ref), (r1_ref, r3_ref, r2_ref), send_sems, recv_sems, w1_ref.shape[1] // TILE)
    y, c = net.y, net.c
    core_lower = lax.rem(c + y, 2)
    chip_lower = lax.rem(c // 2 + y, 2)
    other_chip = lax.rem(c + 2, 4)

    def kv_copy(n, hd):
        src, dst, to = ((0, 1, "x"), (0, 2, "d"), (1, 3, "d"), (0, 4, "y"), (4, 5, "x"), (4, 6, "d"), (5, 7, "d"))[n]
        return net.remote(kv_buf.at[src, hd], kv_buf.at[dst, hd], kv_send.at[n, hd], kv_recv.at[n, hd], to)

    def weight_copy(kind, stage):
        own, held = ((wkv_ref, wkv_sc), (wq_ref, wq_sc), (wo_ref, ro_ref))[kind]
        quarter = own.shape[0] // 4
        sl = pl.ds(pl.multiple_of((other_chip if stage == 3 else c) * quarter, 64), quarter)
        src = own if stage == 0 else held
        return net.remote(src.at[sl, :], held.at[sl, :], wt_send.at[kind, stage], wt_recv.at[kind, stage], "yxdd"[stage])

    def row_slice(i):
        return pl.ds(pl.multiple_of(i * Q_ROWS, Q_ROWS), Q_ROWS)

    def rope(t, sl):
        return (t * cos_ref[sl, :] + pltpu.roll(t, half_dim, 1) * sin_ref[sl, :]).astype(jnp.bfloat16)

    def norm_x():
        def body(i, carry):
            sl = row_slice(i)
            a_sc[sl, :] = normed_rows(x_ref[sl, :].astype(jnp.float32), gain_ref[...].astype(jnp.float32))
            return carry
        lax.fori_loop(0, q_blocks, body, 0)

    def make_kv(w_ref, hd):
        def body(i, carry):
            sl = row_slice(i)
            proj = jnp.dot(a_sc[sl, :], w_ref[...], preferred_element_type=jnp.float32)
            kv_buf[0, hd, 0, sl, :] = rope(proj[:, :head_dim], sl)
            kv_buf[0, hd, 1, sl, :] = proj[:, head_dim:].astype(jnp.bfloat16)
            return carry
        lax.fori_loop(0, q_blocks, body, 0)

    def make_q(w_ref, hd):
        def body(i, carry):
            sl = row_slice(i)
            proj = jnp.dot(a_sc[sl, :], w_ref[...], preferred_element_type=jnp.float32)
            for h in range(heads):
                cols = slice(h * head_dim, (h + 1) * head_dim)
                q_sc[hd, sl, cols] = rope(proj[:, cols], sl)
            return carry
        lax.fori_loop(0, q_blocks, body, 0)

    net.barrier()
    weight_copy(0, 0).start()
    weight_copy(1, 0).start()
    norm_x()
    make_kv(wkv_ref, 0)
    m_sc[...] = jnp.full_like(m_sc, MASK_VALUE)
    l_sc[...] = jnp.zeros_like(l_sc)
    acc_sc[...] = jnp.zeros_like(acc_sc)
    weight_copy(0, 0).wait_recv()
    weight_copy(0, 1).start()
    weight_copy(0, 2).start()
    kv_copy(1, 0).start()
    kv_copy(0, 0).start()
    kv_copy(3, 0).start()
    make_q(wq_ref, 0)

    def block(q_parts, state, start, slot, head, off, masked):
        k_blk = kv_buf[slot, head, 0, pl.ds(off, K_ROWS), :]
        v_blk = kv_buf[slot, head, 1, pl.ds(off, K_ROWS), :]
        for a in range(chains):
            s = lax.dot_general(q_parts[a], k_blk, (((1,), (1,)), ((), ())), preferred_element_type=jnp.float32)
            if masked:
                q_pos = start + lax.rem(lax.broadcasted_iota(jnp.int32, (rows, K_ROWS), 0), Q_ROWS)
                k_pos = off + lax.broadcasted_iota(jnp.int32, (rows, K_ROWS), 1)
                s = jnp.where(k_pos <= q_pos, s, MASK_VALUE)
            m_prev = m_sc[state, a]
            m_new = jnp.maximum(m_prev, jnp.max(s, axis=1, keepdims=True))
            alpha = jnp.exp2((m_prev - m_new) * coef)
            mc = m_new * coef
            sums = l_sc[state, a] * alpha
            p_tiles = []
            for j in range(K_ROWS // 128):
                p = jnp.exp2(s[:, j * 128:(j + 1) * 128] * coef - mc)
                sums = sums + p
                p_tiles.append(p.astype(jnp.bfloat16))
            l_sc[state, a] = sums
            m_sc[state, a] = m_new
            p_all = jnp.concatenate(p_tiles, axis=1)
            acc_sc[state, a] = acc_sc[state, a] * alpha + jnp.dot(p_all, v_blk, preferred_element_type=jnp.float32)

    def load_q(head, qb):
        sl = row_slice(qb)
        return [jnp.concatenate([q_sc[head, sl, (a * per_chain + h) * head_dim:(a * per_chain + h + 1) * head_dim] for h in range(per_chain)], axis=0) for a in range(chains)]

    per_piece = chunk_len // K_ROWS

    def step(s, carry):
        phase = s // q_blocks
        qb = lax.rem(s, q_blocks)
        is_last = phase // 4
        is_mid = (1 - is_last) * lax.rem(phase, 2)
        is_first = 1 - is_last - is_mid
        head = (1 - is_last) * (phase // 2) + is_last * (phase - 4)
        state = head * q_blocks + qb

        @pl.when(s == 0)
        def _():
            kv_copy(1, 0).wait_recv()

        @pl.when(s == 1)
        def _():
            weight_copy(0, 1).wait_recv()
            weight_copy(0, 3).start()

        @pl.when(s == 2)
        def _():
            weight_copy(0, 2).wait_recv()
            weight_copy(0, 3).wait_recv()
            make_kv(wkv_sc, 1)
            weight_copy(1, 0).wait_recv()
            weight_copy(1, 1).start()
            weight_copy(1, 2).start()

        @pl.when(s == 3)
        def _():
            kv_copy(1, 1).start()
            kv_copy(0, 1).start()
            kv_copy(3, 1).start()
            weight_copy(2, 0).start()
            net.start(0, 0)
            net.start(0, 1)
            kv_copy(0, 0).wait_recv()
            kv_copy(2, 0).start()

        @pl.when(s == 4)
        def _():
            kv_copy(2, 0).wait_recv()

        @pl.when(s == 6)
        def _():
            weight_copy(1, 1).wait_recv()
            weight_copy(1, 3).start()
            kv_copy(3, 0).wait_recv()
            kv_copy(4, 0).start()
            kv_copy(5, 0).start()

        @pl.when(s == 7)
        def _():
            weight_copy(1, 2).wait_recv()
            weight_copy(1, 3).wait_recv()
            make_q(wq_sc, 1)

        @pl.when(s == 8)
        def _():
            kv_copy(1, 1).wait_recv()

        @pl.when(s == 9)
        def _():
            kv_copy(0, 1).wait_recv()
            kv_copy(2, 1).start()

        @pl.when(s == 10)
        def _():
            kv_copy(3, 1).wait_recv()
            kv_copy(4, 1).start()
            kv_copy(5, 1).start()

        @pl.when(s == 12)
        def _():
            kv_copy(2, 1).wait_recv()
            weight_copy(2, 0).wait_recv()
            weight_copy(2, 1).start()
            weight_copy(2, 2).start()

        @pl.when(s == 13)
        def _():
            kv_copy(4, 0).wait_recv()
            kv_copy(6, 0).start()

        @pl.when(s == 14)
        def _():
            kv_copy(4, 1).wait_recv()
            kv_copy(6, 1).start()

        @pl.when(s == 16)
        def _():
            for hd in range(2):
                kv_copy(5, hd).wait_recv()
                kv_copy(6, hd).wait_recv()
            weight_copy(2, 1).wait_recv()
            weight_copy(2, 3).start()

        for j, when in EARLY_FORWARD:
            @pl.when(s == when)
            def _(j=j):
                net.arrived(0, j)
                net.start(1, j)
                net.start(2, j)
                if j + 2 < N_EARLY:
                    net.start(0, j + 2)

        for j, when in EARLY_SECOND:
            @pl.when(s == when)
            def _(j=j):
                net.arrived(1, j)
                net.start(3, j)

        q_parts = load_q(head, qb)
        start = qb * Q_ROWS
        diag = start // K_ROWS
        count = is_first * (diag + per_piece * core_lower) + is_mid * 2 * per_piece * chip_lower + is_last * 4 * per_piece * y
        kv_head = head + is_last * (1 - 2 * head)

        def inner(i, carry):
            in_core = (i >= diag).astype(jnp.int32)
            idx = i - is_first * in_core * diag
            slot = is_first * 2 * in_core + is_mid * (1 + 2 * (i // per_piece)) + is_last * (4 + i // per_piece)
            off = (is_first * (in_core * lax.rem(idx, per_piece) + (1 - in_core) * i) + (1 - is_first) * lax.rem(i, per_piece)) * K_ROWS
            block(q_parts, state, start, slot, kv_head, pl.multiple_of(off, K_ROWS), False)
            return carry

        lax.fori_loop(0, count, inner, 0)

        @pl.when(is_first == 1)
        def _():
            block(q_parts, state, start, 0, head, pl.multiple_of(diag * K_ROWS, K_ROWS), True)

        return carry

    lax.fori_loop(0, 6 * q_blocks, step, 0)

    def finish(state, carry):
        head = state // q_blocks
        sl = row_slice(lax.rem(state, q_blocks))
        for a in range(chains):
            total = jnp.sum(l_sc[state, a], axis=1, keepdims=True)
            out = (acc_sc[state, a] / total).astype(jnp.bfloat16)
            for h in range(per_chain):
                o_ref[head, sl, (a * per_chain + h) * head_dim:(a * per_chain + h + 1) * head_dim] = out[h * Q_ROWS:(h + 1) * Q_ROWS]
        return carry

    lax.fori_loop(0, 2 * q_blocks, finish, 0)

    for e in range(2):
        late = c // 2
        owner = (1 - late) * (2 * c + e) + late * (7 - 2 * c - e)
        cross = lax.rem(late + y, 2)
        slot = 4 * cross + 2 * lax.rem(owner + c, 2) + lax.rem(owner // 2 + c // 2, 2)
        kc_ref[e * chunk_len:(e + 1) * chunk_len] = kv_buf[slot, cross, 0]
        vc_ref[e * chunk_len:(e + 1) * chunk_len] = kv_buf[slot, cross, 1]

    weight_copy(2, 2).wait_recv()
    weight_copy(2, 3).wait_recv()
    for hd in range(2):
        for n in range(7):
            kv_copy(n, hd).wait_send()
    for kind in range(3):
        for stage in range(4):
            weight_copy(kind, stage).wait_send()
    for j in range(4, N_CHUNKS):
        net.arrived(0, j)
        net.start(1, j)
        net.start(2, j)
        if j + 2 < N_CHUNKS:
            net.start(0, j + 2)
        net.arrived(1, j - 1)
        net.start(3, j - 1)
    net.arrived(1, N_CHUNKS - 1)
    net.start(3, N_CHUNKS - 1)
    for j in range(N_CHUNKS):
        net.arrived(2, j)
        net.arrived(3, j)
        for stage in range(4):
            net.sent(stage, j)


def attention(x, gain, cos2, sin2, wq, wkv, wo, w1, w3, w2):
    rows, dim = x.shape
    width = wq.shape[1]
    states = 2 * rows // Q_ROWS
    m_rows = width // 128 // 2 * Q_ROWS
    vm = pl.BlockSpec(memory_space=pltpu.VMEM)
    hbm = pl.BlockSpec(memory_space=pl.ANY)
    bf16 = jnp.bfloat16
    n = N_EARLY
    return pl.pallas_call(
        attention_kernel,
        in_specs=[vm] * 6 + [hbm] * 4,
        out_specs=[vm, vm, vm, hbm, hbm, hbm, hbm],
        out_shape=[
            jax.ShapeDtypeStruct((2, rows, width), bf16),
            jax.ShapeDtypeStruct((2 * rows, 128), bf16),
            jax.ShapeDtypeStruct((2 * rows, 128), bf16),
            jax.ShapeDtypeStruct(wo.shape, bf16),
            jax.ShapeDtypeStruct((N_CHUNKS, 4, dim, TILE), bf16),
            jax.ShapeDtypeStruct((N_CHUNKS, 4, dim, TILE), bf16),
            jax.ShapeDtypeStruct((N_CHUNKS, 4, TILE, dim), bf16),
        ],
        scratch_shapes=[
            pltpu.VMEM((rows, dim), bf16),
            pltpu.VMEM((2, rows, width), bf16),
            pltpu.VMEM(wq.shape, bf16),
            pltpu.VMEM(wkv.shape, bf16),
            pltpu.VMEM((8, 2, 2, rows, 128), bf16),
            pltpu.VMEM((states, 2, m_rows, 128), jnp.float32),
            pltpu.VMEM((states, 2, m_rows, 128), jnp.float32),
            pltpu.VMEM((states, 2, m_rows, 128), jnp.float32),
            pltpu.SemaphoreType.DMA((n, 4, 3)),
            pltpu.SemaphoreType.DMA((n, 4, 3)),
            pltpu.SemaphoreType.DMA((7, 2)),
            pltpu.SemaphoreType.DMA((7, 2)),
            pltpu.SemaphoreType.DMA((3, 4)),
            pltpu.SemaphoreType.DMA((3, 4)),
        ],
        compiler_params=pltpu.CompilerParams(collective_id=0, has_side_effects=True, vmem_limit_bytes=VMEM_LIMIT),
        cost_estimate=pl.CostEstimate(flops=16 * rows * 4096 * width, bytes_accessed=32 * 2**20, transcendentals=rows * 4096 * 12),
        name="attention",
    )(x, gain, cos2, sin2, wq, wkv, wo, w1, w3, w2)


M_BLOCK = 512
LATE_FORWARD = {}
LATE_SECOND = {}
END_FORWARD = {}
END_SECOND = {}
LOAD_AFTER = 12


def mlp_kernel(x_ref, gain_ref, o_ref, wo_ref, ro_ref, w1_ref, w3_ref, w2_ref, a1_ref, a3_ref, a2_ref, out_ref, r1_ref, r3_ref, r2_ref,
               w1_sc, w3_sc, w2_sc, b_ref, acc_sc, load_sems, send_sems, recv_sems):
    dim = x_ref.shape[1]
    width = 4 * TILE
    n_tiles = w1_ref.shape[1] // TILE
    net = Links((w1_ref, w3_ref, w2_ref), (r1_ref, r3_ref, r2_ref), send_sems, recv_sems, n_tiles)
    own_last = (n_tiles - 4) * TILE

    def own_loads(j, slot):
        off = min(j * width, own_last) if isinstance(j, int) else pl.multiple_of(jnp.minimum(j * width, own_last), TILE)
        sl = pl.ds(off, width)
        return [
            pltpu.make_async_copy(w1_ref.at[:, sl], w1_sc.at[slot], load_sems.at[slot, 0]),
            pltpu.make_async_copy(w3_ref.at[:, sl], w3_sc.at[slot], load_sems.at[slot, 1]),
            pltpu.make_async_copy(w2_ref.at[sl, :], w2_sc.at[slot], load_sems.at[slot, 2]),
        ]

    def other_loads(j, slot):
        copies = []
        for p in range(4):
            sl = pl.ds(p * TILE, TILE)
            copies.append(pltpu.make_async_copy(r1_ref.at[j, p], w1_sc.at[slot, :, sl], load_sems.at[slot, 0]))
            copies.append(pltpu.make_async_copy(r3_ref.at[j, p], w3_sc.at[slot, :, sl], load_sems.at[slot, 1]))
            copies.append(pltpu.make_async_copy(r2_ref.at[j, p], w2_sc.at[slot, sl, :], load_sems.at[slot, 2]))
        return copies

    def compute(slot, lane_keep):
        def rows_step(m, carry):
            sl = pl.ds(pl.multiple_of(m * M_BLOCK, M_BLOCK), M_BLOCK)
            b = b_ref[sl, :]
            gate = jnp.dot(b, w1_sc[slot], preferred_element_type=jnp.float32)
            up = jnp.dot(b, w3_sc[slot], preferred_element_type=jnp.float32)
            hidden = jax.nn.silu(gate) * up
            hidden = jnp.where(lane_keep > 0.5, hidden, 0.0).astype(jnp.bfloat16)
            acc_sc[sl, :] += jnp.dot(hidden, w2_sc[slot], preferred_element_type=jnp.float32)
            return carry

        lax.fori_loop(0, b_ref.shape[0] // M_BLOCK, rows_step, 0)

    for copy in own_loads(0, 0):
        copy.start()

    def residual_rows(i, carry):
        sl = pl.ds(pl.multiple_of(i * Q_ROWS, Q_ROWS), Q_ROWS)
        attn = jnp.dot(o_ref[0, sl, :], wo_ref[...], preferred_element_type=jnp.float32)
        attn = attn + jnp.dot(o_ref[1, sl, :], ro_ref[...], preferred_element_type=jnp.float32)
        residual = (x_ref[sl, :].astype(jnp.float32) + attn).astype(jnp.bfloat16).astype(jnp.float32)
        acc_sc[sl, :] = residual
        b_ref[sl, :] = normed_rows(residual, gain_ref[...].astype(jnp.float32))
        return carry

    lax.fori_loop(0, x_ref.shape[0] // Q_ROWS, residual_rows, 0)
    lane_tile = lax.broadcasted_iota(jnp.int32, (1, width), 1) // TILE
    source = 2 * lax.rem(lane_tile + net.c // 2, 2) + lax.rem(lane_tile // 2 + lax.rem(net.c, 2), 2)

    def pass_on(s, forward, second):
        for when, chunks in forward.items():
            @pl.when(s == when)
            def _(chunks=chunks):
                for j in chunks:
                    if j >= N_EARLY:
                        net.arrived(0, j)
                    net.start(1, j)
                    net.start(2, j)
                    if N_EARLY + 2 <= j + 2 < N_CHUNKS:
                        net.start(0, j + 2)
        for when, chunks in second.items():
            @pl.when(s == when)
            def _(chunks=chunks):
                for j in chunks:
                    if j >= 4:
                        net.arrived(1, j)
                    net.start(3, j)

    def load_next(s, slot, after):
        for j in range(N_EARLY, N_CHUNKS):
            if (N_CHUNKS - 1 + j >= LOAD_AFTER) == after:
                @pl.when(s == N_CHUNKS - 1 + j)
                def _(j=j):
                    if j >= 4:
                        net.arrived(2, j)
                    net.arrived(3, j)

        if not after:
            @pl.when(s + 1 < N_CHUNKS)
            def _():
                for copy in own_loads(s + 1, 1 - slot):
                    copy.start()

        first, last = (LOAD_AFTER, 2 * N_CHUNKS - 1) if after else (N_CHUNKS - 1, LOAD_AFTER)

        @pl.when((s >= first) & (s < last))
        def _():
            for copy in other_loads(s + 1 - N_CHUNKS, 1 - slot):
                copy.start()

    def step(s, carry):
        slot = lax.rem(s, 2)
        pass_on(s, LATE_FORWARD, LATE_SECOND)
        load_next(s, slot, False)
        for copy in own_loads(0, slot):
            copy.wait()
        own_end = (s == N_CHUNKS - 1).astype(jnp.float32)
        other_end = (s == 2 * N_CHUNKS - 1).astype(jnp.float32)
        keep = 1.0 - own_end * (lane_tile == 0).astype(jnp.float32) - other_end * (source == 3).astype(jnp.float32)
        compute(slot, keep)
        pass_on(s, END_FORWARD, END_SECOND)
        load_next(s, slot, True)
        return carry

    lax.fori_loop(0, 2 * N_CHUNKS, step, 0)
    out_ref[...] = acc_sc[...].astype(out_ref.dtype)


def mlp(x, gain, o, wo, ro, w1, w3, w2, early):
    rows, dim = x.shape
    vm = pl.BlockSpec(memory_space=pltpu.VMEM)
    hbm = pl.BlockSpec(memory_space=pl.ANY)
    bf16 = jnp.bfloat16
    width = 4 * TILE
    n = N_CHUNKS
    return pl.pallas_call(
        mlp_kernel,
        in_specs=[vm] * 5 + [hbm] * 6,
        out_specs=[vm, hbm, hbm, hbm],
        out_shape=[jax.ShapeDtypeStruct((rows, dim), bf16)] + [jax.ShapeDtypeStruct(a.shape, bf16) for a in early],
        input_output_aliases={8: 1, 9: 2, 10: 3},
        scratch_shapes=[
            pltpu.VMEM((2, dim, width), bf16),
            pltpu.VMEM((2, dim, width), bf16),
            pltpu.VMEM((2, width, dim), bf16),
            pltpu.VMEM((rows, dim), bf16),
            pltpu.VMEM((rows, dim), jnp.float32),
            pltpu.SemaphoreType.DMA((2, 3)),
            pltpu.SemaphoreType.DMA((n, 4, 3)),
            pltpu.SemaphoreType.DMA((n, 4, 3)),
        ],
        compiler_params=pltpu.CompilerParams(vmem_limit_bytes=VMEM_LIMIT),
        cost_estimate=pl.CostEstimate(flops=12 * rows * dim * w1.shape[1], bytes_accessed=12 * dim * w1.shape[1], transcendentals=2 * rows * w1.shape[1]),
        name="mlp",
    )(x, gain, o, wo, ro, w1, w3, w2, *early)[0]

def solution(mesh):
    n_pieces = 2 * mesh.shape["cp"]

    def layer_shard(x_loc, norm_attn, norm_mlp, w_query, w_key, w_value, w_out, w_gate, w_up, w_down):
        tok_dev, dim = x_loc.shape
        local_q, head_dim = w_query.shape[1], w_query.shape[2]
        cp_index = lax.axis_index("cp")
        piece = jnp.where(lax.axis_index("tp") == 0, cp_index, n_pieces - 1 - cp_index)
        cosine, sine_tab = rope_tables(piece * tok_dev + jnp.arange(tok_dev, dtype=jnp.int32), head_dim)
        cos2 = jnp.concatenate([cosine, cosine], axis=1)
        sin2 = jnp.concatenate([-sine_tab, sine_tab], axis=1)
        wq = w_query.reshape(dim, local_q * head_dim)
        wkv = jnp.concatenate([w_key.reshape(dim, -1), w_value.reshape(dim, -1)], axis=1)
        wo = w_out.reshape(local_q * head_dim, dim)
        o, k_cache, v_cache, wo_other, *early = attention(x_loc, norm_attn[None], cos2, sin2, wq, wkv, wo, w_gate, w_up, w_down)
        layer_out = mlp(x_loc, norm_mlp[None], o, wo, wo_other, w_gate, w_up, w_down, early)
        return layer_out, k_cache, v_cache

    row_spec = P(("dp", "cp", "tp"), None)
    cache_spec = P(("dp", "cp"), "tp")
    head_spec = P(None, "tp", None)
    return jax.shard_map(
        layer_shard,
        mesh=mesh,
        in_specs=(row_spec, P(None), P(None), head_spec, head_spec, head_spec, P("tp", None, None), P(None, "tp"), P(None, "tp"), P("tp", None)),
        out_specs=(row_spec, cache_spec, cache_spec),
        check_vma=False,
    )
```

```python
import functools

import jax
import jax.numpy as jnp
from jax import lax
from jax.experimental import pallas as pl
from jax.experimental.pallas import tpu as pltpu
from jax.sharding import PartitionSpec as P

ROPE_BASE = 500000.0
NORM_EPS = 1e-5
MASK_VALUE = -1e30
LOG2E = 1.4426950408889634
VMEM_LIMIT = 60 * 1024 * 1024
Q_ROWS = 256
K_ROWS = 512
MESH = pl.DeviceIdType.MESH
TILE = 128
N_CHUNKS = 9
N_EARLY = 5


def rope_tables(positions, head_dim):
    half_dim = head_dim // 2
    lane = jnp.arange(head_dim, dtype=jnp.int32)
    inv_freq = ROPE_BASE ** (-2.0 * (lane % half_dim).astype(jnp.float32) / head_dim)
    angles = positions.astype(jnp.float32)[:, None] * inv_freq[None, :]
    sine_tab = jnp.sin(angles)
    return jnp.cos(angles), jnp.where(lane < half_dim, -sine_tab, sine_tab)


class Links:
    def __init__(self, weights, recv, send_sems, recv_sems, n_tiles):
        self.y, self.c = lax.axis_index("tp"), lax.axis_index("cp")
        self.peer = {
            "y": {"tp": 1 - self.y},
            "x": {"cp": lax.rem(self.c + 2, 4)},
            "d": {"cp": self.c + 1 - 2 * lax.rem(self.c, 2)},
        }
        self.weights, self.recv, self.send_sems, self.recv_sems = weights, recv, send_sems, recv_sems
        self.n_tiles = n_tiles
        self.started = []

    def barrier(self):
        sem = pltpu.get_barrier_semaphore()
        for name in "yxd":
            pl.semaphore_signal(sem, inc=1, device_id=self.peer[name], device_id_type=MESH)
        pl.semaphore_wait(sem, 3)

    def remote(self, src, dst, ssem, rsem, to):
        return pltpu.make_async_remote_copy(src_ref=src, dst_ref=dst, send_sem=ssem, recv_sem=rsem, device_id=self.peer[to], device_id_type=MESH)

    def chunk(self, stage, j):
        to = "yxdd"[stage]
        copies = []
        for a in range(3):
            if stage == 0:
                tile = 4 * j + self.c
                sl = pl.ds(pl.multiple_of(tile * TILE, TILE), TILE)
                src = self.weights[a].at[sl, :] if a == 2 else self.weights[a].at[:, sl]
            else:
                src = self.recv[a].at[j, (0, 0, 0, 1)[stage]]
            copies.append(self.remote(src, self.recv[a].at[j, stage], self.send_sems.at[j, stage, a], self.recv_sems.at[j, stage, a], to))
        return copies

    def last_chunk(self, stage, last):
        half = lax.rem(self.c, 2)
        begin = (self.n_tiles // 4) * 4 * TILE
        copies = []
        for a in range(3):
            depth = last[a].shape[0] // 2
            at = pl.ds(pl.multiple_of(half * depth, 64), depth)
            dst = last[a].at[at, :]
            if stage == 2:
                src = dst
            elif a == 2:
                src = self.weights[a].at[pl.ds(pl.multiple_of(begin + half * depth, 64), depth), :]
            else:
                src = self.weights[a].at[at, pl.ds(begin, last[a].shape[1])]
            j = N_CHUNKS - 1
            copies.append(self.remote(src, dst, self.send_sems.at[j, stage, a], self.recv_sems.at[j, stage, a], "y.d"[stage]))
        return copies

    def pass_on(self, j):
        for first, over_x, over_d in zip(self.chunk(0, j), self.chunk(1, j), self.chunk(2, j)):
            first.wait_recv()
            over_x.start()
            over_d.start()

    def pass_second(self, j):
        for first, over_d in zip(self.chunk(1, j), self.chunk(3, j)):
            first.wait_recv()
            over_d.start()

    def start(self, stage, j):
        for copy in self.chunk(stage, j):
            copy.start()

    def arrived(self, stage, j):
        for copy in self.chunk(stage, j):
            copy.wait_recv()

    def sent(self, stage, j):
        for copy in self.chunk(stage, j):
            copy.wait_send()


EARLY_FORWARD = ((0, 14), (1, 17), (2, 19), (3, 21))
EARLY_SECOND = ((0, 18), (1, 20), (2, 22))
SLOT_SOURCE = (0, 0, 0, 1)


def normed_rows(wide, gain):
    inv_rms = lax.rsqrt(jnp.mean(wide * wide, axis=-1, keepdims=True) + NORM_EPS)
    return (wide * inv_rms * gain).astype(jnp.bfloat16)


def attention_kernel(x_ref, gain_ref, cos_ref, sin_ref, wq_ref, wk_ref, wv_ref, wo_ref, w1_ref, w3_ref, w2_ref,
                     o_ref, kc_ref, vc_ref, ro_ref, r1_ref, r3_ref, r2_ref,
                     a_sc, q_sc, wq_sc, wk_sc, wv_sc, kv_buf, m_sc, l_sc, acc_sc, send_sems, recv_sems, kv_send, kv_recv, wt_send, wt_recv):
    head_dim = 128
    half_dim = head_dim // 2
    chunk_len = x_ref.shape[0]
    heads = wq_ref.shape[0]
    chains = 2
    per_chain = heads // chains
    rows = per_chain * Q_ROWS
    q_blocks = chunk_len // Q_ROWS
    coef = head_dim ** -0.5 * LOG2E
    net = Links((w1_ref, w3_ref, w2_ref), (r1_ref, r3_ref, r2_ref), send_sems, recv_sems, w1_ref.shape[1] // TILE)
    y, c = net.y, net.c
    core_lower = lax.rem(c + y, 2)
    chip_lower = lax.rem(c // 2 + y, 2)
    other_chip = lax.rem(c + 2, 4)

    def kv_copy(n, hd):
        src, dst, to = ((0, 1, "x"), (0, 2, "d"), (1, 3, "d"), (0, 4, "y"), (4, 5, "x"), (4, 6, "d"), (5, 7, "d"))[n]
        return net.remote(kv_buf.at[src, hd], kv_buf.at[dst, hd], kv_send.at[n, hd], kv_recv.at[n, hd], to)

    def weight_copy(kind, stage):
        own, held = ((wk_ref, wk_sc), (wv_ref, wv_sc), (wq_ref, wq_sc), (wo_ref, ro_ref))[kind]
        quarter = own.shape[-2] // 4
        sl = pl.ds(pl.multiple_of((other_chip if stage == 3 else c) * quarter, 64), quarter)
        src = own if stage == 0 else held
        pick = (lambda r: r.at[sl, :]) if kind == 3 else (lambda r: r.at[:, sl, :])
        return net.remote(pick(src), pick(held), wt_send.at[kind, stage], wt_recv.at[kind, stage], "yxdd"[stage])

    def weights_start(kinds, stage):
        for kind in kinds:
            weight_copy(kind, stage).start()

    def weights_arrived(kinds, stage):
        for kind in kinds:
            weight_copy(kind, stage).wait_recv()

    def row_slice(i):
        return pl.ds(pl.multiple_of(i * Q_ROWS, Q_ROWS), Q_ROWS)

    def rope(t, sl):
        return (t * cos_ref[sl, :] + pltpu.roll(t, half_dim, 1) * sin_ref[sl, :]).astype(jnp.bfloat16)

    def norm_x():
        def body(i, carry):
            sl = row_slice(i)
            a_sc[sl, :] = normed_rows(x_ref[sl, :].astype(jnp.float32), gain_ref[...].astype(jnp.float32)[None, :])
            return carry
        lax.fori_loop(0, q_blocks, body, 0)

    def make_kv(k_ref, v_ref, hd):
        def body(i, carry):
            sl = row_slice(i)
            w = jnp.concatenate([k_ref[0], v_ref[0]], axis=1)
            proj = jnp.dot(a_sc[sl, :], w, preferred_element_type=jnp.float32)
            kv_buf[0, hd, 0, sl, :] = rope(proj[:, :head_dim], sl)
            kv_buf[0, hd, 1, sl, :] = proj[:, head_dim:].astype(jnp.bfloat16)
            return carry
        lax.fori_loop(0, q_blocks, body, 0)

    def make_q(w_ref, hd):
        def body(i, carry):
            sl = row_slice(i)
            w = jnp.concatenate([w_ref[h] for h in range(heads)], axis=1)
            proj = jnp.dot(a_sc[sl, :], w, preferred_element_type=jnp.float32)
            for h in range(heads):
                cols = slice(h * head_dim, (h + 1) * head_dim)
                q_sc[hd, sl, cols] = rope(proj[:, cols], sl)
            return carry
        lax.fori_loop(0, q_blocks, body, 0)

    net.barrier()
    weights_start((0, 1, 2), 0)
    norm_x()
    make_kv(wk_ref, wv_ref, 0)
    m_sc[...] = jnp.full_like(m_sc, MASK_VALUE)
    l_sc[...] = jnp.zeros_like(l_sc)
    acc_sc[...] = jnp.zeros_like(acc_sc)
    weights_arrived((0, 1), 0)
    weights_start((0, 1), 1)
    weights_start((0, 1), 2)
    kv_copy(1, 0).start()
    kv_copy(0, 0).start()
    kv_copy(3, 0).start()
    make_q(wq_ref, 0)

    def block(q_parts, state, start, slot, head, off, masked):
        k_blk = kv_buf[slot, head, 0, pl.ds(off, K_ROWS), :]
        v_blk = kv_buf[slot, head, 1, pl.ds(off, K_ROWS), :]
        for a in range(chains):
            s = lax.dot_general(q_parts[a], k_blk, (((1,), (1,)), ((), ())), preferred_element_type=jnp.float32)
            if masked:
                q_pos = start + lax.rem(lax.broadcasted_iota(jnp.int32, (rows, K_ROWS), 0), Q_ROWS)
                k_pos = off + lax.broadcasted_iota(jnp.int32, (rows, K_ROWS), 1)
                s = jnp.where(k_pos <= q_pos, s, MASK_VALUE)
            m_prev = m_sc[state, a]
            m_new = jnp.maximum(m_prev, jnp.max(s, axis=1, keepdims=True))
            alpha = jnp.exp2((m_prev - m_new) * coef)
            mc = m_new * coef
            sums = l_sc[state, a] * alpha
            p_tiles = []
            for j in range(K_ROWS // 128):
                p = jnp.exp2(s[:, j * 128:(j + 1) * 128] * coef - mc)
                sums = sums + p
                p_tiles.append(p.astype(jnp.bfloat16))
            l_sc[state, a] = sums
            m_sc[state, a] = m_new
            p_all = jnp.concatenate(p_tiles, axis=1)
            acc_sc[state, a] = acc_sc[state, a] * alpha + jnp.dot(p_all, v_blk, preferred_element_type=jnp.float32)

    def load_q(head, qb):
        sl = row_slice(qb)
        return [jnp.concatenate([q_sc[head, sl, (a * per_chain + h) * head_dim:(a * per_chain + h + 1) * head_dim] for h in range(per_chain)], axis=0) for a in range(chains)]

    per_piece = chunk_len // K_ROWS

    def step(s, carry):
        phase = s // q_blocks
        qb = lax.rem(s, q_blocks)
        is_last = phase // 4
        is_mid = (1 - is_last) * lax.rem(phase, 2)
        is_first = 1 - is_last - is_mid
        head = (1 - is_last) * (phase // 2) + is_last * (phase - 4)
        state = head * q_blocks + qb

        @pl.when(s == 0)
        def _():
            kv_copy(1, 0).wait_recv()

        @pl.when(s == 1)
        def _():
            weights_arrived((0, 1), 1)
            weights_start((0, 1), 3)

        @pl.when(s == 2)
        def _():
            weights_arrived((0, 1), 2)
            weights_arrived((0, 1), 3)
            make_kv(wk_sc, wv_sc, 1)
            weights_arrived((2,), 0)
            weights_start((2,), 1)
            weights_start((2,), 2)

        @pl.when(s == 3)
        def _():
            kv_copy(1, 1).start()
            kv_copy(0, 1).start()
            kv_copy(3, 1).start()
            weights_start((3,), 0)
            net.start(0, 0)
            net.start(0, 1)
            kv_copy(0, 0).wait_recv()
            kv_copy(2, 0).start()

        @pl.when(s == 4)
        def _():
            kv_copy(2, 0).wait_recv()

        @pl.when(s == 6)
        def _():
            weights_arrived((2,), 1)
            weights_start((2,), 3)
            kv_copy(3, 0).wait_recv()
            kv_copy(4, 0).start()
            kv_copy(5, 0).start()

        @pl.when(s == 7)
        def _():
            weights_arrived((2,), 2)
            weights_arrived((2,), 3)
            make_q(wq_sc, 1)

        @pl.when(s == 8)
        def _():
            kv_copy(1, 1).wait_recv()

        @pl.when(s == 9)
        def _():
            kv_copy(0, 1).wait_recv()
            kv_copy(2, 1).start()

        @pl.when(s == 10)
        def _():
            kv_copy(3, 1).wait_recv()
            kv_copy(4, 1).start()
            kv_copy(5, 1).start()

        @pl.when(s == 12)
        def _():
            kv_copy(2, 1).wait_recv()
            weights_arrived((3,), 0)
            weights_start((3,), 1)
            weights_start((3,), 2)

        @pl.when(s == 13)
        def _():
            kv_copy(4, 0).wait_recv()
            kv_copy(6, 0).start()

        @pl.when(s == 14)
        def _():
            kv_copy(4, 1).wait_recv()
            kv_copy(6, 1).start()

        @pl.when(s == 16)
        def _():
            for hd in range(2):
                kv_copy(5, hd).wait_recv()
                kv_copy(6, hd).wait_recv()
            weights_arrived((3,), 1)
            weights_start((3,), 3)

        for j, when in EARLY_FORWARD:
            @pl.when(s == when)
            def _(j=j):
                net.pass_on(j)
                if j + 2 < N_EARLY:
                    net.start(0, j + 2)

        for j, when in EARLY_SECOND:
            @pl.when(s == when)
            def _(j=j):
                net.pass_second(j)

        q_parts = load_q(head, qb)
        start = qb * Q_ROWS
        diag = start // K_ROWS
        count = is_first * (diag + per_piece * core_lower) + is_mid * 2 * per_piece * chip_lower + is_last * 4 * per_piece * y
        kv_head = head + is_last * (1 - 2 * head)

        def inner(i, carry):
            in_core = (i >= diag).astype(jnp.int32)
            idx = i - is_first * in_core * diag
            slot = is_first * 2 * in_core + is_mid * (1 + 2 * (i // per_piece)) + is_last * (4 + i // per_piece)
            off = (is_first * (in_core * lax.rem(idx, per_piece) + (1 - in_core) * i) + (1 - is_first) * lax.rem(i, per_piece)) * K_ROWS
            block(q_parts, state, start, slot, kv_head, pl.multiple_of(off, K_ROWS), False)
            return carry

        lax.fori_loop(0, count, inner, 0)

        @pl.when(is_first == 1)
        def _():
            block(q_parts, state, start, 0, head, pl.multiple_of(diag * K_ROWS, K_ROWS), True)

        return carry

    lax.fori_loop(0, 6 * q_blocks, step, 0)

    def finish(state, carry):
        head = state // q_blocks
        sl = row_slice(lax.rem(state, q_blocks))
        for a in range(chains):
            total = jnp.sum(l_sc[state, a], axis=1, keepdims=True)
            out = (acc_sc[state, a] / total).astype(jnp.bfloat16)
            for h in range(per_chain):
                o_ref[head, sl, (a * per_chain + h) * head_dim:(a * per_chain + h + 1) * head_dim] = out[h * Q_ROWS:(h + 1) * Q_ROWS]
        return carry

    lax.fori_loop(0, 2 * q_blocks, finish, 0)

    for e in range(2):
        late = c // 2
        owner = (1 - late) * (2 * c + e) + late * (7 - 2 * c - e)
        cross = lax.rem(late + y, 2)
        slot = 4 * cross + 2 * lax.rem(owner + c, 2) + lax.rem(owner // 2 + c // 2, 2)
        kc_ref[e * chunk_len:(e + 1) * chunk_len] = kv_buf[slot, cross, 0]
        vc_ref[e * chunk_len:(e + 1) * chunk_len] = kv_buf[slot, cross, 1]

    weights_arrived((3,), 2)
    weights_arrived((3,), 3)
    for hd in range(2):
        for n in range(7):
            kv_copy(n, hd).wait_send()
    for kind in range(4):
        for stage in range(4):
            weight_copy(kind, stage).wait_send()
    forwarded = [j for j, _ in EARLY_FORWARD]
    second = [j for j, _ in EARLY_SECOND]
    for j in range(N_EARLY):
        if j not in forwarded:
            net.arrived(0, j)
        net.sent(0, j)
    for j in forwarded:
        if j not in second:
            net.arrived(1, j)
        net.arrived(2, j)
        net.sent(1, j)
        net.sent(2, j)
    for j in second:
        net.arrived(3, j)
        net.sent(3, j)


def attention(x, gain, cos2, sin2, wq, wk, wv, wo, w1, w3, w2):
    rows, dim = x.shape
    width = wq.shape[0] * 128
    states = 2 * rows // Q_ROWS
    m_rows = width // 128 // 2 * Q_ROWS
    vm = pl.BlockSpec(memory_space=pltpu.VMEM)
    hbm = pl.BlockSpec(memory_space=pl.ANY)
    bf16 = jnp.bfloat16
    n = N_EARLY
    return pl.pallas_call(
        attention_kernel,
        in_specs=[vm] * 7 + [hbm] * 4,
        out_specs=[vm, vm, vm, hbm, hbm, hbm, hbm],
        out_shape=[
            jax.ShapeDtypeStruct((2, rows, width), bf16),
            jax.ShapeDtypeStruct((2 * rows, 128), bf16),
            jax.ShapeDtypeStruct((2 * rows, 128), bf16),
            jax.ShapeDtypeStruct(wo.shape, bf16),
            jax.ShapeDtypeStruct((N_CHUNKS - 1, 4, dim, TILE), bf16),
            jax.ShapeDtypeStruct((N_CHUNKS - 1, 4, dim, TILE), bf16),
            jax.ShapeDtypeStruct((N_CHUNKS - 1, 4, TILE, dim), bf16),
        ],
        scratch_shapes=[
            pltpu.VMEM((rows, dim), bf16),
            pltpu.VMEM((2, rows, width), bf16),
            pltpu.VMEM(wq.shape, bf16),
            pltpu.VMEM(wk.shape, bf16),
            pltpu.VMEM(wv.shape, bf16),
            pltpu.VMEM((8, 2, 2, rows, 128), bf16),
            pltpu.VMEM((states, 2, m_rows, 128), jnp.float32),
            pltpu.VMEM((states, 2, m_rows, 128), jnp.float32),
            pltpu.VMEM((states, 2, m_rows, 128), jnp.float32),
            pltpu.SemaphoreType.DMA((n, 4, 3)),
            pltpu.SemaphoreType.DMA((n, 4, 3)),
            pltpu.SemaphoreType.DMA((7, 2)),
            pltpu.SemaphoreType.DMA((7, 2)),
            pltpu.SemaphoreType.DMA((4, 4)),
            pltpu.SemaphoreType.DMA((4, 4)),
        ],
        compiler_params=pltpu.CompilerParams(collective_id=0, has_side_effects=True, vmem_limit_bytes=VMEM_LIMIT),
        cost_estimate=pl.CostEstimate(flops=16 * rows * 4096 * width, bytes_accessed=32 * 2**20, transcendentals=rows * 4096 * 12),
        name="attention",
    )(x, gain, cos2, sin2, wq, wk, wv, wo, w1, w3, w2)


M_BLOCK = 512
LATE_FORWARD = {3: (5,), 7: (6,)}
LATE_SECOND = {3: (4,), 8: (5,)}
END_FORWARD = {12: (7,)}
END_SECOND = {12: (6,), 15: (7,)}
LOAD_AFTER = 12


def mlp_kernel(x_ref, gain_ref, o_ref, wo_ref, ro_ref, w1_ref, w3_ref, w2_ref, a1_ref, a3_ref, a2_ref, out_ref, r1_ref, r3_ref, r2_ref, e1_ref, e3_ref, e2_ref,
               w1_sc, w3_sc, w2_sc, b_ref, acc_sc, load_sems, send_sems, recv_sems):
    dim = x_ref.shape[1]
    width = 4 * TILE
    n_tiles = w1_ref.shape[1] // TILE
    net = Links((w1_ref, w3_ref, w2_ref), (r1_ref, r3_ref, r2_ref), send_sems, recv_sems, n_tiles)
    own_last = (n_tiles - 4) * TILE
    ends = (e1_ref, e3_ref, e2_ref)

    def own_loads(j, slot):
        off = min(j * width, own_last) if isinstance(j, int) else pl.multiple_of(jnp.minimum(j * width, own_last), TILE)
        sl = pl.ds(off, width)
        return [
            pltpu.make_async_copy(w1_ref.at[:, sl], w1_sc.at[slot], load_sems.at[slot, 0]),
            pltpu.make_async_copy(w3_ref.at[:, sl], w3_sc.at[slot], load_sems.at[slot, 1]),
            pltpu.make_async_copy(w2_ref.at[sl, :], w2_sc.at[slot], load_sems.at[slot, 2]),
        ]

    def other_loads(j, slot):
        copies = []
        for p in range(4):
            sl = pl.ds(p * TILE, TILE)
            copies.append(pltpu.make_async_copy(r1_ref.at[j, p], w1_sc.at[slot, :, sl], load_sems.at[slot, 0]))
            copies.append(pltpu.make_async_copy(r3_ref.at[j, p], w3_sc.at[slot, :, sl], load_sems.at[slot, 1]))
            copies.append(pltpu.make_async_copy(r2_ref.at[j, p], w2_sc.at[slot, sl, :], load_sems.at[slot, 2]))
        return copies

    def end_loads(slot):
        w = e1_ref.shape[1]
        return [
            pltpu.make_async_copy(e1_ref, w1_sc.at[slot, :, pl.ds(0, w)], load_sems.at[slot, 0]),
            pltpu.make_async_copy(e3_ref, w3_sc.at[slot, :, pl.ds(0, w)], load_sems.at[slot, 1]),
            pltpu.make_async_copy(e2_ref, w2_sc.at[slot, pl.ds(0, w), :], load_sems.at[slot, 2]),
        ]

    def compute(slot, lane_keep):
        def rows_step(m, carry):
            sl = pl.ds(pl.multiple_of(m * M_BLOCK, M_BLOCK), M_BLOCK)
            b = b_ref[sl, :]
            gate = jnp.dot(b, w1_sc[slot], preferred_element_type=jnp.float32)
            up = jnp.dot(b, w3_sc[slot], preferred_element_type=jnp.float32)
            hidden = jax.nn.silu(gate) * up
            hidden = jnp.where(lane_keep > 0.5, hidden, 0.0).astype(jnp.bfloat16)
            acc_sc[sl, :] += jnp.dot(hidden, w2_sc[slot], preferred_element_type=jnp.float32)
            return carry

        lax.fori_loop(0, b_ref.shape[0] // M_BLOCK, rows_step, 0)

    net.barrier()
    net.start(0, N_EARLY)
    net.start(0, N_EARLY + 1)
    net.start(1, N_EARLY - 1)
    net.start(2, N_EARLY - 1)
    net.start(3, N_EARLY - 2)
    for copy in own_loads(0, 0):
        copy.start()

    def residual_rows(i, carry):
        sl = pl.ds(pl.multiple_of(i * Q_ROWS, Q_ROWS), Q_ROWS)
        attn = jnp.dot(o_ref[0, sl, :], wo_ref[...], preferred_element_type=jnp.float32)
        attn = attn + jnp.dot(o_ref[1, sl, :], ro_ref[...], preferred_element_type=jnp.float32)
        residual = (x_ref[sl, :].astype(jnp.float32) + attn).astype(jnp.bfloat16).astype(jnp.float32)
        acc_sc[sl, :] = residual
        b_ref[sl, :] = normed_rows(residual, gain_ref[...].astype(jnp.float32)[None, :])
        return carry

    lax.fori_loop(0, x_ref.shape[0] // Q_ROWS, residual_rows, 0)
    lane_tile = lax.broadcasted_iota(jnp.int32, (1, width), 1) // TILE

    def pass_on(s, forward, second):
        for when, chunks in forward.items():
            @pl.when(s == when)
            def _(chunks=chunks):
                for j in chunks:
                    net.pass_on(j)
                    if j + 2 < N_CHUNKS - 1:
                        net.start(0, j + 2)
                    elif j + 2 == N_CHUNKS - 1:
                        for copy in net.last_chunk(0, ends):
                            copy.start()
        for when, chunks in second.items():
            @pl.when(s == when)
            def _(chunks=chunks):
                for j in chunks:
                    net.pass_second(j)

    def load_next(s, slot, after):
        for j in range(3, N_CHUNKS - 1):
            if (N_CHUNKS - 1 + j >= LOAD_AFTER) == after:
                @pl.when(s == N_CHUNKS - 1 + j)
                def _(j=j):
                    if j >= 4:
                        net.arrived(2, j)
                    net.arrived(3, j)

        if not after:
            @pl.when(s + 1 < N_CHUNKS)
            def _():
                for copy in own_loads(s + 1, 1 - slot):
                    copy.start()

        if after:
            @pl.when(s == 2 * N_CHUNKS - 2)
            def _():
                for copy, on in zip(net.last_chunk(0, ends), net.last_chunk(2, ends)):
                    copy.wait_recv()
                    on.start()
                for on in net.last_chunk(2, ends):
                    on.wait_recv()
                for copy in end_loads(1 - slot):
                    copy.start()

        first, last = (LOAD_AFTER, 2 * N_CHUNKS - 2) if after else (N_CHUNKS - 1, LOAD_AFTER)

        @pl.when((s >= first) & (s < last))
        def _():
            for copy in other_loads(s + 1 - N_CHUNKS, 1 - slot):
                copy.start()

    def step(s, carry):
        slot = lax.rem(s, 2)
        pass_on(s, LATE_FORWARD, LATE_SECOND)
        load_next(s, slot, False)
        @pl.when(s < 2 * N_CHUNKS - 1)
        def _():
            for copy in own_loads(0, slot):
                copy.wait()

        @pl.when(s == 2 * N_CHUNKS - 1)
        def _():
            for copy in end_loads(slot):
                copy.wait()

        own_end = (s == N_CHUNKS - 1).astype(jnp.float32)
        other_end = (s == 2 * N_CHUNKS - 1).astype(jnp.float32)
        keep = 1.0 - own_end * (lane_tile == 0).astype(jnp.float32) - other_end * (lane_tile == 3).astype(jnp.float32)
        compute(slot, keep)
        pass_on(s, END_FORWARD, END_SECOND)
        load_next(s, slot, True)
        return carry

    lax.fori_loop(0, 2 * N_CHUNKS, step, 0)
    out_ref[...] = acc_sc[...].astype(out_ref.dtype)
    for j in range(N_EARLY, N_CHUNKS - 1):
        net.sent(0, j)
    for j in range(N_EARLY - 1, N_CHUNKS - 1):
        net.sent(1, j)
        net.sent(2, j)
    for j in range(N_EARLY - 2, N_CHUNKS - 1):
        net.sent(3, j)
    for stage in (0, 2):
        for copy in net.last_chunk(stage, ends):
            copy.wait_send()


def mlp(x, gain, o, wo, ro, w1, w3, w2, early):
    rows, dim = x.shape
    vm = pl.BlockSpec(memory_space=pltpu.VMEM)
    hbm = pl.BlockSpec(memory_space=pl.ANY)
    bf16 = jnp.bfloat16
    width = 4 * TILE
    left = w1.shape[1] % width
    n = N_CHUNKS
    return pl.pallas_call(
        mlp_kernel,
        in_specs=[vm] * 5 + [hbm] * 6,
        out_specs=[vm] + [hbm] * 6,
        out_shape=[jax.ShapeDtypeStruct((rows, dim), bf16)] + [jax.ShapeDtypeStruct(a.shape, bf16) for a in early] + [jax.ShapeDtypeStruct(s, bf16) for s in ((dim, left), (dim, left), (left, dim))],
        input_output_aliases={8: 1, 9: 2, 10: 3},
        scratch_shapes=[
            pltpu.VMEM((2, dim, width), bf16),
            pltpu.VMEM((2, dim, width), bf16),
            pltpu.VMEM((2, width, dim), bf16),
            pltpu.VMEM((rows, dim), bf16),
            pltpu.VMEM((rows, dim), jnp.float32),
            pltpu.SemaphoreType.DMA((2, 3)),
            pltpu.SemaphoreType.DMA((n, 4, 3)),
            pltpu.SemaphoreType.DMA((n, 4, 3)),
        ],
        compiler_params=pltpu.CompilerParams(collective_id=1, has_side_effects=True, vmem_limit_bytes=VMEM_LIMIT),
        cost_estimate=pl.CostEstimate(flops=12 * rows * dim * w1.shape[1], bytes_accessed=12 * dim * w1.shape[1], transcendentals=2 * rows * w1.shape[1]),
        name="mlp",
    )(x, gain, o, wo, ro, w1, w3, w2, *early)[0]

def solution(mesh):
    n_pieces = 2 * mesh.shape["cp"]

    def layer_shard(x_loc, norm_attn, norm_mlp, w_query, w_key, w_value, w_out, w_gate, w_up, w_down):
        tok_dev, dim = x_loc.shape
        local_q, head_dim = w_query.shape[1], w_query.shape[2]
        cp_index = lax.axis_index("cp")
        piece = jnp.where(lax.axis_index("tp") == 0, cp_index, n_pieces - 1 - cp_index)
        cos2, sin2 = rope_tables(piece * tok_dev + jnp.arange(tok_dev, dtype=jnp.int32), head_dim)
        wq, wk, wv = (jnp.transpose(w, (1, 0, 2)) for w in (w_query, w_key, w_value))
        wo = w_out.reshape(local_q * head_dim, dim)
        o, k_cache, v_cache, wo_other, *early = attention(x_loc, norm_attn, cos2, sin2, wq, wk, wv, wo, w_gate, w_up, w_down)
        layer_out = mlp(x_loc, norm_mlp, o, wo, wo_other, w_gate, w_up, w_down, early)
        return layer_out, k_cache, v_cache

    row_spec = P(("dp", "cp", "tp"), None)
    cache_spec = P(("dp", "cp"), "tp")
    head_spec = P(None, "tp", None)
    return jax.shard_map(
        layer_shard,
        mesh=mesh,
        in_specs=(row_spec, P(None), P(None), head_spec, head_spec, head_spec, P("tp", None, None), P(None, "tp"), P(None, "tp"), P("tp", None)),
        out_specs=(row_spec, cache_spec, cache_spec),
        check_vma=False,
    )
```

```python
import functools

import jax
import jax.numpy as jnp
from jax import lax
from jax.experimental import pallas as pl
from jax.experimental.pallas import tpu as pltpu
from jax.sharding import PartitionSpec as P

ROPE_BASE = 500000.0
NORM_EPS = 1e-5
MASK_VALUE = -1e30
LOG2E = 1.4426950408889634
VMEM_LIMIT = 60 * 1024 * 1024
Q_ROWS = 256
K_ROWS = 512
MESH = pl.DeviceIdType.MESH
TILE = 128
N_CHUNKS = 9
N_EARLY = 5
PART = 1


def rope_frequencies(head_dim):
    lane = jnp.arange(head_dim, dtype=jnp.int32)
    return ROPE_BASE ** (-2.0 * (lane % (head_dim // 2)).astype(jnp.float32) / head_dim)


class Links:
    def __init__(self, weights, recv, send_sems, recv_sems, n_tiles):
        self.y, self.c = lax.axis_index("tp"), lax.axis_index("cp")
        self.peer = {
            "y": {"tp": 1 - self.y},
            "x": {"cp": lax.rem(self.c + 2, 4)},
            "d": {"cp": self.c + 1 - 2 * lax.rem(self.c, 2)},
        }
        self.weights, self.recv, self.send_sems, self.recv_sems = weights, recv, send_sems, recv_sems
        self.n_tiles = n_tiles
        self.started = []

    def barrier(self):
        sem = pltpu.get_barrier_semaphore()
        for name in "yxd":
            pl.semaphore_signal(sem, inc=1, device_id=self.peer[name], device_id_type=MESH)
        pl.semaphore_wait(sem, 3)

    def remote(self, src, dst, ssem, rsem, to):
        return pltpu.make_async_remote_copy(src_ref=src, dst_ref=dst, send_sem=ssem, recv_sem=rsem, device_id=self.peer[to], device_id_type=MESH)

    def chunk(self, stage, j, arrays=slice(0, 3)):
        to = "yxdd"[stage]
        copies = []
        for a in range(3)[arrays]:
            if stage == 0:
                tile = 4 * j + self.c
                sl = pl.ds(pl.multiple_of(tile * TILE, TILE), TILE)
                src = self.weights[a].at[sl, :] if a == 2 else self.weights[a].at[:, sl]
            else:
                src = self.recv[a].at[j, (0, 0, 0, 1)[stage]]
            copies.append(self.remote(src, self.recv[a].at[j, stage], self.send_sems.at[j, stage, a], self.recv_sems.at[j, stage, a], to))
        return copies

    def last_chunk(self, stage, last):
        half = lax.rem(self.c, 2)
        begin = (self.n_tiles // 4) * 4 * TILE
        copies = []
        for a in range(3):
            depth = last[a].shape[0] // 2
            at = pl.ds(pl.multiple_of(half * depth, 64), depth)
            dst = last[a].at[at, :]
            if stage == 2:
                src = dst
            elif a == 2:
                src = self.weights[a].at[pl.ds(pl.multiple_of(begin + half * depth, 64), depth), :]
            else:
                src = self.weights[a].at[at, pl.ds(begin, last[a].shape[1])]
            j = N_CHUNKS - 1
            copies.append(self.remote(src, dst, self.send_sems.at[j, stage, a], self.recv_sems.at[j, stage, a], "y.d"[stage]))
        return copies

    def pass_on(self, j, here=0):
        for a in range(3):
            if a >= here:
                self.arrived(0, j, slice(a, a + 1))
            self.start(1, j, slice(a, a + 1))
            self.start(2, j, slice(a, a + 1))

    def pass_second(self, j):
        for first, over_d in zip(self.chunk(1, j), self.chunk(3, j)):
            first.wait_recv()
            over_d.start()

    def start(self, stage, j, arrays=slice(0, 3)):
        for copy in self.chunk(stage, j, arrays):
            copy.start()

    def arrived(self, stage, j, arrays=slice(0, 3)):
        for copy in self.chunk(stage, j, arrays):
            copy.wait_recv()

    def sent(self, stage, j, arrays=slice(0, 3)):
        for copy in self.chunk(stage, j, arrays):
            copy.wait_send()


EARLY_FORWARD = ((0, 14), (1, 17), (2, 19), (3, 21))
EARLY_SECOND = ((0, 18), (1, 20), (2, 22))
SLOT_SOURCE = (0, 0, 0, 1)


def normed_rows(wide, gain):
    inv_rms = lax.rsqrt(jnp.mean(wide * wide, axis=-1, keepdims=True) + NORM_EPS)
    return (wide * inv_rms * gain).astype(jnp.bfloat16)


def attention_kernel(x_ref, gain_ref, freq_ref, wq_ref, wk_ref, wv_ref, wo_ref, w1_ref, w3_ref, w2_ref,
                     o_ref, kc_ref, vc_ref, ro_ref, r1_ref, r3_ref, r2_ref,
                     cos_ref, sin_ref, a_sc, q_sc, wq_sc, wk_sc, wv_sc, kv_buf, m_sc, l_sc, acc_sc, send_sems, recv_sems, kv_send, kv_recv, wt_send, wt_recv):
    head_dim = 128
    half_dim = head_dim // 2
    chunk_len = x_ref.shape[0]
    heads = wq_ref.shape[0]
    chains = 2
    per_chain = heads // chains
    rows = per_chain * Q_ROWS
    q_blocks = chunk_len // Q_ROWS
    coef = head_dim ** -0.5 * LOG2E
    net = Links((w1_ref, w3_ref, w2_ref), (r1_ref, r3_ref, r2_ref), send_sems, recv_sems, w1_ref.shape[1] // TILE)
    y, c = net.y, net.c
    core_lower = lax.rem(c + y, 2)
    chip_lower = lax.rem(c // 2 + y, 2)
    other_chip = lax.rem(c + 2, 4)

    def kv_copy(n, hd):
        src, dst, to = ((0, 1, "x"), (0, 2, "d"), (1, 3, "d"), (0, 4, "y"), (4, 5, "x"), (4, 6, "d"), (5, 7, "d"))[n]
        return net.remote(kv_buf.at[src, hd], kv_buf.at[dst, hd], kv_send.at[n, hd], kv_recv.at[n, hd], to)

    def weight_copy(kind, stage):
        own, held = ((wk_ref, wk_sc), (wv_ref, wv_sc), (wq_ref, wq_sc), (wo_ref, ro_ref))[kind]
        quarter = own.shape[-2] // 4
        sl = pl.ds(pl.multiple_of((other_chip if stage == 3 else c) * quarter, 64), quarter)
        src = own if stage == 0 else held
        pick = (lambda r: r.at[sl, :]) if kind == 3 else (lambda r: r.at[:, sl, :])
        return net.remote(pick(src), pick(held), wt_send.at[kind, stage], wt_recv.at[kind, stage], "yxdd"[stage])

    def weights_start(kinds, stage):
        for kind in kinds:
            weight_copy(kind, stage).start()

    def weights_arrived(kinds, stage):
        for kind in kinds:
            weight_copy(kind, stage).wait_recv()

    def row_slice(i):
        return pl.ds(pl.multiple_of(i * Q_ROWS, Q_ROWS), Q_ROWS)

    def rope(t, sl):
        return (t * cos_ref[sl, :] + pltpu.roll(t, half_dim, 1) * sin_ref[sl, :]).astype(jnp.bfloat16)

    def norm_x():
        def body(i, carry):
            sl = row_slice(i)
            row = (y * (7 - 2 * c) + c) * chunk_len + i * Q_ROWS + lax.broadcasted_iota(jnp.int32, (Q_ROWS, head_dim), 0)
            angles = row.astype(jnp.float32) * freq_ref[...][None, :]
            sine_tab = jnp.sin(angles)
            cos_ref[sl, :] = jnp.cos(angles)
            sin_ref[sl, :] = jnp.where(lax.broadcasted_iota(jnp.int32, (Q_ROWS, head_dim), 1) < half_dim, -sine_tab, sine_tab)
            a_sc[sl, :] = normed_rows(x_ref[sl, :].astype(jnp.float32), gain_ref[...].astype(jnp.float32)[None, :])
            return carry
        lax.fori_loop(0, q_blocks, body, 0)

    def make_kv(k_ref, v_ref, hd):
        def body(i, carry):
            sl = row_slice(i)
            w = jnp.concatenate([k_ref[0], v_ref[0]], axis=1)
            proj = jnp.dot(a_sc[sl, :], w, preferred_element_type=jnp.float32)
            kv_buf[0, hd, 0, sl, :] = rope(proj[:, :head_dim], sl)
            kv_buf[0, hd, 1, sl, :] = proj[:, head_dim:].astype(jnp.bfloat16)
            return carry
        lax.fori_loop(0, q_blocks, body, 0)

    def make_q(w_ref, hd):
        def body(i, carry):
            sl = row_slice(i)
            w = jnp.concatenate([w_ref[h] for h in range(heads)], axis=1)
            proj = jnp.dot(a_sc[sl, :], w, preferred_element_type=jnp.float32)
            for h in range(heads):
                cols = slice(h * head_dim, (h + 1) * head_dim)
                q_sc[hd, sl, cols] = rope(proj[:, cols], sl)
            return carry
        lax.fori_loop(0, q_blocks, body, 0)

    net.barrier()
    weights_start((0, 1, 2), 0)
    norm_x()
    make_kv(wk_ref, wv_ref, 0)
    m_sc[...] = jnp.full_like(m_sc, MASK_VALUE)
    l_sc[...] = jnp.zeros_like(l_sc)
    acc_sc[...] = jnp.zeros_like(acc_sc)
    weights_arrived((0, 1), 0)
    weights_start((0, 1), 1)
    weights_start((0, 1), 2)
    kv_copy(1, 0).start()
    kv_copy(0, 0).start()
    kv_copy(3, 0).start()
    make_q(wq_ref, 0)

    def block(q_parts, state, start, slot, head, off, masked):
        k_blk = kv_buf[slot, head, 0, pl.ds(off, K_ROWS), :]
        v_blk = kv_buf[slot, head, 1, pl.ds(off, K_ROWS), :]
        for a in range(chains):
            s = lax.dot_general(q_parts[a], k_blk, (((1,), (1,)), ((), ())), preferred_element_type=jnp.float32)
            if masked:
                q_pos = start + lax.rem(lax.broadcasted_iota(jnp.int32, (rows, K_ROWS), 0), Q_ROWS)
                k_pos = off + lax.broadcasted_iota(jnp.int32, (rows, K_ROWS), 1)
                s = jnp.where(k_pos <= q_pos, s, MASK_VALUE)
            m_prev = m_sc[state, a]
            m_new = jnp.maximum(m_prev, jnp.max(s, axis=1, keepdims=True))
            alpha = jnp.exp2((m_prev - m_new) * coef)
            mc = m_new * coef
            sums = l_sc[state, a] * alpha
            p_tiles = []
            for j in range(K_ROWS // 128):
                p = jnp.exp2(s[:, j * 128:(j + 1) * 128] * coef - mc)
                sums = sums + p
                p_tiles.append(p.astype(jnp.bfloat16))
            l_sc[state, a] = sums
            m_sc[state, a] = m_new
            p_all = jnp.concatenate(p_tiles, axis=1)
            acc_sc[state, a] = acc_sc[state, a] * alpha + jnp.dot(p_all, v_blk, preferred_element_type=jnp.float32)

    def load_q(head, qb):
        sl = row_slice(qb)
        return [jnp.concatenate([q_sc[head, sl, (a * per_chain + h) * head_dim:(a * per_chain + h + 1) * head_dim] for h in range(per_chain)], axis=0) for a in range(chains)]

    per_piece = chunk_len // K_ROWS

    def step(s, carry):
        phase = s // q_blocks
        qb = lax.rem(s, q_blocks)
        is_last = phase // 4
        is_mid = (1 - is_last) * lax.rem(phase, 2)
        is_first = 1 - is_last - is_mid
        head = (1 - is_last) * (phase // 2) + is_last * (phase - 4)
        state = head * q_blocks + qb

        @pl.when(s == 0)
        def _():
            kv_copy(1, 0).wait_recv()

        @pl.when(s == 1)
        def _():
            weights_arrived((0, 1), 1)
            weights_start((0, 1), 3)

        @pl.when(s == 2)
        def _():
            weights_arrived((0, 1), 2)
            weights_arrived((0, 1), 3)
            make_kv(wk_sc, wv_sc, 1)
            weights_arrived((2,), 0)
            weights_start((2,), 1)
            weights_start((2,), 2)

        @pl.when(s == 3)
        def _():
            kv_copy(1, 1).start()
            kv_copy(0, 1).start()
            kv_copy(3, 1).start()
            weights_start((3,), 0)
            net.start(0, 0)
            net.start(0, 1)
            kv_copy(0, 0).wait_recv()
            kv_copy(2, 0).start()

        @pl.when(s == 4)
        def _():
            kv_copy(2, 0).wait_recv()

        @pl.when(s == 6)
        def _():
            weights_arrived((2,), 1)
            weights_start((2,), 3)
            kv_copy(3, 0).wait_recv()
            kv_copy(4, 0).start()
            kv_copy(5, 0).start()

        @pl.when(s == 7)
        def _():
            weights_arrived((2,), 2)
            weights_arrived((2,), 3)
            make_q(wq_sc, 1)

        @pl.when(s == 8)
        def _():
            kv_copy(1, 1).wait_recv()

        @pl.when(s == 9)
        def _():
            kv_copy(0, 1).wait_recv()
            kv_copy(2, 1).start()

        @pl.when(s == 10)
        def _():
            kv_copy(3, 1).wait_recv()
            kv_copy(4, 1).start()
            kv_copy(5, 1).start()

        @pl.when(s == 12)
        def _():
            kv_copy(2, 1).wait_recv()
            weights_arrived((3,), 0)
            weights_start((3,), 1)
            weights_start((3,), 2)

        @pl.when(s == 13)
        def _():
            kv_copy(4, 0).wait_recv()
            kv_copy(6, 0).start()

        @pl.when(s == 14)
        def _():
            kv_copy(4, 1).wait_recv()
            kv_copy(6, 1).start()

        @pl.when(s == 16)
        def _():
            for hd in range(2):
                kv_copy(5, hd).wait_recv()
                kv_copy(6, hd).wait_recv()
            weights_arrived((3,), 1)
            weights_start((3,), 3)

        for j, when in EARLY_FORWARD:
            @pl.when(s == when)
            def _(j=j):
                net.pass_on(j)
                if j + 2 < N_EARLY:
                    net.start(0, j + 2)
                elif j + 2 == N_EARLY:
                    net.start(0, N_EARLY, slice(0, PART))

        for j, when in EARLY_SECOND:
            @pl.when(s == when)
            def _(j=j):
                net.pass_second(j)

        q_parts = load_q(head, qb)
        start = qb * Q_ROWS
        diag = start // K_ROWS
        count = is_first * (diag + per_piece * core_lower) + is_mid * 2 * per_piece * chip_lower + is_last * 4 * per_piece * y
        kv_head = head + is_last * (1 - 2 * head)

        def inner(i, carry):
            in_core = (i >= diag).astype(jnp.int32)
            idx = i - is_first * in_core * diag
            slot = is_first * 2 * in_core + is_mid * (1 + 2 * (i // per_piece)) + is_last * (4 + i // per_piece)
            off = (is_first * (in_core * lax.rem(idx, per_piece) + (1 - in_core) * i) + (1 - is_first) * lax.rem(i, per_piece)) * K_ROWS
            block(q_parts, state, start, slot, kv_head, pl.multiple_of(off, K_ROWS), False)
            return carry

        lax.fori_loop(0, count, inner, 0)

        @pl.when(is_first == 1)
        def _():
            block(q_parts, state, start, 0, head, pl.multiple_of(diag * K_ROWS, K_ROWS), True)

        return carry

    lax.fori_loop(0, 6 * q_blocks, step, 0)

    def finish(state, carry):
        head = state // q_blocks
        sl = row_slice(lax.rem(state, q_blocks))
        for a in range(chains):
            total = jnp.sum(l_sc[state, a], axis=1, keepdims=True)
            out = (acc_sc[state, a] / total).astype(jnp.bfloat16)
            for h in range(per_chain):
                o_ref[head, sl, (a * per_chain + h) * head_dim:(a * per_chain + h + 1) * head_dim] = out[h * Q_ROWS:(h + 1) * Q_ROWS]
        return carry

    lax.fori_loop(0, 2 * q_blocks, finish, 0)

    for e in range(2):
        late = c // 2
        owner = (1 - late) * (2 * c + e) + late * (7 - 2 * c - e)
        cross = lax.rem(late + y, 2)
        slot = 4 * cross + 2 * lax.rem(owner + c, 2) + lax.rem(owner // 2 + c // 2, 2)
        kc_ref[e * chunk_len:(e + 1) * chunk_len] = kv_buf[slot, cross, 0]
        vc_ref[e * chunk_len:(e + 1) * chunk_len] = kv_buf[slot, cross, 1]

    weights_arrived((3,), 2)
    weights_arrived((3,), 3)
    for hd in range(2):
        for n in range(7):
            kv_copy(n, hd).wait_send()
    for kind in range(4):
        for stage in range(4):
            weight_copy(kind, stage).wait_send()
    forwarded = [j for j, _ in EARLY_FORWARD]
    second = [j for j, _ in EARLY_SECOND]
    for j in range(N_EARLY):
        if j not in forwarded:
            net.arrived(0, j)
        net.sent(0, j)
    net.arrived(0, N_EARLY, slice(0, PART))
    net.sent(0, N_EARLY, slice(0, PART))
    for j in forwarded:
        if j not in second:
            net.arrived(1, j)
        net.arrived(2, j)
        net.sent(1, j)
        net.sent(2, j)
    for j in second:
        net.arrived(3, j)
        net.sent(3, j)


def attention(x, gain, freq, wq, wk, wv, wo, w1, w3, w2):
    rows, dim = x.shape
    width = wq.shape[0] * 128
    states = 2 * rows // Q_ROWS
    m_rows = width // 128 // 2 * Q_ROWS
    vm = pl.BlockSpec(memory_space=pltpu.VMEM)
    hbm = pl.BlockSpec(memory_space=pl.ANY)
    bf16 = jnp.bfloat16
    n = N_EARLY + 1
    return pl.pallas_call(
        attention_kernel,
        in_specs=[vm] * 6 + [hbm] * 4,
        out_specs=[vm, vm, vm, hbm, hbm, hbm, hbm],
        out_shape=[
            jax.ShapeDtypeStruct((2, rows, width), bf16),
            jax.ShapeDtypeStruct((2 * rows, 128), bf16),
            jax.ShapeDtypeStruct((2 * rows, 128), bf16),
            jax.ShapeDtypeStruct(wo.shape, bf16),
            jax.ShapeDtypeStruct((N_CHUNKS - 1, 4, dim, TILE), bf16),
            jax.ShapeDtypeStruct((N_CHUNKS - 1, 4, dim, TILE), bf16),
            jax.ShapeDtypeStruct((N_CHUNKS - 1, 4, TILE, dim), bf16),
        ],
        scratch_shapes=[
            pltpu.VMEM((rows, 128), jnp.float32),
            pltpu.VMEM((rows, 128), jnp.float32),
            pltpu.VMEM((rows, dim), bf16),
            pltpu.VMEM((2, rows, width), bf16),
            pltpu.VMEM(wq.shape, bf16),
            pltpu.VMEM(wk.shape, bf16),
            pltpu.VMEM(wv.shape, bf16),
            pltpu.VMEM((8, 2, 2, rows, 128), bf16),
            pltpu.VMEM((states, 2, m_rows, 128), jnp.float32),
            pltpu.VMEM((states, 2, m_rows, 128), jnp.float32),
            pltpu.VMEM((states, 2, m_rows, 128), jnp.float32),
            pltpu.SemaphoreType.DMA((n, 4, 3)),
            pltpu.SemaphoreType.DMA((n, 4, 3)),
            pltpu.SemaphoreType.DMA((7, 2)),
            pltpu.SemaphoreType.DMA((7, 2)),
            pltpu.SemaphoreType.DMA((4, 4)),
            pltpu.SemaphoreType.DMA((4, 4)),
        ],
        compiler_params=pltpu.CompilerParams(collective_id=0, has_side_effects=True, vmem_limit_bytes=VMEM_LIMIT),
        cost_estimate=pl.CostEstimate(flops=16 * rows * 4096 * width, bytes_accessed=32 * 2**20, transcendentals=rows * 4096 * 12),
        name="attention",
    )(x, gain, freq, wq, wk, wv, wo, w1, w3, w2)


M_BLOCK = 512
LATE_FORWARD = {3: (5,), 7: (6,)}
LATE_SECOND = {3: (4,), 8: (5,)}
END_FORWARD = {12: (7,)}
END_SECOND = {12: (6,), 15: (7,)}
LOAD_AFTER = 12


def mlp_kernel(x_ref, gain_ref, o_ref, wo_ref, ro_ref, w1_ref, w3_ref, w2_ref, a1_ref, a3_ref, a2_ref, out_ref, r1_ref, r3_ref, r2_ref, e1_ref, e3_ref, e2_ref,
               w1_sc, w3_sc, w2_sc, b_ref, acc_sc, load_sems, send_sems, recv_sems):
    dim = x_ref.shape[1]
    width = 4 * TILE
    n_tiles = w1_ref.shape[1] // TILE
    net = Links((w1_ref, w3_ref, w2_ref), (r1_ref, r3_ref, r2_ref), send_sems, recv_sems, n_tiles)
    own_last = (n_tiles - 4) * TILE
    ends = (e1_ref, e3_ref, e2_ref)

    def own_loads(j, slot):
        off = min(j * width, own_last) if isinstance(j, int) else pl.multiple_of(jnp.minimum(j * width, own_last), TILE)
        sl = pl.ds(off, width)
        return [
            pltpu.make_async_copy(w1_ref.at[:, sl], w1_sc.at[slot], load_sems.at[slot, 0]),
            pltpu.make_async_copy(w3_ref.at[:, sl], w3_sc.at[slot], load_sems.at[slot, 1]),
            pltpu.make_async_copy(w2_ref.at[sl, :], w2_sc.at[slot], load_sems.at[slot, 2]),
        ]

    def other_loads(j, slot):
        copies = []
        for p in range(4):
            sl = pl.ds(p * TILE, TILE)
            copies.append(pltpu.make_async_copy(r1_ref.at[j, p], w1_sc.at[slot, :, sl], load_sems.at[slot, 0]))
            copies.append(pltpu.make_async_copy(r3_ref.at[j, p], w3_sc.at[slot, :, sl], load_sems.at[slot, 1]))
            copies.append(pltpu.make_async_copy(r2_ref.at[j, p], w2_sc.at[slot, sl, :], load_sems.at[slot, 2]))
        return copies

    def end_loads(slot):
        w = e1_ref.shape[1]
        return [
            pltpu.make_async_copy(e1_ref, w1_sc.at[slot, :, pl.ds(0, w)], load_sems.at[slot, 0]),
            pltpu.make_async_copy(e3_ref, w3_sc.at[slot, :, pl.ds(0, w)], load_sems.at[slot, 1]),
            pltpu.make_async_copy(e2_ref, w2_sc.at[slot, pl.ds(0, w), :], load_sems.at[slot, 2]),
        ]

    def compute(slot, lane_keep):
        def rows_step(m, carry):
            sl = pl.ds(pl.multiple_of(m * M_BLOCK, M_BLOCK), M_BLOCK)
            b = b_ref[sl, :]
            gate = jnp.dot(b, w1_sc[slot], preferred_element_type=jnp.float32)
            up = jnp.dot(b, w3_sc[slot], preferred_element_type=jnp.float32)
            hidden = jax.nn.silu(gate) * up
            hidden = jnp.where(lane_keep > 0.5, hidden, 0.0).astype(jnp.bfloat16)
            total = acc_sc[sl, :] + jnp.dot(hidden, w2_sc[slot], preferred_element_type=jnp.float32)
            acc_sc[sl, :] = total
            out_ref[sl, :] = total.astype(out_ref.dtype)
            return carry

        lax.fori_loop(0, b_ref.shape[0] // M_BLOCK, rows_step, 0)

    net.barrier()
    net.start(0, N_EARLY, slice(PART, 3))
    net.start(0, N_EARLY + 1)
    net.start(1, N_EARLY - 1)
    net.start(2, N_EARLY - 1)
    net.start(3, N_EARLY - 2)
    for copy in own_loads(0, 0):
        copy.start()

    def residual_rows(i, carry):
        sl = pl.ds(pl.multiple_of(i * Q_ROWS, Q_ROWS), Q_ROWS)
        attn = jnp.dot(o_ref[0, sl, :], wo_ref[...], preferred_element_type=jnp.float32)
        attn = attn + jnp.dot(o_ref[1, sl, :], ro_ref[...], preferred_element_type=jnp.float32)
        residual = (x_ref[sl, :].astype(jnp.float32) + attn).astype(jnp.bfloat16).astype(jnp.float32)
        acc_sc[sl, :] = residual
        b_ref[sl, :] = normed_rows(residual, gain_ref[...].astype(jnp.float32)[None, :])
        return carry

    lax.fori_loop(0, x_ref.shape[0] // Q_ROWS, residual_rows, 0)
    lane_tile = lax.broadcasted_iota(jnp.int32, (1, width), 1) // TILE

    def pass_on(s, forward, second):
        for when, chunks in forward.items():
            @pl.when(s == when)
            def _(chunks=chunks):
                for j in chunks:
                    net.pass_on(j, PART if j == N_EARLY else 0)
                    if j + 2 < N_CHUNKS - 1:
                        net.start(0, j + 2)
                    elif j + 2 == N_CHUNKS - 1:
                        for copy in net.last_chunk(0, ends):
                            copy.start()
        for when, chunks in second.items():
            @pl.when(s == when)
            def _(chunks=chunks):
                for j in chunks:
                    net.pass_second(j)

    def load_next(s, slot, after):
        for j in range(3, N_CHUNKS - 1):
            if (N_CHUNKS - 1 + j >= LOAD_AFTER) == after:
                @pl.when(s == N_CHUNKS - 1 + j)
                def _(j=j):
                    if j >= 4:
                        net.arrived(2, j)
                    net.arrived(3, j)

        if not after:
            @pl.when(s + 1 < N_CHUNKS)
            def _():
                for copy in own_loads(s + 1, 1 - slot):
                    copy.start()

        if after:
            @pl.when(s == 2 * N_CHUNKS - 2)
            def _():
                for copy, on in zip(net.last_chunk(0, ends), net.last_chunk(2, ends)):
                    copy.wait_recv()
                    on.start()
                for on in net.last_chunk(2, ends):
                    on.wait_recv()
                for copy in end_loads(1 - slot):
                    copy.start()

        first, last = (LOAD_AFTER, 2 * N_CHUNKS - 2) if after else (N_CHUNKS - 1, LOAD_AFTER)

        @pl.when((s >= first) & (s < last))
        def _():
            for copy in other_loads(s + 1 - N_CHUNKS, 1 - slot):
                copy.start()

    def step(s, carry):
        slot = lax.rem(s, 2)
        pass_on(s, LATE_FORWARD, LATE_SECOND)
        load_next(s, slot, False)
        @pl.when(s < 2 * N_CHUNKS - 1)
        def _():
            for copy in own_loads(0, slot):
                copy.wait()

        @pl.when(s == 2 * N_CHUNKS - 1)
        def _():
            for copy in end_loads(slot):
                copy.wait()

        own_end = (s == N_CHUNKS - 1).astype(jnp.float32)
        other_end = (s == 2 * N_CHUNKS - 1).astype(jnp.float32)
        keep = 1.0 - own_end * (lane_tile == 0).astype(jnp.float32) - other_end * (lane_tile == 3).astype(jnp.float32)
        compute(slot, keep)
        pass_on(s, END_FORWARD, END_SECOND)
        load_next(s, slot, True)
        return carry

    lax.fori_loop(0, 2 * N_CHUNKS, step, 0)
    net.sent(0, N_EARLY, slice(PART, 3))
    for j in range(N_EARLY + 1, N_CHUNKS - 1):
        net.sent(0, j)
    for j in range(N_EARLY - 1, N_CHUNKS - 1):
        net.sent(1, j)
        net.sent(2, j)
    for j in range(N_EARLY - 2, N_CHUNKS - 1):
        net.sent(3, j)
    for stage in (0, 2):
        for copy in net.last_chunk(stage, ends):
            copy.wait_send()


def mlp(x, gain, o, wo, ro, w1, w3, w2, early):
    rows, dim = x.shape
    vm = pl.BlockSpec(memory_space=pltpu.VMEM)
    hbm = pl.BlockSpec(memory_space=pl.ANY)
    bf16 = jnp.bfloat16
    width = 4 * TILE
    left = w1.shape[1] % width
    n = N_CHUNKS
    return pl.pallas_call(
        mlp_kernel,
        in_specs=[vm] * 5 + [hbm] * 6,
        out_specs=[vm] + [hbm] * 6,
        out_shape=[jax.ShapeDtypeStruct((rows, dim), bf16)] + [jax.ShapeDtypeStruct(a.shape, bf16) for a in early] + [jax.ShapeDtypeStruct(s, bf16) for s in ((dim, left), (dim, left), (left, dim))],
        input_output_aliases={8: 1, 9: 2, 10: 3},
        scratch_shapes=[
            pltpu.VMEM((2, dim, width), bf16),
            pltpu.VMEM((2, dim, width), bf16),
            pltpu.VMEM((2, width, dim), bf16),
            pltpu.VMEM((rows, dim), bf16),
            pltpu.VMEM((rows, dim), jnp.float32),
            pltpu.SemaphoreType.DMA((2, 3)),
            pltpu.SemaphoreType.DMA((n, 4, 3)),
            pltpu.SemaphoreType.DMA((n, 4, 3)),
        ],
        compiler_params=pltpu.CompilerParams(collective_id=1, has_side_effects=True, vmem_limit_bytes=VMEM_LIMIT),
        cost_estimate=pl.CostEstimate(flops=12 * rows * dim * w1.shape[1], bytes_accessed=12 * dim * w1.shape[1], transcendentals=2 * rows * w1.shape[1]),
        name="mlp",
    )(x, gain, o, wo, ro, w1, w3, w2, *early)[0]

def solution(mesh):
    def layer_shard(x_loc, norm_attn, norm_mlp, w_query, w_key, w_value, w_out, w_gate, w_up, w_down):
        wq, wk, wv = (jnp.transpose(w, (1, 0, 2)) for w in (w_query, w_key, w_value))
        wo = w_out.reshape(-1, w_out.shape[2])
        o, k_cache, v_cache, wo_other, *early = attention(x_loc, norm_attn, rope_frequencies(w_query.shape[2]), wq, wk, wv, wo, w_gate, w_up, w_down)
        layer_out = mlp(x_loc, norm_mlp, o, wo, wo_other, w_gate, w_up, w_down, early)
        return layer_out, k_cache, v_cache

    row_spec = P(("dp", "cp", "tp"), None)
    cache_spec = P(("dp", "cp"), "tp")
    head_spec = P(None, "tp", None)
    return jax.shard_map(
        layer_shard,
        mesh=mesh,
        in_specs=(row_spec, P(None), P(None), head_spec, head_spec, head_spec, P("tp", None, None), P(None, "tp"), P(None, "tp"), P("tp", None)),
        out_specs=(row_spec, cache_spec, cache_spec),
        check_vma=False,
    )
```

```python
import functools

import jax
import jax.numpy as jnp
from jax import lax
from jax.experimental import pallas as pl
from jax.experimental.pallas import tpu as pltpu
from jax.sharding import PartitionSpec as P

ROPE_BASE = 500000.0
NORM_EPS = 1e-5
MASK_VALUE = -1e30
LOG2E = 1.4426950408889634
VMEM_LIMIT = 60 * 1024 * 1024
Q_ROWS = 256
K_ROWS = 512
MESH = pl.DeviceIdType.MESH
TILE = 128
N_CHUNKS = 9
N_EARLY = 5
PART = 1


def rope_frequencies(head_dim):
    lane = jnp.arange(head_dim, dtype=jnp.int32)
    return ROPE_BASE ** (-2.0 * (lane % (head_dim // 2)).astype(jnp.float32) / head_dim)


class Links:
    def __init__(self, weights, recv, send_sems, recv_sems, n_tiles):
        self.y, self.c = lax.axis_index("tp"), lax.axis_index("cp")
        self.peer = {
            "y": {"tp": 1 - self.y},
            "x": {"cp": lax.rem(self.c + 2, 4)},
            "d": {"cp": self.c + 1 - 2 * lax.rem(self.c, 2)},
        }
        self.weights, self.recv, self.send_sems, self.recv_sems = weights, recv, send_sems, recv_sems
        self.n_tiles = n_tiles
        self.started = []

    def barrier(self):
        sem = pltpu.get_barrier_semaphore()
        for name in "yxd":
            pl.semaphore_signal(sem, inc=1, device_id=self.peer[name], device_id_type=MESH)
        pl.semaphore_wait(sem, 3)

    def remote(self, src, dst, ssem, rsem, to):
        return pltpu.make_async_remote_copy(src_ref=src, dst_ref=dst, send_sem=ssem, recv_sem=rsem, device_id=self.peer[to], device_id_type=MESH)

    def chunk(self, stage, j, arrays=slice(0, 3)):
        to = "yxdd"[stage]
        copies = []
        for a in range(3)[arrays]:
            if stage == 0:
                tile = 4 * j + self.c
                sl = pl.ds(pl.multiple_of(tile * TILE, TILE), TILE)
                src = self.weights[a].at[sl, :] if a == 2 else self.weights[a].at[:, sl]
            else:
                src = self.recv[a].at[j, (0, 0, 0, 1)[stage]]
            copies.append(self.remote(src, self.recv[a].at[j, stage], self.send_sems.at[j, stage, a], self.recv_sems.at[j, stage, a], to))
        return copies

    def last_chunk(self, stage, last, arrays=slice(0, 3)):
        half = lax.rem(self.c, 2)
        begin = (self.n_tiles // 4) * 4 * TILE
        copies = []
        for a in range(3)[arrays]:
            depth = last[a].shape[0] // 2
            at = pl.ds(pl.multiple_of(half * depth, 64), depth)
            dst = last[a].at[at, :]
            if stage == 2:
                src = dst
            elif a == 2:
                src = self.weights[a].at[pl.ds(pl.multiple_of(begin + half * depth, 64), depth), :]
            else:
                src = self.weights[a].at[at, pl.ds(begin, last[a].shape[1])]
            j = N_CHUNKS - 1
            copies.append(self.remote(src, dst, self.send_sems.at[j, stage, a], self.recv_sems.at[j, stage, a], "y.d"[stage]))
        return copies

    def pass_on(self, j, here=0):
        for a in range(3):
            if a >= here:
                self.arrived(0, j, slice(a, a + 1))
            self.start(1, j, slice(a, a + 1))
            self.start(2, j, slice(a, a + 1))

    def pass_second(self, j):
        for first, over_d in zip(self.chunk(1, j), self.chunk(3, j)):
            first.wait_recv()
            over_d.start()

    def start(self, stage, j, arrays=slice(0, 3)):
        for copy in self.chunk(stage, j, arrays):
            copy.start()

    def arrived(self, stage, j, arrays=slice(0, 3)):
        for copy in self.chunk(stage, j, arrays):
            copy.wait_recv()

    def sent(self, stage, j, arrays=slice(0, 3)):
        for copy in self.chunk(stage, j, arrays):
            copy.wait_send()


EARLY_FORWARD = ((0, 15), (1, 18), (2, 20), (3, 22))
EARLY_SECOND = ((0, 19), (1, 21), (2, 23))
SLOT_SOURCE = (0, 0, 0, 1)


def normed_rows(wide, gain):
    inv_rms = lax.rsqrt(jnp.mean(wide * wide, axis=-1, keepdims=True) + NORM_EPS)
    return (wide * inv_rms * gain).astype(jnp.bfloat16)


def attention_kernel(x_ref, gain_ref, freq_ref, wq_ref, wk_ref, wv_ref, wo_ref, w1_ref, w3_ref, w2_ref,
                     o_ref, kc_ref, vc_ref, ro_ref, r1_ref, r3_ref, r2_ref,
                     cos_ref, sin_ref, a_sc, q_sc, wq_sc, wk_sc, wv_sc, kv_buf, m_sc, l_sc, acc_sc, send_sems, recv_sems, kv_send, kv_recv, wt_send, wt_recv):
    head_dim = 128
    half_dim = head_dim // 2
    chunk_len = x_ref.shape[0]
    heads = wq_ref.shape[0]
    chains = 2
    per_chain = heads // chains
    rows = per_chain * Q_ROWS
    q_blocks = chunk_len // Q_ROWS
    coef = head_dim ** -0.5 * LOG2E
    net = Links((w1_ref, w3_ref, w2_ref), (r1_ref, r3_ref, r2_ref), send_sems, recv_sems, w1_ref.shape[1] // TILE)
    y, c = net.y, net.c
    core_lower = lax.rem(c + y, 2)
    chip_lower = lax.rem(c // 2 + y, 2)
    other_chip = lax.rem(c + 2, 4)

    def kv_copy(n, hd):
        src, dst, to = ((0, 1, "x"), (0, 2, "d"), (1, 3, "d"), (0, 4, "y"), (4, 5, "x"), (4, 6, "d"), (5, 7, "d"))[n]
        return net.remote(kv_buf.at[src, hd], kv_buf.at[dst, hd], kv_send.at[n, hd], kv_recv.at[n, hd], to)

    def weight_copy(kind, stage):
        own, held = ((wk_ref, wk_sc), (wv_ref, wv_sc), (wq_ref, wq_sc), (wo_ref, ro_ref))[kind]
        quarter = own.shape[-2] // 4
        sl = pl.ds(pl.multiple_of((other_chip if stage == 3 else c) * quarter, 64), quarter)
        src = own if stage == 0 else held
        pick = (lambda r: r.at[sl, :]) if kind == 3 else (lambda r: r.at[:, sl, :])
        return net.remote(pick(src), pick(held), wt_send.at[kind, stage], wt_recv.at[kind, stage], "yxdd"[stage])

    def weights_start(kinds, stage):
        for kind in kinds:
            weight_copy(kind, stage).start()

    def weights_arrived(kinds, stage):
        for kind in kinds:
            weight_copy(kind, stage).wait_recv()

    def row_slice(i):
        return pl.ds(pl.multiple_of(i * Q_ROWS, Q_ROWS), Q_ROWS)

    def rope(t, sl):
        return (t * cos_ref[sl, :] + pltpu.roll(t, half_dim, 1) * sin_ref[sl, :]).astype(jnp.bfloat16)

    def norm_x():
        def body(i, carry):
            sl = row_slice(i)
            row = (y * (7 - 2 * c) + c) * chunk_len + i * Q_ROWS + lax.broadcasted_iota(jnp.int32, (Q_ROWS, head_dim), 0)
            angles = row.astype(jnp.float32) * freq_ref[...][None, :]
            sine_tab = jnp.sin(angles)
            cos_ref[sl, :] = jnp.cos(angles)
            sin_ref[sl, :] = jnp.where(lax.broadcasted_iota(jnp.int32, (Q_ROWS, head_dim), 1) < half_dim, -sine_tab, sine_tab)
            a_sc[sl, :] = normed_rows(x_ref[sl, :].astype(jnp.float32), gain_ref[...].astype(jnp.float32)[None, :])
            return carry
        lax.fori_loop(0, q_blocks, body, 0)

    def make_kv(k_ref, v_ref, hd):
        def body(i, carry):
            sl = row_slice(i)
            w = jnp.concatenate([k_ref[0], v_ref[0]], axis=1)
            proj = jnp.dot(a_sc[sl, :], w, preferred_element_type=jnp.float32)
            kv_buf[0, hd, 0, sl, :] = rope(proj[:, :head_dim], sl)
            kv_buf[0, hd, 1, sl, :] = proj[:, head_dim:].astype(jnp.bfloat16)
            return carry
        lax.fori_loop(0, q_blocks, body, 0)

    def make_q(w_ref, hd):
        def body(i, carry):
            sl = row_slice(i)
            w = jnp.concatenate([w_ref[h] for h in range(heads)], axis=1)
            proj = jnp.dot(a_sc[sl, :], w, preferred_element_type=jnp.float32)
            for h in range(heads):
                cols = slice(h * head_dim, (h + 1) * head_dim)
                q_sc[hd, sl, cols] = rope(proj[:, cols], sl)
            return carry
        lax.fori_loop(0, q_blocks, body, 0)

    net.barrier()
    weights_start((0, 1, 2), 0)
    norm_x()
    make_kv(wk_ref, wv_ref, 0)
    m_sc[...] = jnp.full_like(m_sc, MASK_VALUE)
    l_sc[...] = jnp.zeros_like(l_sc)
    acc_sc[...] = jnp.zeros_like(acc_sc)
    weights_arrived((0, 1), 0)
    weights_start((0, 1), 1)
    weights_start((0, 1), 2)
    kv_copy(1, 0).start()
    kv_copy(0, 0).start()
    kv_copy(3, 0).start()
    make_q(wq_ref, 0)

    def block(q_parts, state, start, slot, head, off, masked):
        k_blk = kv_buf[slot, head, 0, pl.ds(off, K_ROWS), :]
        v_blk = kv_buf[slot, head, 1, pl.ds(off, K_ROWS), :]
        for a in range(chains):
            s = lax.dot_general(q_parts[a], k_blk, (((1,), (1,)), ((), ())), preferred_element_type=jnp.float32)
            if masked:
                q_pos = start + lax.rem(lax.broadcasted_iota(jnp.int32, (rows, K_ROWS), 0), Q_ROWS)
                k_pos = off + lax.broadcasted_iota(jnp.int32, (rows, K_ROWS), 1)
                s = jnp.where(k_pos <= q_pos, s, MASK_VALUE)
            m_prev = m_sc[state, a]
            m_new = jnp.maximum(m_prev, jnp.max(s, axis=1, keepdims=True))
            alpha = jnp.exp2((m_prev - m_new) * coef)
            mc = m_new * coef
            sums = l_sc[state, a] * alpha
            p_tiles = []
            for j in range(K_ROWS // 128):
                p = jnp.exp2(s[:, j * 128:(j + 1) * 128] * coef - mc)
                sums = sums + p
                p_tiles.append(p.astype(jnp.bfloat16))
            l_sc[state, a] = sums
            m_sc[state, a] = m_new
            p_all = jnp.concatenate(p_tiles, axis=1)
            acc_sc[state, a] = acc_sc[state, a] * alpha + jnp.dot(p_all, v_blk, preferred_element_type=jnp.float32)

    def load_q(head, qb):
        sl = row_slice(qb)
        return [jnp.concatenate([q_sc[head, sl, (a * per_chain + h) * head_dim:(a * per_chain + h + 1) * head_dim] for h in range(per_chain)], axis=0) for a in range(chains)]

    per_piece = chunk_len // K_ROWS

    def step(s, carry):
        phase = s // q_blocks
        qb = lax.rem(s, q_blocks)
        is_last = phase // 4
        is_mid = (1 - is_last) * lax.rem(phase, 2)
        is_first = 1 - is_last - is_mid
        head = (1 - is_last) * (phase // 2) + is_last * (phase - 4)
        state = head * q_blocks + qb

        @pl.when(s == 0)
        def _():
            kv_copy(1, 0).wait_recv()

        @pl.when(s == 1)
        def _():
            weights_arrived((0, 1), 1)
            weights_start((0, 1), 3)

        @pl.when(s == 2)
        def _():
            weights_arrived((0, 1), 2)
            weights_arrived((0, 1), 3)
            make_kv(wk_sc, wv_sc, 1)
            weights_arrived((2,), 0)
            weights_start((2,), 1)
            weights_start((2,), 2)

        @pl.when(s == 3)
        def _():
            kv_copy(1, 1).start()
            kv_copy(0, 1).start()
            kv_copy(3, 1).start()
            weights_start((3,), 0)
            net.start(0, 0)
            net.start(0, 1)
            kv_copy(0, 0).wait_recv()
            kv_copy(2, 0).start()

        @pl.when(s == 4)
        def _():
            kv_copy(2, 0).wait_recv()

        @pl.when(s == 6)
        def _():
            weights_arrived((2,), 1)
            weights_start((2,), 3)
            kv_copy(3, 0).wait_recv()
            kv_copy(4, 0).start()
            kv_copy(5, 0).start()

        @pl.when(s == 7)
        def _():
            weights_arrived((2,), 2)
            weights_arrived((2,), 3)
            make_q(wq_sc, 1)

        @pl.when(s == 8)
        def _():
            kv_copy(1, 1).wait_recv()

        @pl.when(s == 9)
        def _():
            kv_copy(0, 1).wait_recv()
            kv_copy(2, 1).start()

        @pl.when(s == 10)
        def _():
            kv_copy(3, 1).wait_recv()
            kv_copy(4, 1).start()
            kv_copy(5, 1).start()

        @pl.when(s == 12)
        def _():
            kv_copy(2, 1).wait_recv()
            weights_arrived((3,), 0)
            weights_start((3,), 1)
            weights_start((3,), 2)

        @pl.when(s == 13)
        def _():
            kv_copy(4, 0).wait_recv()
            kv_copy(6, 0).start()

        @pl.when(s == 14)
        def _():
            kv_copy(4, 1).wait_recv()
            kv_copy(6, 1).start()

        @pl.when(s == 16)
        def _():
            for hd in range(2):
                kv_copy(5, hd).wait_recv()
                kv_copy(6, hd).wait_recv()
            weights_arrived((3,), 1)
            weights_start((3,), 3)

        for j, when in EARLY_FORWARD:
            @pl.when(s == when)
            def _(j=j):
                net.pass_on(j)
                if j + 2 < N_EARLY:
                    net.start(0, j + 2)
                elif j + 2 == N_EARLY:
                    net.start(0, N_EARLY, slice(0, PART))

        for j, when in EARLY_SECOND:
            @pl.when(s == when)
            def _(j=j):
                net.pass_second(j)

        q_parts = load_q(head, qb)
        start = qb * Q_ROWS
        diag = start // K_ROWS
        count = is_first * (diag + per_piece * core_lower) + is_mid * 2 * per_piece * chip_lower + is_last * 4 * per_piece * y
        kv_head = head + is_last * (1 - 2 * head)

        def inner(i, carry):
            in_core = (i >= diag).astype(jnp.int32)
            idx = i - is_first * in_core * diag
            slot = is_first * 2 * in_core + is_mid * (1 + 2 * (i // per_piece)) + is_last * (4 + i // per_piece)
            off = (is_first * (in_core * lax.rem(idx, per_piece) + (1 - in_core) * i) + (1 - is_first) * lax.rem(i, per_piece)) * K_ROWS
            block(q_parts, state, start, slot, kv_head, pl.multiple_of(off, K_ROWS), False)
            return carry

        lax.fori_loop(0, count, inner, 0)

        @pl.when(is_first == 1)
        def _():
            block(q_parts, state, start, 0, head, pl.multiple_of(diag * K_ROWS, K_ROWS), True)

        return carry

    lax.fori_loop(0, 6 * q_blocks, step, 0)

    def finish(state, carry):
        head = state // q_blocks
        sl = row_slice(lax.rem(state, q_blocks))
        for a in range(chains):
            total = jnp.sum(l_sc[state, a], axis=1, keepdims=True)
            out = (acc_sc[state, a] / total).astype(jnp.bfloat16)
            for h in range(per_chain):
                o_ref[head, sl, (a * per_chain + h) * head_dim:(a * per_chain + h + 1) * head_dim] = out[h * Q_ROWS:(h + 1) * Q_ROWS]
        return carry

    lax.fori_loop(0, 2 * q_blocks, finish, 0)

    for e in range(2):
        late = c // 2
        owner = (1 - late) * (2 * c + e) + late * (7 - 2 * c - e)
        cross = lax.rem(late + y, 2)
        slot = 4 * cross + 2 * lax.rem(owner + c, 2) + lax.rem(owner // 2 + c // 2, 2)
        kc_ref[e * chunk_len:(e + 1) * chunk_len] = kv_buf[slot, cross, 0]
        vc_ref[e * chunk_len:(e + 1) * chunk_len] = kv_buf[slot, cross, 1]

    weights_arrived((3,), 2)
    weights_arrived((3,), 3)
    for hd in range(2):
        for n in range(7):
            kv_copy(n, hd).wait_send()
    for kind in range(4):
        for stage in range(4):
            weight_copy(kind, stage).wait_send()
    forwarded = [j for j, _ in EARLY_FORWARD]
    second = [j for j, _ in EARLY_SECOND]
    for j in range(N_EARLY):
        if j not in forwarded:
            net.arrived(0, j)
        net.sent(0, j)
    net.arrived(0, N_EARLY, slice(0, PART))
    net.sent(0, N_EARLY, slice(0, PART))
    for j in forwarded:
        if j not in second:
            net.arrived(1, j)
        net.arrived(2, j)
        net.sent(1, j)
        net.sent(2, j)
    for j in second:
        net.arrived(3, j)
        net.sent(3, j)


def attention(x, gain, freq, wq, wk, wv, wo, w1, w3, w2):
    rows, dim = x.shape
    width = wq.shape[0] * 128
    states = 2 * rows // Q_ROWS
    m_rows = width // 128 // 2 * Q_ROWS
    vm = pl.BlockSpec(memory_space=pltpu.VMEM)
    hbm = pl.BlockSpec(memory_space=pl.ANY)
    bf16 = jnp.bfloat16
    n = N_EARLY + 1
    return pl.pallas_call(
        attention_kernel,
        in_specs=[vm] * 6 + [hbm] * 4,
        out_specs=[vm, vm, vm, hbm, hbm, hbm, hbm],
        out_shape=[
            jax.ShapeDtypeStruct((2, rows, width), bf16),
            jax.ShapeDtypeStruct((2 * rows, 128), bf16),
            jax.ShapeDtypeStruct((2 * rows, 128), bf16),
            jax.ShapeDtypeStruct(wo.shape, bf16),
            jax.ShapeDtypeStruct((N_CHUNKS - 1, 4, dim, TILE), bf16),
            jax.ShapeDtypeStruct((N_CHUNKS - 1, 4, dim, TILE), bf16),
            jax.ShapeDtypeStruct((N_CHUNKS - 1, 4, TILE, dim), bf16),
        ],
        scratch_shapes=[
            pltpu.VMEM((rows, 128), jnp.float32),
            pltpu.VMEM((rows, 128), jnp.float32),
            pltpu.VMEM((rows, dim), bf16),
            pltpu.VMEM((2, rows, width), bf16),
            pltpu.VMEM(wq.shape, bf16),
            pltpu.VMEM(wk.shape, bf16),
            pltpu.VMEM(wv.shape, bf16),
            pltpu.VMEM((8, 2, 2, rows, 128), bf16),
            pltpu.VMEM((states, 2, m_rows, 128), jnp.float32),
            pltpu.VMEM((states, 2, m_rows, 128), jnp.float32),
            pltpu.VMEM((states, 2, m_rows, 128), jnp.float32),
            pltpu.SemaphoreType.DMA((n, 4, 3)),
            pltpu.SemaphoreType.DMA((n, 4, 3)),
            pltpu.SemaphoreType.DMA((7, 2)),
            pltpu.SemaphoreType.DMA((7, 2)),
            pltpu.SemaphoreType.DMA((4, 4)),
            pltpu.SemaphoreType.DMA((4, 4)),
        ],
        compiler_params=pltpu.CompilerParams(collective_id=0, has_side_effects=True, vmem_limit_bytes=VMEM_LIMIT),
        cost_estimate=pl.CostEstimate(flops=16 * rows * 4096 * width, bytes_accessed=32 * 2**20, transcendentals=rows * 4096 * 12),
        name="attention",
    )(x, gain, freq, wq, wk, wv, wo, w1, w3, w2)


M_BLOCK = 512
LATE_FORWARD = {3: (5,), 7: (6,), 11: (7,)}
LATE_SECOND = {3: (4,), 8: (5,), 12: (6,)}
END_SECOND = {15: (7,)}
LOAD_AFTER = 15
STEPS = 2 * N_CHUNKS - 1


def mlp_kernel(x_ref, gain_ref, o_ref, wo_ref, ro_ref, w1_ref, w3_ref, w2_ref, a1_ref, a3_ref, a2_ref, out_ref, r1_ref, r3_ref, r2_ref, e1_ref, e3_ref, e2_ref,
               w1_sc, w3_sc, w2_sc, b_ref, acc_sc, hid_sc, load_sems, send_sems, recv_sems):
    dim = x_ref.shape[1]
    width = 4 * TILE
    n_tiles = w1_ref.shape[1] // TILE
    net = Links((w1_ref, w3_ref, w2_ref), (r1_ref, r3_ref, r2_ref), send_sems, recv_sems, n_tiles)
    own_last = (n_tiles - 4) * TILE
    ends = (e1_ref, e3_ref, e2_ref)

    def own_loads(j, slot):
        off = min(j * width, own_last) if isinstance(j, int) else pl.multiple_of(jnp.minimum(j * width, own_last), TILE)
        sl = pl.ds(off, width)
        return [
            pltpu.make_async_copy(w1_ref.at[:, sl], w1_sc.at[slot], load_sems.at[slot, 0]),
            pltpu.make_async_copy(w3_ref.at[:, sl], w3_sc.at[slot], load_sems.at[slot, 1]),
            pltpu.make_async_copy(w2_ref.at[sl, :], w2_sc.at[slot], load_sems.at[slot, 2]),
        ]

    def other_loads(j, slot):
        copies = []
        for p in range(4):
            sl = pl.ds(p * TILE, TILE)
            copies.append(pltpu.make_async_copy(r1_ref.at[j, p], w1_sc.at[slot, :, sl], load_sems.at[slot, 0]))
            copies.append(pltpu.make_async_copy(r3_ref.at[j, p], w3_sc.at[slot, :, sl], load_sems.at[slot, 1]))
            copies.append(pltpu.make_async_copy(r2_ref.at[j, p], w2_sc.at[slot, sl, :], load_sems.at[slot, 2]))
        return copies

    def end_load(slot, a):
        w = pl.ds(0, e1_ref.shape[1])
        dst = w2_sc.at[slot, w, :] if a == 2 else (w1_sc, w3_sc)[a].at[slot, :, w]
        return pltpu.make_async_copy(ends[a], dst, load_sems.at[slot, a])

    def compute(slot, lane_keep):
        def rows_step(m, carry):
            sl = pl.ds(pl.multiple_of(m * M_BLOCK, M_BLOCK), M_BLOCK)
            b = b_ref[sl, :]
            gate = jnp.dot(b, w1_sc[slot], preferred_element_type=jnp.float32)
            up = jnp.dot(b, w3_sc[slot], preferred_element_type=jnp.float32)
            hidden = jax.nn.silu(gate) * up
            hidden = jnp.where(lane_keep > 0.5, hidden, 0.0).astype(jnp.bfloat16)
            acc_sc[sl, :] += jnp.dot(hidden, w2_sc[slot], preferred_element_type=jnp.float32)
            return carry

        lax.fori_loop(0, b_ref.shape[0] // M_BLOCK, rows_step, 0)

    net.barrier()
    net.start(0, N_EARLY, slice(PART, 3))
    net.start(0, N_EARLY + 1)
    net.start(1, N_EARLY - 1)
    net.start(2, N_EARLY - 1)
    net.start(3, N_EARLY - 2)
    for copy in own_loads(0, 0):
        copy.start()

    def residual_rows(i, carry):
        sl = pl.ds(pl.multiple_of(i * Q_ROWS, Q_ROWS), Q_ROWS)
        attn = jnp.dot(o_ref[0, sl, :], wo_ref[...], preferred_element_type=jnp.float32)
        attn = attn + jnp.dot(o_ref[1, sl, :], ro_ref[...], preferred_element_type=jnp.float32)
        residual = (x_ref[sl, :].astype(jnp.float32) + attn).astype(jnp.bfloat16).astype(jnp.float32)
        acc_sc[sl, :] = residual
        b_ref[sl, :] = normed_rows(residual, gain_ref[...].astype(jnp.float32)[None, :])
        return carry

    lax.fori_loop(0, x_ref.shape[0] // Q_ROWS, residual_rows, 0)
    lane_tile = lax.broadcasted_iota(jnp.int32, (1, width), 1) // TILE

    def pass_on(s, forward, second):
        for when, chunks in forward.items():
            @pl.when(s == when)
            def _(chunks=chunks):
                for j in chunks:
                    net.pass_on(j, PART if j == N_EARLY else 0)
                    if j + 2 < N_CHUNKS - 1:
                        net.start(0, j + 2)
                    elif j + 2 == N_CHUNKS - 1:
                        for copy in net.last_chunk(0, ends):
                            copy.start()
        for when, chunks in second.items():
            @pl.when(s == when)
            def _(chunks=chunks):
                for j in chunks:
                    net.pass_second(j)

    def load_next(s, slot, after):
        for j in range(3, N_CHUNKS - 1):
            if (N_CHUNKS - 1 + j >= LOAD_AFTER) == after:
                @pl.when(s == N_CHUNKS - 1 + j)
                def _(j=j):
                    if j >= 4:
                        net.arrived(2, j)
                    net.arrived(3, j)

        if not after:
            @pl.when(s + 1 < N_CHUNKS)
            def _():
                for copy in own_loads(s + 1, 1 - slot):
                    copy.start()

        if not after:
            @pl.when(s == STEPS - 1)
            def _():
                for a in range(2):
                    net.last_chunk(2, ends, slice(a, a + 1))[0].wait_recv()
                    end_load(1 - slot, a).start()

        first, last = (LOAD_AFTER, STEPS - 1) if after else (N_CHUNKS - 1, LOAD_AFTER)

        @pl.when((s >= first) & (s < last))
        def _():
            for copy in other_loads(s + 1 - N_CHUNKS, 1 - slot):
                copy.start()

    def step(s, carry):
        slot = lax.rem(s, 2)
        pass_on(s, LATE_FORWARD, LATE_SECOND)
        load_next(s, slot, False)
        for copy in own_loads(0, slot):
            copy.wait()

        keep = 1.0 - (s == N_CHUNKS - 1).astype(jnp.float32) * (lane_tile == 0).astype(jnp.float32)
        compute(slot, keep)
        pass_on(s, {}, END_SECOND)

        @pl.when(s == STEPS - 2)
        def _():
            for a in range(2):
                net.last_chunk(0, ends, slice(a, a + 1))[0].wait_recv()
                net.last_chunk(2, ends, slice(a, a + 1))[0].start()

        load_next(s, slot, True)
        return carry

    lax.fori_loop(0, STEPS, step, 0)

    slot = STEPS % 2
    left = e1_ref.shape[1]
    net.last_chunk(0, ends, slice(2, 3))[0].wait_recv()
    net.last_chunk(2, ends, slice(2, 3))[0].start()
    for a in range(2):
        end_load(slot, a).wait()

    def hidden_rows(m, carry):
        sl = pl.ds(pl.multiple_of(m * M_BLOCK, M_BLOCK), M_BLOCK)
        gate = jnp.dot(b_ref[sl, :], w1_sc[slot, :, :left], preferred_element_type=jnp.float32)
        up = jnp.dot(b_ref[sl, :], w3_sc[slot, :, :left], preferred_element_type=jnp.float32)
        hid_sc[sl, :] = (jax.nn.silu(gate) * up).astype(jnp.bfloat16)
        return carry

    lax.fori_loop(0, x_ref.shape[0] // M_BLOCK, hidden_rows, 0)
    net.last_chunk(2, ends, slice(2, 3))[0].wait_recv()
    end_load(slot, 2).start()
    end_load(slot, 2).wait()

    def out_rows(m, carry):
        sl = pl.ds(pl.multiple_of(m * M_BLOCK, M_BLOCK), M_BLOCK)
        total = acc_sc[sl, :] + jnp.dot(hid_sc[sl, :], w2_sc[slot, :left, :], preferred_element_type=jnp.float32)
        out_ref[sl, :] = total.astype(out_ref.dtype)
        return carry

    lax.fori_loop(0, x_ref.shape[0] // M_BLOCK, out_rows, 0)
    net.sent(0, N_EARLY, slice(PART, 3))
    for j in range(N_EARLY + 1, N_CHUNKS - 1):
        net.sent(0, j)
    for j in range(N_EARLY - 1, N_CHUNKS - 1):
        net.sent(1, j)
        net.sent(2, j)
    for j in range(N_EARLY - 2, N_CHUNKS - 1):
        net.sent(3, j)
    for stage in (0, 2):
        for copy in net.last_chunk(stage, ends):
            copy.wait_send()


def mlp(x, gain, o, wo, ro, w1, w3, w2, early):
    rows, dim = x.shape
    vm = pl.BlockSpec(memory_space=pltpu.VMEM)
    hbm = pl.BlockSpec(memory_space=pl.ANY)
    bf16 = jnp.bfloat16
    width = 4 * TILE
    left = w1.shape[1] % width
    n = N_CHUNKS
    return pl.pallas_call(
        mlp_kernel,
        in_specs=[vm] * 5 + [hbm] * 6,
        out_specs=[vm] + [hbm] * 6,
        out_shape=[jax.ShapeDtypeStruct((rows, dim), bf16)] + [jax.ShapeDtypeStruct(a.shape, bf16) for a in early] + [jax.ShapeDtypeStruct(s, bf16) for s in ((dim, left), (dim, left), (left, dim))],
        input_output_aliases={8: 1, 9: 2, 10: 3},
        scratch_shapes=[
            pltpu.VMEM((2, dim, width), bf16),
            pltpu.VMEM((2, dim, width), bf16),
            pltpu.VMEM((2, width, dim), bf16),
            pltpu.VMEM((rows, dim), bf16),
            pltpu.VMEM((rows, dim), jnp.float32),
            pltpu.VMEM((rows, left), bf16),
            pltpu.SemaphoreType.DMA((2, 3)),
            pltpu.SemaphoreType.DMA((n, 4, 3)),
            pltpu.SemaphoreType.DMA((n, 4, 3)),
        ],
        compiler_params=pltpu.CompilerParams(collective_id=1, has_side_effects=True, vmem_limit_bytes=VMEM_LIMIT),
        cost_estimate=pl.CostEstimate(flops=12 * rows * dim * w1.shape[1], bytes_accessed=12 * dim * w1.shape[1], transcendentals=2 * rows * w1.shape[1]),
        name="mlp",
    )(x, gain, o, wo, ro, w1, w3, w2, *early)[0]

def solution(mesh):
    def layer_shard(x_loc, norm_attn, norm_mlp, w_query, w_key, w_value, w_out, w_gate, w_up, w_down):
        wq, wk, wv = (jnp.transpose(w, (1, 0, 2)) for w in (w_query, w_key, w_value))
        wo = w_out.reshape(-1, w_out.shape[2])
        o, k_cache, v_cache, wo_other, *early = attention(x_loc, norm_attn, rope_frequencies(w_query.shape[2]), wq, wk, wv, wo, w_gate, w_up, w_down)
        layer_out = mlp(x_loc, norm_mlp, o, wo, wo_other, w_gate, w_up, w_down, early)
        return layer_out, k_cache, v_cache

    row_spec = P(("dp", "cp", "tp"), None)
    cache_spec = P(("dp", "cp"), "tp")
    head_spec = P(None, "tp", None)
    return jax.shard_map(
        layer_shard,
        mesh=mesh,
        in_specs=(row_spec, P(None), P(None), head_spec, head_spec, head_spec, P("tp", None, None), P(None, "tp"), P(None, "tp"), P("tp", None)),
        out_specs=(row_spec, cache_spec, cache_spec),
        check_vma=False,
    )
```

```python
import functools

import jax
import jax.numpy as jnp
from jax import lax
from jax.experimental import pallas as pl
from jax.experimental.pallas import tpu as pltpu
from jax.sharding import PartitionSpec as P

ROPE_BASE = 500000.0
NORM_EPS = 1e-5
MASK_VALUE = -1e30
LOG2E = 1.4426950408889634
VMEM_LIMIT = 60 * 1024 * 1024
Q_ROWS = 256
K_ROWS = 512
MESH = pl.DeviceIdType.MESH
TILE = 128
N_CHUNKS = 9
N_EARLY = 5
PART = 1


def rope_frequencies(head_dim):
    lane = jnp.arange(head_dim, dtype=jnp.int32)
    return ROPE_BASE ** (-2.0 * (lane % (head_dim // 2)).astype(jnp.float32) / head_dim)


class Links:
    def __init__(self, weights, recv, send_sems, recv_sems, n_tiles):
        self.y, self.c = lax.axis_index("tp"), lax.axis_index("cp")
        self.peer = {
            "y": {"tp": 1 - self.y},
            "x": {"cp": lax.rem(self.c + 2, 4)},
            "d": {"cp": self.c + 1 - 2 * lax.rem(self.c, 2)},
        }
        self.weights, self.recv, self.send_sems, self.recv_sems = weights, recv, send_sems, recv_sems
        self.n_tiles = n_tiles
        self.started = []

    def barrier(self):
        sem = pltpu.get_barrier_semaphore()
        for name in "yxd":
            pl.semaphore_signal(sem, inc=1, device_id=self.peer[name], device_id_type=MESH)
        pl.semaphore_wait(sem, 3)

    def remote(self, src, dst, ssem, rsem, to):
        return pltpu.make_async_remote_copy(src_ref=src, dst_ref=dst, send_sem=ssem, recv_sem=rsem, device_id=self.peer[to], device_id_type=MESH)

    def chunk(self, stage, j, arrays=slice(0, 3)):
        to = "yxdd"[stage]
        copies = []
        for a in range(3)[arrays]:
            if stage == 0:
                w = self.weights[a]
                if a == 2:
                    src = w.at[pl.ds(pl.multiple_of((4 * j + self.c) * TILE, TILE), TILE), :]
                else:
                    depth = w.shape[0] // 4
                    src = w.at[pl.ds(pl.multiple_of(self.c * depth, TILE), depth), pl.ds(4 * j * TILE, 4 * TILE)]
            else:
                src = self.recv[a].at[j, (0, 0, 0, 1)[stage]]
            copies.append(self.remote(src, self.recv[a].at[j, stage], self.send_sems.at[j, stage, a], self.recv_sems.at[j, stage, a], to))
        return copies

    def last_chunk(self, stage, last, arrays=slice(0, 3)):
        half = lax.rem(self.c, 2)
        begin = (self.n_tiles // 4) * 4 * TILE
        copies = []
        for a in range(3)[arrays]:
            depth = last[a].shape[0] // 2
            at = pl.ds(pl.multiple_of(half * depth, 64), depth)
            dst = last[a].at[at, :]
            if stage == 2:
                src = dst
            elif a == 2:
                src = self.weights[a].at[pl.ds(pl.multiple_of(begin + half * depth, 64), depth), :]
            else:
                src = self.weights[a].at[at, pl.ds(begin, last[a].shape[1])]
            j = N_CHUNKS - 1
            copies.append(self.remote(src, dst, self.send_sems.at[j, stage, a], self.recv_sems.at[j, stage, a], "y.d"[stage]))
        return copies

    def pass_on(self, j, here=0):
        for a in range(3):
            if a >= here:
                self.arrived(0, j, slice(a, a + 1))
            self.start(1, j, slice(a, a + 1))
            self.start(2, j, slice(a, a + 1))

    def pass_second(self, j):
        for first, over_d in zip(self.chunk(1, j), self.chunk(3, j)):
            first.wait_recv()
            over_d.start()

    def start(self, stage, j, arrays=slice(0, 3)):
        for copy in self.chunk(stage, j, arrays):
            copy.start()

    def arrived(self, stage, j, arrays=slice(0, 3)):
        for copy in self.chunk(stage, j, arrays):
            copy.wait_recv()

    def sent(self, stage, j, arrays=slice(0, 3)):
        for copy in self.chunk(stage, j, arrays):
            copy.wait_send()


EARLY_FORWARD = ((0, 15), (1, 18), (2, 20), (3, 22))
EARLY_SECOND = ((0, 19), (1, 21), (2, 23))
SLOT_SOURCE = (0, 0, 0, 1)


def normed_rows(wide, gain):
    inv_rms = lax.rsqrt(jnp.mean(wide * wide, axis=-1, keepdims=True) + NORM_EPS)
    return (wide * inv_rms * gain).astype(jnp.bfloat16)


def attention_kernel(x_ref, gain_ref, freq_ref, wq_ref, wk_ref, wv_ref, wo_ref, w1_ref, w3_ref, w2_ref,
                     o_ref, kc_ref, vc_ref, ro_ref, r1_ref, r3_ref, r2_ref,
                     cos_ref, sin_ref, a_sc, q_sc, wq_sc, wk_sc, wv_sc, kv_buf, m_sc, l_sc, acc_sc, send_sems, recv_sems, kv_send, kv_recv, wt_send, wt_recv):
    head_dim = 128
    half_dim = head_dim // 2
    chunk_len = x_ref.shape[0]
    heads = wq_ref.shape[0]
    chains = 2
    per_chain = heads // chains
    rows = per_chain * Q_ROWS
    q_blocks = chunk_len // Q_ROWS
    coef = head_dim ** -0.5 * LOG2E
    net = Links((w1_ref, w3_ref, w2_ref), (r1_ref, r3_ref, r2_ref), send_sems, recv_sems, w1_ref.shape[1] // TILE)
    y, c = net.y, net.c
    core_lower = lax.rem(c + y, 2)
    chip_lower = lax.rem(c // 2 + y, 2)
    other_chip = lax.rem(c + 2, 4)

    def kv_copy(n, hd):
        src, dst, to = ((0, 1, "x"), (0, 2, "d"), (1, 3, "d"), (0, 4, "y"), (4, 5, "x"), (4, 6, "d"), (5, 7, "d"))[n]
        return net.remote(kv_buf.at[src, hd], kv_buf.at[dst, hd], kv_send.at[n, hd], kv_recv.at[n, hd], to)

    def weight_copy(kind, stage):
        own, held = ((wk_ref, wk_sc), (wv_ref, wv_sc), (wq_ref, wq_sc), (wo_ref, ro_ref))[kind]
        quarter = own.shape[-2] // 4
        sl = pl.ds(pl.multiple_of((other_chip if stage == 3 else c) * quarter, 64), quarter)
        src = own if stage == 0 else held
        pick = (lambda r: r.at[sl, :]) if kind == 3 else (lambda r: r.at[:, sl, :])
        return net.remote(pick(src), pick(held), wt_send.at[kind, stage], wt_recv.at[kind, stage], "yxdd"[stage])

    def weights_start(kinds, stage):
        for kind in kinds:
            weight_copy(kind, stage).start()

    def weights_arrived(kinds, stage):
        for kind in kinds:
            weight_copy(kind, stage).wait_recv()

    def row_slice(i):
        return pl.ds(pl.multiple_of(i * Q_ROWS, Q_ROWS), Q_ROWS)

    def rope(t, sl):
        return (t * cos_ref[sl, :] + pltpu.roll(t, half_dim, 1) * sin_ref[sl, :]).astype(jnp.bfloat16)

    def norm_x():
        def body(i, carry):
            sl = row_slice(i)
            row = (y * (7 - 2 * c) + c) * chunk_len + i * Q_ROWS + lax.broadcasted_iota(jnp.int32, (Q_ROWS, head_dim), 0)
            angles = row.astype(jnp.float32) * freq_ref[...][None, :]
            sine_tab = jnp.sin(angles)
            cos_ref[sl, :] = jnp.cos(angles)
            sin_ref[sl, :] = jnp.where(lax.broadcasted_iota(jnp.int32, (Q_ROWS, head_dim), 1) < half_dim, -sine_tab, sine_tab)
            a_sc[sl, :] = normed_rows(x_ref[sl, :].astype(jnp.float32), gain_ref[...].astype(jnp.float32)[None, :])
            return carry
        lax.fori_loop(0, q_blocks, body, 0)

    def make_kv(k_ref, v_ref, hd):
        def body(i, carry):
            sl = row_slice(i)
            w = jnp.concatenate([k_ref[0], v_ref[0]], axis=1)
            proj = jnp.dot(a_sc[sl, :], w, preferred_element_type=jnp.float32)
            kv_buf[0, hd, 0, sl, :] = rope(proj[:, :head_dim], sl)
            kv_buf[0, hd, 1, sl, :] = proj[:, head_dim:].astype(jnp.bfloat16)
            return carry
        lax.fori_loop(0, q_blocks, body, 0)

    def make_q(w_ref, hd):
        def body(i, carry):
            sl = row_slice(i)
            w = jnp.concatenate([w_ref[h] for h in range(heads)], axis=1)
            proj = jnp.dot(a_sc[sl, :], w, preferred_element_type=jnp.float32)
            for h in range(heads):
                cols = slice(h * head_dim, (h + 1) * head_dim)
                q_sc[hd, sl, cols] = rope(proj[:, cols], sl)
            return carry
        lax.fori_loop(0, q_blocks, body, 0)

    net.barrier()
    weights_start((0, 1, 2), 0)
    norm_x()
    make_kv(wk_ref, wv_ref, 0)
    m_sc[...] = jnp.full_like(m_sc, MASK_VALUE)
    l_sc[...] = jnp.zeros_like(l_sc)
    acc_sc[...] = jnp.zeros_like(acc_sc)
    weights_arrived((0, 1), 0)
    weights_start((0, 1), 1)
    weights_start((0, 1), 2)
    kv_copy(1, 0).start()
    kv_copy(0, 0).start()
    kv_copy(3, 0).start()
    make_q(wq_ref, 0)

    def block(q_parts, state, start, slot, head, off, masked):
        k_blk = kv_buf[slot, head, 0, pl.ds(off, K_ROWS), :]
        v_blk = kv_buf[slot, head, 1, pl.ds(off, K_ROWS), :]
        for a in range(chains):
            s = lax.dot_general(q_parts[a], k_blk, (((1,), (1,)), ((), ())), preferred_element_type=jnp.float32)
            if masked:
                q_pos = start + lax.rem(lax.broadcasted_iota(jnp.int32, (rows, K_ROWS), 0), Q_ROWS)
                k_pos = off + lax.broadcasted_iota(jnp.int32, (rows, K_ROWS), 1)
                s = jnp.where(k_pos <= q_pos, s, MASK_VALUE)
            m_prev = m_sc[state, a]
            m_new = jnp.maximum(m_prev, jnp.max(s, axis=1, keepdims=True))
            alpha = jnp.exp2((m_prev - m_new) * coef)
            mc = m_new * coef
            sums = l_sc[state, a] * alpha
            p_tiles = []
            for j in range(K_ROWS // 128):
                p = jnp.exp2(s[:, j * 128:(j + 1) * 128] * coef - mc)
                sums = sums + p
                p_tiles.append(p.astype(jnp.bfloat16))
            l_sc[state, a] = sums
            m_sc[state, a] = m_new
            p_all = jnp.concatenate(p_tiles, axis=1)
            acc_sc[state, a] = acc_sc[state, a] * alpha + jnp.dot(p_all, v_blk, preferred_element_type=jnp.float32)

    def load_q(head, qb):
        sl = row_slice(qb)
        return [jnp.concatenate([q_sc[head, sl, (a * per_chain + h) * head_dim:(a * per_chain + h + 1) * head_dim] for h in range(per_chain)], axis=0) for a in range(chains)]

    per_piece = chunk_len // K_ROWS

    def step(s, carry):
        phase = s // q_blocks
        qb = lax.rem(s, q_blocks)
        is_last = phase // 4
        is_mid = (1 - is_last) * lax.rem(phase, 2)
        is_first = 1 - is_last - is_mid
        head = (1 - is_last) * (phase // 2) + is_last * (phase - 4)
        state = head * q_blocks + qb

        @pl.when(s == 0)
        def _():
            kv_copy(1, 0).wait_recv()

        @pl.when(s == 1)
        def _():
            weights_arrived((0, 1), 1)
            weights_start((0, 1), 3)

        @pl.when(s == 2)
        def _():
            weights_arrived((0, 1), 2)
            weights_arrived((0, 1), 3)
            make_kv(wk_sc, wv_sc, 1)
            weights_arrived((2,), 0)
            weights_start((2,), 1)
            weights_start((2,), 2)

        @pl.when(s == 3)
        def _():
            kv_copy(1, 1).start()
            kv_copy(0, 1).start()
            kv_copy(3, 1).start()
            weights_start((3,), 0)
            net.start(0, 0)
            net.start(0, 1)
            kv_copy(0, 0).wait_recv()
            kv_copy(2, 0).start()

        @pl.when(s == 4)
        def _():
            kv_copy(2, 0).wait_recv()

        @pl.when(s == 6)
        def _():
            weights_arrived((2,), 1)
            weights_start((2,), 3)
            kv_copy(3, 0).wait_recv()
            kv_copy(4, 0).start()
            kv_copy(5, 0).start()

        @pl.when(s == 7)
        def _():
            weights_arrived((2,), 2)
            weights_arrived((2,), 3)
            make_q(wq_sc, 1)

        @pl.when(s == 8)
        def _():
            kv_copy(1, 1).wait_recv()

        @pl.when(s == 9)
        def _():
            kv_copy(0, 1).wait_recv()
            kv_copy(2, 1).start()

        @pl.when(s == 10)
        def _():
            kv_copy(3, 1).wait_recv()
            kv_copy(4, 1).start()
            kv_copy(5, 1).start()

        @pl.when(s == 12)
        def _():
            kv_copy(2, 1).wait_recv()
            weights_arrived((3,), 0)
            weights_start((3,), 1)
            weights_start((3,), 2)

        @pl.when(s == 13)
        def _():
            kv_copy(4, 0).wait_recv()
            kv_copy(6, 0).start()

        @pl.when(s == 14)
        def _():
            kv_copy(4, 1).wait_recv()
            kv_copy(6, 1).start()

        @pl.when(s == 16)
        def _():
            for hd in range(2):
                kv_copy(5, hd).wait_recv()
                kv_copy(6, hd).wait_recv()
            weights_arrived((3,), 1)
            weights_start((3,), 3)

        for j, when in EARLY_FORWARD:
            @pl.when(s == when)
            def _(j=j):
                net.pass_on(j)
                if j + 2 < N_EARLY:
                    net.start(0, j + 2)
                elif j + 2 == N_EARLY:
                    net.start(0, N_EARLY, slice(0, PART))

        for j, when in EARLY_SECOND:
            @pl.when(s == when)
            def _(j=j):
                net.pass_second(j)

        q_parts = load_q(head, qb)
        start = qb * Q_ROWS
        diag = start // K_ROWS
        count = is_first * (diag + per_piece * core_lower) + is_mid * 2 * per_piece * chip_lower + is_last * 4 * per_piece * y
        kv_head = head + is_last * (1 - 2 * head)

        def inner(i, carry):
            in_core = (i >= diag).astype(jnp.int32)
            idx = i - is_first * in_core * diag
            slot = is_first * 2 * in_core + is_mid * (1 + 2 * (i // per_piece)) + is_last * (4 + i // per_piece)
            off = (is_first * (in_core * lax.rem(idx, per_piece) + (1 - in_core) * i) + (1 - is_first) * lax.rem(i, per_piece)) * K_ROWS
            block(q_parts, state, start, slot, kv_head, pl.multiple_of(off, K_ROWS), False)
            return carry

        lax.fori_loop(0, count, inner, 0)

        @pl.when(is_first == 1)
        def _():
            block(q_parts, state, start, 0, head, pl.multiple_of(diag * K_ROWS, K_ROWS), True)

        return carry

    lax.fori_loop(0, 6 * q_blocks, step, 0)

    def finish(state, carry):
        head = state // q_blocks
        sl = row_slice(lax.rem(state, q_blocks))
        for a in range(chains):
            total = jnp.sum(l_sc[state, a], axis=1, keepdims=True)
            out = (acc_sc[state, a] / total).astype(jnp.bfloat16)
            for h in range(per_chain):
                o_ref[head, sl, (a * per_chain + h) * head_dim:(a * per_chain + h + 1) * head_dim] = out[h * Q_ROWS:(h + 1) * Q_ROWS]
        return carry

    lax.fori_loop(0, 2 * q_blocks, finish, 0)

    for e in range(2):
        late = c // 2
        owner = (1 - late) * (2 * c + e) + late * (7 - 2 * c - e)
        cross = lax.rem(late + y, 2)
        slot = 4 * cross + 2 * lax.rem(owner + c, 2) + lax.rem(owner // 2 + c // 2, 2)
        kc_ref[e * chunk_len:(e + 1) * chunk_len] = kv_buf[slot, cross, 0]
        vc_ref[e * chunk_len:(e + 1) * chunk_len] = kv_buf[slot, cross, 1]

    weights_arrived((3,), 2)
    weights_arrived((3,), 3)
    for hd in range(2):
        for n in range(7):
            kv_copy(n, hd).wait_send()
    for kind in range(4):
        for stage in range(4):
            weight_copy(kind, stage).wait_send()
    forwarded = [j for j, _ in EARLY_FORWARD]
    second = [j for j, _ in EARLY_SECOND]
    for j in range(N_EARLY):
        if j not in forwarded:
            net.arrived(0, j)
        net.sent(0, j)
    net.arrived(0, N_EARLY, slice(0, PART))
    net.sent(0, N_EARLY, slice(0, PART))
    for j in forwarded:
        if j not in second:
            net.arrived(1, j)
        net.arrived(2, j)
        net.sent(1, j)
        net.sent(2, j)
    for j in second:
        net.arrived(3, j)
        net.sent(3, j)


def attention(x, gain, freq, wq, wk, wv, wo, w1, w3, w2):
    rows, dim = x.shape
    width = wq.shape[0] * 128
    states = 2 * rows // Q_ROWS
    m_rows = width // 128 // 2 * Q_ROWS
    vm = pl.BlockSpec(memory_space=pltpu.VMEM)
    hbm = pl.BlockSpec(memory_space=pl.ANY)
    bf16 = jnp.bfloat16
    n = N_EARLY + 1
    return pl.pallas_call(
        attention_kernel,
        in_specs=[vm] * 6 + [hbm] * 4,
        out_specs=[vm, vm, vm, hbm, hbm, hbm, hbm],
        out_shape=[
            jax.ShapeDtypeStruct((2, rows, width), bf16),
            jax.ShapeDtypeStruct((2 * rows, 128), bf16),
            jax.ShapeDtypeStruct((2 * rows, 128), bf16),
            jax.ShapeDtypeStruct(wo.shape, bf16),
            jax.ShapeDtypeStruct((N_CHUNKS - 1, 4, dim // 4, 4 * TILE), bf16),
            jax.ShapeDtypeStruct((N_CHUNKS - 1, 4, dim // 4, 4 * TILE), bf16),
            jax.ShapeDtypeStruct((N_CHUNKS - 1, 4, TILE, dim), bf16),
        ],
        scratch_shapes=[
            pltpu.VMEM((rows, 128), jnp.float32),
            pltpu.VMEM((rows, 128), jnp.float32),
            pltpu.VMEM((rows, dim), bf16),
            pltpu.VMEM((2, rows, width), bf16),
            pltpu.VMEM(wq.shape, bf16),
            pltpu.VMEM(wk.shape, bf16),
            pltpu.VMEM(wv.shape, bf16),
            pltpu.VMEM((8, 2, 2, rows, 128), bf16),
            pltpu.VMEM((states, 2, m_rows, 128), jnp.float32),
            pltpu.VMEM((states, 2, m_rows, 128), jnp.float32),
            pltpu.VMEM((states, 2, m_rows, 128), jnp.float32),
            pltpu.SemaphoreType.DMA((n, 4, 3)),
            pltpu.SemaphoreType.DMA((n, 4, 3)),
            pltpu.SemaphoreType.DMA((7, 2)),
            pltpu.SemaphoreType.DMA((7, 2)),
            pltpu.SemaphoreType.DMA((4, 4)),
            pltpu.SemaphoreType.DMA((4, 4)),
        ],
        compiler_params=pltpu.CompilerParams(collective_id=0, has_side_effects=True, vmem_limit_bytes=VMEM_LIMIT),
        cost_estimate=pl.CostEstimate(flops=16 * rows * 4096 * width, bytes_accessed=32 * 2**20, transcendentals=rows * 4096 * 12),
        name="attention",
    )(x, gain, freq, wq, wk, wv, wo, w1, w3, w2)


M_BLOCK = 512
LATE_FORWARD = {3: (5,), 7: (6,), 11: (7,)}
LATE_SECOND = {3: (4,), 8: (5,), 12: (6,)}
END_SECOND = {15: (7,)}
LOAD_AFTER = 15
STEPS = 2 * N_CHUNKS - 1


def mlp_kernel(x_ref, gain_ref, o_ref, wo_ref, ro_ref, w1_ref, w3_ref, w2_ref, a1_ref, a3_ref, a2_ref, out_ref, hid_ref, r1_ref, r3_ref, r2_ref, e1_ref, e3_ref, e2_ref,
               w1_sc, w3_sc, w2_sc, b_ref, acc_sc, hid_sc, load_sems, store_sems, send_sems, recv_sems):
    dim = x_ref.shape[1]
    width = 4 * TILE
    n_tiles = w1_ref.shape[1] // TILE
    net = Links((w1_ref, w3_ref, w2_ref), (r1_ref, r3_ref, r2_ref), send_sems, recv_sems, n_tiles)
    own_last = (n_tiles - 4) * TILE
    ends = (e1_ref, e3_ref, e2_ref)

    def own_loads(j, slot):
        off = min(j * width, own_last) if isinstance(j, int) else pl.multiple_of(jnp.minimum(j * width, own_last), TILE)
        sl = pl.ds(off, width)
        return [
            pltpu.make_async_copy(w1_ref.at[:, sl], w1_sc.at[slot], load_sems.at[slot, 0]),
            pltpu.make_async_copy(w3_ref.at[:, sl], w3_sc.at[slot], load_sems.at[slot, 1]),
            pltpu.make_async_copy(w2_ref.at[sl, :], w2_sc.at[slot], load_sems.at[slot, 2]),
        ]

    def other_loads(j, slot):
        copies = []
        depth = dim // 4
        for p in range(4):
            source = 2 * lax.rem(net.c // 2 + p % 2, 2) + lax.rem(net.c + p // 2, 2)
            deep = pl.ds(pl.multiple_of(source * depth, TILE), depth)
            sl = pl.ds(pl.multiple_of(source * TILE, TILE), TILE)
            copies.append(pltpu.make_async_copy(r1_ref.at[j, p], w1_sc.at[slot, deep, :], load_sems.at[slot, 0]))
            copies.append(pltpu.make_async_copy(r3_ref.at[j, p], w3_sc.at[slot, deep, :], load_sems.at[slot, 1]))
            copies.append(pltpu.make_async_copy(r2_ref.at[j, p], w2_sc.at[slot, sl, :], load_sems.at[slot, 2]))
        return copies

    def end_load(slot, a):
        w = pl.ds(0, e1_ref.shape[1])
        dst = w2_sc.at[slot, w, :] if a == 2 else (w1_sc, w3_sc)[a].at[slot, :, w]
        return pltpu.make_async_copy(ends[a], dst, load_sems.at[slot, a])

    def compute(slot, lane_keep):
        def rows_step(m, carry):
            sl = pl.ds(pl.multiple_of(m * M_BLOCK, M_BLOCK), M_BLOCK)
            b = b_ref[sl, :]
            gate = jnp.dot(b, w1_sc[slot], preferred_element_type=jnp.float32)
            up = jnp.dot(b, w3_sc[slot], preferred_element_type=jnp.float32)
            hidden = jax.nn.silu(gate) * up
            hidden = jnp.where(lane_keep > 0.5, hidden, 0.0).astype(jnp.bfloat16)
            acc_sc[sl, :] += jnp.dot(hidden, w2_sc[slot], preferred_element_type=jnp.float32)
            return carry

        lax.fori_loop(0, b_ref.shape[0] // M_BLOCK, rows_step, 0)

    net.barrier()
    net.start(0, N_EARLY, slice(PART, 3))
    net.start(0, N_EARLY + 1)
    net.start(1, N_EARLY - 1)
    net.start(2, N_EARLY - 1)
    net.start(3, N_EARLY - 2)
    for copy in own_loads(0, 0):
        copy.start()

    def residual_rows(i, carry):
        sl = pl.ds(pl.multiple_of(i * Q_ROWS, Q_ROWS), Q_ROWS)
        attn = jnp.dot(o_ref[0, sl, :], wo_ref[...], preferred_element_type=jnp.float32)
        attn = attn + jnp.dot(o_ref[1, sl, :], ro_ref[...], preferred_element_type=jnp.float32)
        residual = (x_ref[sl, :].astype(jnp.float32) + attn).astype(jnp.bfloat16).astype(jnp.float32)
        acc_sc[sl, :] = residual
        b_ref[sl, :] = normed_rows(residual, gain_ref[...].astype(jnp.float32)[None, :])
        return carry

    lax.fori_loop(0, x_ref.shape[0] // Q_ROWS, residual_rows, 0)
    lane_tile = lax.broadcasted_iota(jnp.int32, (1, width), 1) // TILE

    def pass_on(s, forward, second):
        for when, chunks in forward.items():
            @pl.when(s == when)
            def _(chunks=chunks):
                for j in chunks:
                    net.pass_on(j, PART if j == N_EARLY else 0)
                    if j + 2 < N_CHUNKS - 1:
                        net.start(0, j + 2)
                    elif j + 2 == N_CHUNKS - 1:
                        for copy in net.last_chunk(0, ends):
                            copy.start()
        for when, chunks in second.items():
            @pl.when(s == when)
            def _(chunks=chunks):
                for j in chunks:
                    net.pass_second(j)

    def load_next(s, slot, after):
        for j in range(3, N_CHUNKS - 1):
            if (N_CHUNKS - 1 + j >= LOAD_AFTER) == after:
                @pl.when(s == N_CHUNKS - 1 + j)
                def _(j=j):
                    if j >= 4:
                        net.arrived(2, j)
                    net.arrived(3, j)

        if not after:
            @pl.when(s + 1 < N_CHUNKS)
            def _():
                for copy in own_loads(s + 1, 1 - slot):
                    copy.start()

        if not after:
            @pl.when(s == STEPS - 1)
            def _():
                for a in range(2):
                    net.last_chunk(2, ends, slice(a, a + 1))[0].wait_recv()
                    end_load(1 - slot, a).start()

        first, last = (LOAD_AFTER, STEPS - 1) if after else (N_CHUNKS - 1, LOAD_AFTER)

        @pl.when((s >= first) & (s < last))
        def _():
            for copy in other_loads(s + 1 - N_CHUNKS, 1 - slot):
                copy.start()

    def step(s, carry):
        slot = lax.rem(s, 2)
        pass_on(s, LATE_FORWARD, LATE_SECOND)
        load_next(s, slot, False)
        for copy in own_loads(0, slot):
            copy.wait()

        keep = 1.0 - (s == N_CHUNKS - 1).astype(jnp.float32) * (lane_tile == 0).astype(jnp.float32)
        compute(slot, keep)
        pass_on(s, {}, END_SECOND)

        @pl.when(s == STEPS - 2)
        def _():
            for a in range(2):
                net.last_chunk(0, ends, slice(a, a + 1))[0].wait_recv()
                net.last_chunk(2, ends, slice(a, a + 1))[0].start()

        load_next(s, slot, True)
        return carry

    lax.fori_loop(0, STEPS, step, 0)

    store_sum = pltpu.make_async_copy(acc_sc, out_ref, store_sems.at[0])
    store_sum.start()
    slot = STEPS % 2
    left = e1_ref.shape[1]
    net.last_chunk(0, ends, slice(2, 3))[0].wait_recv()
    net.last_chunk(2, ends, slice(2, 3))[0].start()
    for a in range(2):
        end_load(slot, a).wait()

    def hidden_rows(m, carry):
        sl = pl.ds(pl.multiple_of(m * M_BLOCK, M_BLOCK), M_BLOCK)
        gate = jnp.dot(b_ref[sl, :], w1_sc[slot, :, :left], preferred_element_type=jnp.float32)
        up = jnp.dot(b_ref[sl, :], w3_sc[slot, :, :left], preferred_element_type=jnp.float32)
        hid_sc[sl, :] = (jax.nn.silu(gate) * up).astype(jnp.bfloat16)
        return carry

    lax.fori_loop(0, x_ref.shape[0] // M_BLOCK, hidden_rows, 0)
    store_hidden = pltpu.make_async_copy(hid_sc, hid_ref, store_sems.at[1])
    store_hidden.start()
    net.last_chunk(2, ends, slice(2, 3))[0].wait_recv()
    store_sum.wait()
    store_hidden.wait()
    net.sent(0, N_EARLY, slice(PART, 3))
    for j in range(N_EARLY + 1, N_CHUNKS - 1):
        net.sent(0, j)
    for j in range(N_EARLY - 1, N_CHUNKS - 1):
        net.sent(1, j)
        net.sent(2, j)
    for j in range(N_EARLY - 2, N_CHUNKS - 1):
        net.sent(3, j)
    for stage in (0, 2):
        for copy in net.last_chunk(stage, ends):
            copy.wait_send()


def mlp(x, gain, o, wo, ro, w1, w3, w2, early):
    rows, dim = x.shape
    vm = pl.BlockSpec(memory_space=pltpu.VMEM)
    hbm = pl.BlockSpec(memory_space=pl.ANY)
    bf16 = jnp.bfloat16
    width = 4 * TILE
    left = w1.shape[1] % width
    n = N_CHUNKS
    return pl.pallas_call(
        mlp_kernel,
        in_specs=[vm] * 5 + [hbm] * 6,
        out_specs=[hbm] * 8,
        out_shape=[jax.ShapeDtypeStruct((rows, dim), jnp.float32), jax.ShapeDtypeStruct((rows, left), bf16)] + [jax.ShapeDtypeStruct(a.shape, bf16) for a in early] + [jax.ShapeDtypeStruct(s, bf16) for s in ((dim, left), (dim, left), (left, dim))],
        input_output_aliases={8: 2, 9: 3, 10: 4},
        scratch_shapes=[
            pltpu.VMEM((2, dim, width), bf16),
            pltpu.VMEM((2, dim, width), bf16),
            pltpu.VMEM((2, width, dim), bf16),
            pltpu.VMEM((rows, dim), bf16),
            pltpu.VMEM((rows, dim), jnp.float32),
            pltpu.VMEM((rows, left), bf16),
            pltpu.SemaphoreType.DMA((2, 3)),
            pltpu.SemaphoreType.DMA((2,)),
            pltpu.SemaphoreType.DMA((n, 4, 3)),
            pltpu.SemaphoreType.DMA((n, 4, 3)),
        ],
        compiler_params=pltpu.CompilerParams(collective_id=1, has_side_effects=True, vmem_limit_bytes=VMEM_LIMIT),
        cost_estimate=pl.CostEstimate(flops=12 * rows * dim * w1.shape[1], bytes_accessed=12 * dim * w1.shape[1], transcendentals=2 * rows * w1.shape[1]),
        name="mlp",
    )(x, gain, o, wo, ro, w1, w3, w2, *early)


def last_kernel(sum_ref, hid_ref, w2_ref, kc_ref, vc_ref, out_ref, k_ref, v_ref):
    out_ref[...] = (sum_ref[...] + jnp.dot(hid_ref[...], w2_ref[...], preferred_element_type=jnp.float32)).astype(out_ref.dtype)
    k_ref[...] = kc_ref[...]
    v_ref[...] = vc_ref[...]


def last_product(total, hidden, w2, k_cache, v_cache):
    rows, dim = total.shape
    steps = rows // Q_ROWS

    def by_rows(a):
        return pl.BlockSpec((a.shape[0] // steps, a.shape[1]), lambda i: (i, 0))

    out = jax.ShapeDtypeStruct((rows, dim), jnp.bfloat16)
    return pl.pallas_call(
        last_kernel,
        grid=(steps,),
        in_specs=[by_rows(total), by_rows(hidden), pl.BlockSpec(w2.shape, lambda i: (0, 0)), by_rows(k_cache), by_rows(v_cache)],
        out_specs=[by_rows(out), by_rows(k_cache), by_rows(v_cache)],
        out_shape=[out, jax.ShapeDtypeStruct(k_cache.shape, k_cache.dtype), jax.ShapeDtypeStruct(v_cache.shape, v_cache.dtype)],
        cost_estimate=pl.CostEstimate(flops=2 * rows * dim * w2.shape[0], bytes_accessed=6 * rows * dim, transcendentals=0),
        name="last_product",
    )(total, hidden, w2, k_cache, v_cache)

def solution(mesh):
    def layer_shard(x_loc, norm_attn, norm_mlp, w_query, w_key, w_value, w_out, w_gate, w_up, w_down):
        wq, wk, wv = (jnp.transpose(w, (1, 0, 2)) for w in (w_query, w_key, w_value))
        wo = w_out.reshape(-1, w_out.shape[2])
        o, k_cache, v_cache, wo_other, *early = attention(x_loc, norm_attn, rope_frequencies(w_query.shape[2]), wq, wk, wv, wo, w_gate, w_up, w_down)
        total, hidden, *_, last_w2 = mlp(x_loc, norm_mlp, o, wo, wo_other, w_gate, w_up, w_down, early)
        return tuple(last_product(total, hidden, last_w2, k_cache, v_cache))

    row_spec = P(("dp", "cp", "tp"), None)
    cache_spec = P(("dp", "cp"), "tp")
    head_spec = P(None, "tp", None)
    return jax.shard_map(
        layer_shard,
        mesh=mesh,
        in_specs=(row_spec, P(None), P(None), head_spec, head_spec, head_spec, P("tp", None, None), P(None, "tp"), P(None, "tp"), P("tp", None)),
        out_specs=(row_spec, cache_spec, cache_spec),
        check_vma=False,
    )
```

```python
import functools

import jax
import jax.numpy as jnp
from jax import lax
from jax.experimental import pallas as pl
from jax.experimental.pallas import tpu as pltpu
from jax.sharding import PartitionSpec as P

ROPE_BASE = 500000.0
NORM_EPS = 1e-5
MASK_VALUE = -1e30
LOG2E = 1.4426950408889634
VMEM_LIMIT = 60 * 1024 * 1024
Q_ROWS = 256
K_ROWS = 512
MESH = pl.DeviceIdType.MESH
TILE = 128
N_CHUNKS = 9
N_EARLY = 5
PART = 1


def rope_frequencies(head_dim):
    lane = jnp.arange(head_dim, dtype=jnp.int32)
    return ROPE_BASE ** (-2.0 * (lane % (head_dim // 2)).astype(jnp.float32) / head_dim)


class Links:
    def __init__(self, weights, recv, send_sems, recv_sems, n_tiles):
        self.y, self.c = lax.axis_index("tp"), lax.axis_index("cp")
        self.peer = {
            "y": {"tp": 1 - self.y},
            "x": {"cp": lax.rem(self.c + 2, 4)},
            "d": {"cp": self.c + 1 - 2 * lax.rem(self.c, 2)},
        }
        self.weights, self.recv, self.send_sems, self.recv_sems = weights, recv, send_sems, recv_sems
        self.n_tiles = n_tiles
        self.started = []

    def barrier(self):
        sem = pltpu.get_barrier_semaphore()
        for name in "yxd":
            pl.semaphore_signal(sem, inc=1, device_id=self.peer[name], device_id_type=MESH)
        pl.semaphore_wait(sem, 3)

    def remote(self, src, dst, ssem, rsem, to):
        return pltpu.make_async_remote_copy(src_ref=src, dst_ref=dst, send_sem=ssem, recv_sem=rsem, device_id=self.peer[to], device_id_type=MESH)

    def chunk(self, stage, j, arrays=slice(0, 3)):
        to = "yxdd"[stage]
        copies = []
        for a in range(3)[arrays]:
            if stage == 0:
                w = self.weights[a]
                if a == 2:
                    src = w.at[pl.ds(pl.multiple_of((4 * j + self.c) * TILE, TILE), TILE), :]
                else:
                    depth = w.shape[0] // 4
                    src = w.at[pl.ds(pl.multiple_of(self.c * depth, TILE), depth), pl.ds(4 * j * TILE, 4 * TILE)]
            else:
                src = self.recv[a].at[j, (0, 0, 0, 1)[stage]]
            copies.append(self.remote(src, self.recv[a].at[j, stage], self.send_sems.at[j, stage, a], self.recv_sems.at[j, stage, a], to))
        return copies

    def last_chunk(self, stage, last, arrays=slice(0, 3)):
        half = lax.rem(self.c, 2)
        begin = (self.n_tiles // 4) * 4 * TILE
        copies = []
        for a in range(3)[arrays]:
            depth = last[a].shape[0] // 2
            at = pl.ds(pl.multiple_of(half * depth, 64), depth)
            dst = last[a].at[at, :]
            if stage == 2:
                src = dst
            elif a == 2:
                src = self.weights[a].at[pl.ds(pl.multiple_of(begin + half * depth, 64), depth), :]
            else:
                src = self.weights[a].at[at, pl.ds(begin, last[a].shape[1])]
            j = N_CHUNKS - 1
            copies.append(self.remote(src, dst, self.send_sems.at[j, stage, a], self.recv_sems.at[j, stage, a], "y.d"[stage]))
        return copies

    def pass_on(self, j, here=0):
        for a in range(3):
            if a >= here:
                self.arrived(0, j, slice(a, a + 1))
            self.start(1, j, slice(a, a + 1))
            self.start(2, j, slice(a, a + 1))

    def pass_second(self, j):
        for first, over_d in zip(self.chunk(1, j), self.chunk(3, j)):
            first.wait_recv()
            over_d.start()

    def start(self, stage, j, arrays=slice(0, 3)):
        for copy in self.chunk(stage, j, arrays):
            copy.start()

    def arrived(self, stage, j, arrays=slice(0, 3)):
        for copy in self.chunk(stage, j, arrays):
            copy.wait_recv()

    def sent(self, stage, j, arrays=slice(0, 3)):
        for copy in self.chunk(stage, j, arrays):
            copy.wait_send()


EARLY_FORWARD = ((0, 15), (1, 18), (2, 20), (3, 22))
EARLY_SECOND = ((0, 19), (1, 21), (2, 23))
SLOT_SOURCE = (0, 0, 0, 1)


def normed_rows(wide, gain):
    inv_rms = lax.rsqrt(jnp.mean(wide * wide, axis=-1, keepdims=True) + NORM_EPS)
    return (wide * inv_rms * gain).astype(jnp.bfloat16)


def attention_kernel(x_hbm, gain_ref, freq_ref, wq_hbm, wk_hbm, wv_hbm, wo_ref, w1_ref, w3_ref, w2_ref,
                     o_hbm, kc_ref, vc_ref, ro_ref, r1_ref, r3_ref, r2_ref,
                     x_ref, wq_ref, wk_ref, wv_ref, o_ref, local_sems, cos_ref, sin_ref, a_sc, q_sc, wq_sc, wk_sc, wv_sc, kv_buf, m_sc, l_sc, acc_sc, send_sems, recv_sems, kv_send, kv_recv, wt_send, wt_recv):
    head_dim = 128
    half_dim = head_dim // 2
    chunk_len = x_ref.shape[0]
    heads = wq_ref.shape[0]
    chains = 2
    per_chain = heads // chains
    rows = per_chain * Q_ROWS
    q_blocks = chunk_len // Q_ROWS
    coef = head_dim ** -0.5 * LOG2E
    net = Links((w1_ref, w3_ref, w2_ref), (r1_ref, r3_ref, r2_ref), send_sems, recv_sems, w1_ref.shape[1] // TILE)
    y, c = net.y, net.c
    core_lower = lax.rem(c + y, 2)
    chip_lower = lax.rem(c // 2 + y, 2)
    other_chip = lax.rem(c + 2, 4)

    def kv_copy(n, hd):
        src, dst, to = ((0, 1, "x"), (0, 2, "d"), (1, 3, "d"), (0, 4, "y"), (4, 5, "x"), (4, 6, "d"), (5, 7, "d"))[n]
        return net.remote(kv_buf.at[src, hd], kv_buf.at[dst, hd], kv_send.at[n, hd], kv_recv.at[n, hd], to)

    def weight_copy(kind, stage):
        own, held = ((wk_hbm, wk_sc), (wv_hbm, wv_sc), (wq_hbm, wq_sc), (wo_ref, ro_ref))[kind]
        quarter = own.shape[-2] // 4
        sl = pl.ds(pl.multiple_of((other_chip if stage == 3 else c) * quarter, 64), quarter)
        src = own if stage == 0 else held
        pick = (lambda r: r.at[sl, :]) if kind == 3 else (lambda r: r.at[:, sl, :])
        return net.remote(pick(src), pick(held), wt_send.at[kind, stage], wt_recv.at[kind, stage], "yxdd"[stage])

    def weights_start(kinds, stage):
        for kind in kinds:
            weight_copy(kind, stage).start()

    def weights_arrived(kinds, stage):
        for kind in kinds:
            weight_copy(kind, stage).wait_recv()

    def row_slice(i):
        return pl.ds(pl.multiple_of(i * Q_ROWS, Q_ROWS), Q_ROWS)

    def rope(t, sl):
        return (t * cos_ref[sl, :] + pltpu.roll(t, half_dim, 1) * sin_ref[sl, :]).astype(jnp.bfloat16)

    def norm_x():
        def body(i, carry):
            sl = row_slice(i)
            row = (y * (7 - 2 * c) + c) * chunk_len + i * Q_ROWS + lax.broadcasted_iota(jnp.int32, (Q_ROWS, head_dim), 0)
            angles = row.astype(jnp.float32) * freq_ref[...][None, :]
            sine_tab = jnp.sin(angles)
            cos_ref[sl, :] = jnp.cos(angles)
            sin_ref[sl, :] = jnp.where(lax.broadcasted_iota(jnp.int32, (Q_ROWS, head_dim), 1) < half_dim, -sine_tab, sine_tab)
            a_sc[sl, :] = normed_rows(x_ref[sl, :].astype(jnp.float32), gain_ref[...].astype(jnp.float32)[None, :])
            return carry
        lax.fori_loop(0, q_blocks, body, 0)

    def make_kv(k_ref, v_ref, hd):
        def body(i, carry):
            sl = row_slice(i)
            w = jnp.concatenate([k_ref[0], v_ref[0]], axis=1)
            proj = jnp.dot(a_sc[sl, :], w, preferred_element_type=jnp.float32)
            kv_buf[0, hd, 0, sl, :] = rope(proj[:, :head_dim], sl)
            kv_buf[0, hd, 1, sl, :] = proj[:, head_dim:].astype(jnp.bfloat16)
            return carry
        lax.fori_loop(0, q_blocks, body, 0)

    def make_q(w_ref, hd):
        def body(i, carry):
            sl = row_slice(i)
            w = jnp.concatenate([w_ref[h] for h in range(heads)], axis=1)
            proj = jnp.dot(a_sc[sl, :], w, preferred_element_type=jnp.float32)
            for h in range(heads):
                cols = slice(h * head_dim, (h + 1) * head_dim)
                q_sc[hd, sl, cols] = rope(proj[:, cols], sl)
            return carry
        lax.fori_loop(0, q_blocks, body, 0)

    loads = [pltpu.make_async_copy(*pair, local_sems.at[n]) for n, pair in enumerate(((x_hbm, x_ref), (wk_hbm, wk_ref), (wv_hbm, wv_ref), (wq_hbm, wq_ref)))]
    for load in loads:
        load.start()
    net.barrier()
    weights_start((0, 1, 2), 0)
    loads[0].wait()
    norm_x()
    loads[1].wait()
    loads[2].wait()
    make_kv(wk_ref, wv_ref, 0)
    m_sc[...] = jnp.full_like(m_sc, MASK_VALUE)
    l_sc[...] = jnp.zeros_like(l_sc)
    acc_sc[...] = jnp.zeros_like(acc_sc)
    weights_arrived((0, 1), 0)
    weights_start((0, 1), 1)
    weights_start((0, 1), 2)
    kv_copy(1, 0).start()
    kv_copy(0, 0).start()
    kv_copy(3, 0).start()
    loads[3].wait()
    make_q(wq_ref, 0)

    def block(q_parts, state, start, slot, head, off, masked):
        k_blk = kv_buf[slot, head, 0, pl.ds(off, K_ROWS), :]
        v_blk = kv_buf[slot, head, 1, pl.ds(off, K_ROWS), :]
        for a in range(chains):
            s = lax.dot_general(q_parts[a], k_blk, (((1,), (1,)), ((), ())), preferred_element_type=jnp.float32)
            if masked:
                q_pos = start + lax.rem(lax.broadcasted_iota(jnp.int32, (rows, K_ROWS), 0), Q_ROWS)
                k_pos = off + lax.broadcasted_iota(jnp.int32, (rows, K_ROWS), 1)
                s = jnp.where(k_pos <= q_pos, s, MASK_VALUE)
            m_prev = m_sc[state, a]
            m_new = jnp.maximum(m_prev, jnp.max(s, axis=1, keepdims=True))
            alpha = jnp.exp2((m_prev - m_new) * coef)
            mc = m_new * coef
            sums = l_sc[state, a] * alpha
            p_tiles = []
            for j in range(K_ROWS // 128):
                p = jnp.exp2(s[:, j * 128:(j + 1) * 128] * coef - mc)
                sums = sums + p
                p_tiles.append(p.astype(jnp.bfloat16))
            l_sc[state, a] = sums
            m_sc[state, a] = m_new
            p_all = jnp.concatenate(p_tiles, axis=1)
            acc_sc[state, a] = acc_sc[state, a] * alpha + jnp.dot(p_all, v_blk, preferred_element_type=jnp.float32)

    def load_q(head, qb):
        sl = row_slice(qb)
        return [jnp.concatenate([q_sc[head, sl, (a * per_chain + h) * head_dim:(a * per_chain + h + 1) * head_dim] for h in range(per_chain)], axis=0) for a in range(chains)]

    per_piece = chunk_len // K_ROWS

    def step(s, carry):
        phase = s // q_blocks
        qb = lax.rem(s, q_blocks)
        is_last = phase // 4
        is_mid = (1 - is_last) * lax.rem(phase, 2)
        is_first = 1 - is_last - is_mid
        head = (1 - is_last) * (phase // 2) + is_last * (phase - 4)
        state = head * q_blocks + qb

        @pl.when(s == 0)
        def _():
            kv_copy(1, 0).wait_recv()

        @pl.when(s == 1)
        def _():
            weights_arrived((0, 1), 1)
            weights_start((0, 1), 3)

        @pl.when(s == 2)
        def _():
            weights_arrived((0, 1), 2)
            weights_arrived((0, 1), 3)
            make_kv(wk_sc, wv_sc, 1)
            weights_arrived((2,), 0)
            weights_start((2,), 1)
            weights_start((2,), 2)

        @pl.when(s == 3)
        def _():
            kv_copy(1, 1).start()
            kv_copy(0, 1).start()
            kv_copy(3, 1).start()
            weights_start((3,), 0)
            net.start(0, 0)
            net.start(0, 1)
            kv_copy(0, 0).wait_recv()
            kv_copy(2, 0).start()

        @pl.when(s == 4)
        def _():
            kv_copy(2, 0).wait_recv()

        @pl.when(s == 6)
        def _():
            weights_arrived((2,), 1)
            weights_start((2,), 3)
            kv_copy(3, 0).wait_recv()
            kv_copy(4, 0).start()
            kv_copy(5, 0).start()

        @pl.when(s == 7)
        def _():
            weights_arrived((2,), 2)
            weights_arrived((2,), 3)
            make_q(wq_sc, 1)

        @pl.when(s == 8)
        def _():
            kv_copy(1, 1).wait_recv()

        @pl.when(s == 9)
        def _():
            kv_copy(0, 1).wait_recv()
            kv_copy(2, 1).start()

        @pl.when(s == 10)
        def _():
            kv_copy(3, 1).wait_recv()
            kv_copy(4, 1).start()
            kv_copy(5, 1).start()

        @pl.when(s == 12)
        def _():
            kv_copy(2, 1).wait_recv()
            weights_arrived((3,), 0)
            weights_start((3,), 1)
            weights_start((3,), 2)

        @pl.when(s == 13)
        def _():
            kv_copy(4, 0).wait_recv()
            kv_copy(6, 0).start()

        @pl.when(s == 14)
        def _():
            kv_copy(4, 1).wait_recv()
            kv_copy(6, 1).start()

        @pl.when(s == 16)
        def _():
            for hd in range(2):
                kv_copy(5, hd).wait_recv()
                kv_copy(6, hd).wait_recv()
            weights_arrived((3,), 1)
            weights_start((3,), 3)

        for j, when in EARLY_FORWARD:
            @pl.when(s == when)
            def _(j=j):
                net.pass_on(j)
                if j + 2 < N_EARLY:
                    net.start(0, j + 2)
                elif j + 2 == N_EARLY:
                    net.start(0, N_EARLY, slice(0, PART))

        for j, when in EARLY_SECOND:
            @pl.when(s == when)
            def _(j=j):
                net.pass_second(j)

        q_parts = load_q(head, qb)
        start = qb * Q_ROWS
        diag = start // K_ROWS
        count = is_first * (diag + per_piece * core_lower) + is_mid * 2 * per_piece * chip_lower + is_last * 4 * per_piece * y
        kv_head = head + is_last * (1 - 2 * head)

        def inner(i, carry):
            in_core = (i >= diag).astype(jnp.int32)
            idx = i - is_first * in_core * diag
            slot = is_first * 2 * in_core + is_mid * (1 + 2 * (i // per_piece)) + is_last * (4 + i // per_piece)
            off = (is_first * (in_core * lax.rem(idx, per_piece) + (1 - in_core) * i) + (1 - is_first) * lax.rem(i, per_piece)) * K_ROWS
            block(q_parts, state, start, slot, kv_head, pl.multiple_of(off, K_ROWS), False)
            return carry

        lax.fori_loop(0, count, inner, 0)

        @pl.when(is_first == 1)
        def _():
            block(q_parts, state, start, 0, head, pl.multiple_of(diag * K_ROWS, K_ROWS), True)

        return carry

    lax.fori_loop(0, 6 * q_blocks, step, 0)

    def finish(state, carry):
        head = state // q_blocks
        sl = row_slice(lax.rem(state, q_blocks))
        for a in range(chains):
            total = jnp.sum(l_sc[state, a], axis=1, keepdims=True)
            out = (acc_sc[state, a] / total).astype(jnp.bfloat16)
            for h in range(per_chain):
                o_ref[head, sl, (a * per_chain + h) * head_dim:(a * per_chain + h + 1) * head_dim] = out[h * Q_ROWS:(h + 1) * Q_ROWS]
        return carry

    lax.fori_loop(0, 2 * q_blocks, finish, 0)

    stores = [pltpu.make_async_copy(o_ref, o_hbm, local_sems.at[0])]
    for e in range(2):
        late = c // 2
        owner = (1 - late) * (2 * c + e) + late * (7 - 2 * c - e)
        cross = lax.rem(late + y, 2)
        slot = 4 * cross + 2 * lax.rem(owner + c, 2) + lax.rem(owner // 2 + c // 2, 2)
        sl = pl.ds(e * chunk_len, chunk_len)
        stores.append(pltpu.make_async_copy(kv_buf.at[slot, cross, 0], kc_ref.at[sl, :], local_sems.at[1 + 2 * e]))
        stores.append(pltpu.make_async_copy(kv_buf.at[slot, cross, 1], vc_ref.at[sl, :], local_sems.at[2 + 2 * e]))
    for store in stores[::-1]:
        store.start()

    weights_arrived((3,), 2)
    weights_arrived((3,), 3)
    for store in stores:
        store.wait()
    for hd in range(2):
        for n in range(7):
            kv_copy(n, hd).wait_send()
    for kind in range(4):
        for stage in range(4):
            weight_copy(kind, stage).wait_send()
    forwarded = [j for j, _ in EARLY_FORWARD]
    second = [j for j, _ in EARLY_SECOND]
    for j in range(N_EARLY):
        if j not in forwarded:
            net.arrived(0, j)
        net.sent(0, j)
    net.arrived(0, N_EARLY, slice(0, PART))
    net.sent(0, N_EARLY, slice(0, PART))
    for j in forwarded:
        if j not in second:
            net.arrived(1, j)
        net.arrived(2, j)
        net.sent(1, j)
        net.sent(2, j)
    for j in second:
        net.arrived(3, j)
        net.sent(3, j)


def attention(x, gain, freq, wq, wk, wv, wo, w1, w3, w2):
    rows, dim = x.shape
    width = wq.shape[0] * 128
    states = 2 * rows // Q_ROWS
    m_rows = width // 128 // 2 * Q_ROWS
    vm = pl.BlockSpec(memory_space=pltpu.VMEM)
    hbm = pl.BlockSpec(memory_space=pl.ANY)
    bf16 = jnp.bfloat16
    n = N_EARLY + 1
    return pl.pallas_call(
        attention_kernel,
        in_specs=[hbm, vm, vm] + [hbm] * 7,
        out_specs=[hbm] * 7,
        out_shape=[
            jax.ShapeDtypeStruct((2, rows, width), bf16),
            jax.ShapeDtypeStruct((2 * rows, 128), bf16),
            jax.ShapeDtypeStruct((2 * rows, 128), bf16),
            jax.ShapeDtypeStruct(wo.shape, bf16),
            jax.ShapeDtypeStruct((N_CHUNKS - 1, 4, dim // 4, 4 * TILE), bf16),
            jax.ShapeDtypeStruct((N_CHUNKS - 1, 4, dim // 4, 4 * TILE), bf16),
            jax.ShapeDtypeStruct((N_CHUNKS - 1, 4, TILE, dim), bf16),
        ],
        scratch_shapes=[
            pltpu.VMEM((rows, dim), bf16),
            pltpu.VMEM(wq.shape, bf16),
            pltpu.VMEM(wk.shape, bf16),
            pltpu.VMEM(wv.shape, bf16),
            pltpu.VMEM((2, rows, width), bf16),
            pltpu.SemaphoreType.DMA((5,)),
            pltpu.VMEM((rows, 128), jnp.float32),
            pltpu.VMEM((rows, 128), jnp.float32),
            pltpu.VMEM((rows, dim), bf16),
            pltpu.VMEM((2, rows, width), bf16),
            pltpu.VMEM(wq.shape, bf16),
            pltpu.VMEM(wk.shape, bf16),
            pltpu.VMEM(wv.shape, bf16),
            pltpu.VMEM((8, 2, 2, rows, 128), bf16),
            pltpu.VMEM((states, 2, m_rows, 128), jnp.float32),
            pltpu.VMEM((states, 2, m_rows, 128), jnp.float32),
            pltpu.VMEM((states, 2, m_rows, 128), jnp.float32),
            pltpu.SemaphoreType.DMA((n, 4, 3)),
            pltpu.SemaphoreType.DMA((n, 4, 3)),
            pltpu.SemaphoreType.DMA((7, 2)),
            pltpu.SemaphoreType.DMA((7, 2)),
            pltpu.SemaphoreType.DMA((4, 4)),
            pltpu.SemaphoreType.DMA((4, 4)),
        ],
        compiler_params=pltpu.CompilerParams(collective_id=0, has_side_effects=True, vmem_limit_bytes=VMEM_LIMIT),
        cost_estimate=pl.CostEstimate(flops=16 * rows * 4096 * width, bytes_accessed=32 * 2**20, transcendentals=rows * 4096 * 12),
        name="attention",
    )(x, gain, freq, wq, wk, wv, wo, w1, w3, w2)


M_BLOCK = 1024
LATE_FORWARD = {3: (5,), 7: (6,), 11: (7,)}
LATE_SECOND = {3: (4,), 8: (5,), 12: (6,)}
END_SECOND = {15: (7,)}
LOAD_AFTER = 15
STEPS = 2 * N_CHUNKS - 1


def mlp_kernel(x_hbm, gain_ref, o_hbm, wo_hbm, ro_hbm, w1_ref, w3_ref, w2_ref, a1_ref, a3_ref, a2_ref, out_ref, hid_ref, r1_ref, r3_ref, r2_ref, e1_ref, e3_ref, e2_ref,
               w1_sc, w3_sc, w2_sc, x_ref, o_ref, wo_ref, ro_ref, first_sems, b_ref, acc_sc, hid_sc, load_sems, store_sems, send_sems, recv_sems):
    dim = x_ref.shape[1]
    width = 4 * TILE
    n_tiles = w1_ref.shape[1] // TILE
    net = Links((w1_ref, w3_ref, w2_ref), (r1_ref, r3_ref, r2_ref), send_sems, recv_sems, n_tiles)
    own_last = (n_tiles - 4) * TILE
    ends = (e1_ref, e3_ref, e2_ref)

    def own_loads(j, slot):
        off = min(j * width, own_last) if isinstance(j, int) else pl.multiple_of(jnp.minimum(j * width, own_last), TILE)
        sl = pl.ds(off, width)
        return [
            pltpu.make_async_copy(w1_ref.at[:, sl], w1_sc.at[slot], load_sems.at[slot, 0]),
            pltpu.make_async_copy(w3_ref.at[:, sl], w3_sc.at[slot], load_sems.at[slot, 1]),
            pltpu.make_async_copy(w2_ref.at[sl, :], w2_sc.at[slot], load_sems.at[slot, 2]),
        ]

    def other_loads(j, slot):
        copies = []
        depth = dim // 4
        for p in range(4):
            source = 2 * lax.rem(net.c // 2 + p % 2, 2) + lax.rem(net.c + p // 2, 2)
            deep = pl.ds(pl.multiple_of(source * depth, TILE), depth)
            sl = pl.ds(pl.multiple_of(source * TILE, TILE), TILE)
            copies.append(pltpu.make_async_copy(r1_ref.at[j, p], w1_sc.at[slot, deep, :], load_sems.at[slot, 0]))
            copies.append(pltpu.make_async_copy(r3_ref.at[j, p], w3_sc.at[slot, deep, :], load_sems.at[slot, 1]))
            copies.append(pltpu.make_async_copy(r2_ref.at[j, p], w2_sc.at[slot, sl, :], load_sems.at[slot, 2]))
        return copies

    def end_load(slot, a):
        w = pl.ds(0, e1_ref.shape[1])
        dst = w2_sc.at[slot, w, :] if a == 2 else (w1_sc, w3_sc)[a].at[slot, :, w]
        return pltpu.make_async_copy(ends[a], dst, load_sems.at[slot, a])

    def compute(slot, lane_keep):
        def rows_step(m, carry):
            sl = pl.ds(pl.multiple_of(m * M_BLOCK, M_BLOCK), M_BLOCK)
            b = b_ref[sl, :]
            gate = jnp.dot(b, w1_sc[slot], preferred_element_type=jnp.float32)
            up = jnp.dot(b, w3_sc[slot], preferred_element_type=jnp.float32)
            hidden = jax.nn.silu(gate) * up
            hidden = jnp.where(lane_keep > 0.5, hidden, 0.0).astype(jnp.bfloat16)
            acc_sc[sl, :] += jnp.dot(hidden, w2_sc[slot], preferred_element_type=jnp.float32)
            return carry

        lax.fori_loop(0, b_ref.shape[0] // M_BLOCK, rows_step, 0)

    firsts = [pltpu.make_async_copy(*pair, first_sems.at[n]) for n, pair in enumerate(((wo_hbm, wo_ref), (ro_hbm, ro_ref), (o_hbm, o_ref), (x_hbm, x_ref)))]
    for first in firsts:
        first.start()
    net.barrier()
    net.start(0, N_EARLY, slice(PART, 3))
    net.start(0, N_EARLY + 1)
    net.start(1, N_EARLY - 1)
    net.start(2, N_EARLY - 1)
    net.start(3, N_EARLY - 2)
    for copy in own_loads(0, 0):
        copy.start()

    def residual_rows(i, carry):
        sl = pl.ds(pl.multiple_of(i * Q_ROWS, Q_ROWS), Q_ROWS)
        attn = jnp.dot(o_ref[0, sl, :], wo_ref[...], preferred_element_type=jnp.float32)
        attn = attn + jnp.dot(o_ref[1, sl, :], ro_ref[...], preferred_element_type=jnp.float32)
        residual = (x_ref[sl, :].astype(jnp.float32) + attn).astype(jnp.bfloat16).astype(jnp.float32)
        acc_sc[sl, :] = residual
        b_ref[sl, :] = normed_rows(residual, gain_ref[...].astype(jnp.float32)[None, :])
        return carry

    for first in firsts:
        first.wait()
    lax.fori_loop(0, x_ref.shape[0] // Q_ROWS, residual_rows, 0)
    lane_tile = lax.broadcasted_iota(jnp.int32, (1, width), 1) // TILE

    def pass_on(s, forward, second):
        for when, chunks in forward.items():
            @pl.when(s == when)
            def _(chunks=chunks):
                for j in chunks:
                    net.pass_on(j, PART if j == N_EARLY else 0)
                    if j + 2 < N_CHUNKS - 1:
                        net.start(0, j + 2)
                    elif j + 2 == N_CHUNKS - 1:
                        for copy in net.last_chunk(0, ends):
                            copy.start()
        for when, chunks in second.items():
            @pl.when(s == when)
            def _(chunks=chunks):
                for j in chunks:
                    net.pass_second(j)

    def load_next(s, slot, after):
        for j in range(3, N_CHUNKS - 1):
            if (N_CHUNKS - 1 + j >= LOAD_AFTER) == after:
                @pl.when(s == N_CHUNKS - 1 + j)
                def _(j=j):
                    if j >= 4:
                        net.arrived(2, j)
                    net.arrived(3, j)

        if not after:
            @pl.when(s + 1 < N_CHUNKS)
            def _():
                for copy in own_loads(s + 1, 1 - slot):
                    copy.start()

        if not after:
            @pl.when(s == STEPS - 1)
            def _():
                for a in range(2):
                    net.last_chunk(2, ends, slice(a, a + 1))[0].wait_recv()
                    end_load(1 - slot, a).start()

        first, last = (LOAD_AFTER, STEPS - 1) if after else (N_CHUNKS - 1, LOAD_AFTER)

        @pl.when((s >= first) & (s < last))
        def _():
            for copy in other_loads(s + 1 - N_CHUNKS, 1 - slot):
                copy.start()

    def step(s, carry):
        slot = lax.rem(s, 2)
        pass_on(s, LATE_FORWARD, LATE_SECOND)
        load_next(s, slot, False)
        for copy in own_loads(0, slot):
            copy.wait()

        keep = 1.0 - (s == N_CHUNKS - 1).astype(jnp.float32) * (lane_tile == 0).astype(jnp.float32)
        compute(slot, keep)
        pass_on(s, {}, END_SECOND)

        @pl.when(s == STEPS - 2)
        def _():
            for a in range(2):
                net.last_chunk(0, ends, slice(a, a + 1))[0].wait_recv()
                net.last_chunk(2, ends, slice(a, a + 1))[0].start()

        load_next(s, slot, True)
        return carry

    lax.fori_loop(0, STEPS, step, 0)

    store_sum = pltpu.make_async_copy(acc_sc, out_ref, store_sems.at[0])
    store_sum.start()
    slot = STEPS % 2
    left = e1_ref.shape[1]
    net.last_chunk(0, ends, slice(2, 3))[0].wait_recv()
    net.last_chunk(2, ends, slice(2, 3))[0].start()
    for a in range(2):
        end_load(slot, a).wait()

    def hidden_rows(m, carry):
        sl = pl.ds(pl.multiple_of(m * M_BLOCK, M_BLOCK), M_BLOCK)
        gate = jnp.dot(b_ref[sl, :], w1_sc[slot, :, :left], preferred_element_type=jnp.float32)
        up = jnp.dot(b_ref[sl, :], w3_sc[slot, :, :left], preferred_element_type=jnp.float32)
        hid_sc[sl, :] = (jax.nn.silu(gate) * up).astype(jnp.bfloat16)
        return carry

    lax.fori_loop(0, x_ref.shape[0] // M_BLOCK, hidden_rows, 0)
    store_hidden = pltpu.make_async_copy(hid_sc, hid_ref, store_sems.at[1])
    store_hidden.start()
    net.last_chunk(2, ends, slice(2, 3))[0].wait_recv()
    store_sum.wait()
    store_hidden.wait()
    net.sent(0, N_EARLY, slice(PART, 3))
    for j in range(N_EARLY + 1, N_CHUNKS - 1):
        net.sent(0, j)
    for j in range(N_EARLY - 1, N_CHUNKS - 1):
        net.sent(1, j)
        net.sent(2, j)
    for j in range(N_EARLY - 2, N_CHUNKS - 1):
        net.sent(3, j)
    for stage in (0, 2):
        for copy in net.last_chunk(stage, ends):
            copy.wait_send()


def mlp(x, gain, o, wo, ro, w1, w3, w2, early):
    rows, dim = x.shape
    vm = pl.BlockSpec(memory_space=pltpu.VMEM)
    hbm = pl.BlockSpec(memory_space=pl.ANY)
    bf16 = jnp.bfloat16
    width = 4 * TILE
    left = w1.shape[1] % width
    n = N_CHUNKS
    return pl.pallas_call(
        mlp_kernel,
        in_specs=[hbm, vm] + [hbm] * 9,
        out_specs=[hbm] * 8,
        out_shape=[jax.ShapeDtypeStruct((rows, dim), jnp.float32), jax.ShapeDtypeStruct((rows, left), bf16)] + [jax.ShapeDtypeStruct(a.shape, bf16) for a in early] + [jax.ShapeDtypeStruct(s, bf16) for s in ((dim, left), (dim, left), (left, dim))],
        input_output_aliases={8: 2, 9: 3, 10: 4},
        scratch_shapes=[
            pltpu.VMEM((2, dim, width), bf16),
            pltpu.VMEM((2, dim, width), bf16),
            pltpu.VMEM((2, width, dim), bf16),
            pltpu.VMEM(x.shape, bf16),
            pltpu.VMEM(o.shape, bf16),
            pltpu.VMEM(wo.shape, bf16),
            pltpu.VMEM(ro.shape, bf16),
            pltpu.SemaphoreType.DMA((4,)),
            pltpu.VMEM((rows, dim), bf16),
            pltpu.VMEM((rows, dim), jnp.float32),
            pltpu.VMEM((rows, left), bf16),
            pltpu.SemaphoreType.DMA((2, 3)),
            pltpu.SemaphoreType.DMA((2,)),
            pltpu.SemaphoreType.DMA((n, 4, 3)),
            pltpu.SemaphoreType.DMA((n, 4, 3)),
        ],
        compiler_params=pltpu.CompilerParams(collective_id=1, has_side_effects=True, vmem_limit_bytes=VMEM_LIMIT),
        cost_estimate=pl.CostEstimate(flops=12 * rows * dim * w1.shape[1], bytes_accessed=12 * dim * w1.shape[1], transcendentals=2 * rows * w1.shape[1]),
        name="mlp",
    )(x, gain, o, wo, ro, w1, w3, w2, *early)


def last_kernel(sum_ref, hid_ref, w2_ref, kc_ref, vc_ref, out_ref, k_ref, v_ref):
    out_ref[...] = (sum_ref[...] + jnp.dot(hid_ref[...], w2_ref[...], preferred_element_type=jnp.float32)).astype(out_ref.dtype)
    k_ref[...] = kc_ref[...]
    v_ref[...] = vc_ref[...]


def last_product(total, hidden, w2, k_cache, v_cache):
    rows, dim = total.shape
    steps = rows // 128

    def by_rows(a):
        return pl.BlockSpec((a.shape[0] // steps, a.shape[1]), lambda i: (i, 0))

    out = jax.ShapeDtypeStruct((rows, dim), jnp.bfloat16)
    return pl.pallas_call(
        last_kernel,
        grid=(steps,),
        in_specs=[by_rows(total), by_rows(hidden), pl.BlockSpec(w2.shape, lambda i: (0, 0)), by_rows(k_cache), by_rows(v_cache)],
        out_specs=[by_rows(out), by_rows(k_cache), by_rows(v_cache)],
        out_shape=[out, jax.ShapeDtypeStruct(k_cache.shape, k_cache.dtype), jax.ShapeDtypeStruct(v_cache.shape, v_cache.dtype)],
        cost_estimate=pl.CostEstimate(flops=2 * rows * dim * w2.shape[0], bytes_accessed=6 * rows * dim, transcendentals=0),
        name="last_product",
    )(total, hidden, w2, k_cache, v_cache)

def solution(mesh):
    def layer_shard(x_loc, norm_attn, norm_mlp, w_query, w_key, w_value, w_out, w_gate, w_up, w_down):
        wq, wk, wv = (jnp.transpose(w, (1, 0, 2)) for w in (w_query, w_key, w_value))
        wo = w_out.reshape(-1, w_out.shape[2])
        o, k_cache, v_cache, wo_other, *early = attention(x_loc, norm_attn, rope_frequencies(w_query.shape[2]), wq, wk, wv, wo, w_gate, w_up, w_down)
        total, hidden, *_, last_w2 = mlp(x_loc, norm_mlp, o, wo, wo_other, w_gate, w_up, w_down, early)
        return tuple(last_product(total, hidden, last_w2, k_cache, v_cache))

    row_spec = P(("dp", "cp", "tp"), None)
    cache_spec = P(("dp", "cp"), "tp")
    head_spec = P(None, "tp", None)
    return jax.shard_map(
        layer_shard,
        mesh=mesh,
        in_specs=(row_spec, P(None), P(None), head_spec, head_spec, head_spec, P("tp", None, None), P(None, "tp"), P(None, "tp"), P("tp", None)),
        out_specs=(row_spec, cache_spec, cache_spec),
        check_vma=False,
    )
```

```python
import functools

import jax
import jax.numpy as jnp
from jax import lax
from jax.experimental import pallas as pl
from jax.experimental.pallas import tpu as pltpu
from jax.sharding import PartitionSpec as P

ROPE_BASE = 500000.0
NORM_EPS = 1e-5
MASK_VALUE = -1e30
LOG2E = 1.4426950408889634
VMEM_LIMIT = 60 * 1024 * 1024
Q_ROWS = 256
K_ROWS = 512
MESH = pl.DeviceIdType.MESH
TILE = 128
N_CHUNKS = 9
N_EARLY = 5
PART = 1


def rope_frequencies(head_dim):
    lane = jnp.arange(head_dim, dtype=jnp.int32)
    return ROPE_BASE ** (-2.0 * (lane % (head_dim // 2)).astype(jnp.float32) / head_dim)


class Links:
    def __init__(self, weights, recv, send_sems, recv_sems, n_tiles):
        self.y, self.c = lax.axis_index("tp"), lax.axis_index("cp")
        self.peer = {
            "y": {"tp": 1 - self.y},
            "x": {"cp": lax.rem(self.c + 2, 4)},
            "d": {"cp": self.c + 1 - 2 * lax.rem(self.c, 2)},
        }
        self.weights, self.recv, self.send_sems, self.recv_sems = weights, recv, send_sems, recv_sems
        self.n_tiles = n_tiles
        self.started = []

    def barrier(self):
        sem = pltpu.get_barrier_semaphore()
        for name in "yxd":
            pl.semaphore_signal(sem, inc=1, device_id=self.peer[name], device_id_type=MESH)
        pl.semaphore_wait(sem, 3)

    def remote(self, src, dst, ssem, rsem, to):
        return pltpu.make_async_remote_copy(src_ref=src, dst_ref=dst, send_sem=ssem, recv_sem=rsem, device_id=self.peer[to], device_id_type=MESH)

    def chunk(self, stage, j, arrays=slice(0, 3)):
        to = "yxdd"[stage]
        copies = []
        for a in range(3)[arrays]:
            if stage == 0:
                w = self.weights[a]
                if a == 2:
                    src = w.at[pl.ds(pl.multiple_of((4 * j + self.c) * TILE, TILE), TILE), :]
                else:
                    depth = w.shape[0] // 4
                    src = w.at[pl.ds(pl.multiple_of(self.c * depth, TILE), depth), pl.ds(4 * j * TILE, 4 * TILE)]
            else:
                src = self.recv[a].at[j, (0, 0, 0, 1)[stage]]
            copies.append(self.remote(src, self.recv[a].at[j, stage], self.send_sems.at[j, stage, a], self.recv_sems.at[j, stage, a], to))
        return copies

    def last_chunk(self, stage, last, arrays=slice(0, 3)):
        half = lax.rem(self.c, 2)
        begin = (self.n_tiles // 4) * 4 * TILE
        copies = []
        for a in range(3)[arrays]:
            depth = last[a].shape[0] // 2
            at = pl.ds(pl.multiple_of(half * depth, 64), depth)
            dst = last[a].at[at, :]
            if stage == 2:
                src = dst
            elif a == 2:
                src = self.weights[a].at[pl.ds(pl.multiple_of(begin + half * depth, 64), depth), :]
            else:
                src = self.weights[a].at[at, pl.ds(begin, last[a].shape[1])]
            j = N_CHUNKS - 1
            copies.append(self.remote(src, dst, self.send_sems.at[j, stage, a], self.recv_sems.at[j, stage, a], "y.d"[stage]))
        return copies

    def pass_on(self, j, here=0):
        for a in range(3):
            if a >= here:
                self.arrived(0, j, slice(a, a + 1))
            self.start(1, j, slice(a, a + 1))
            self.start(2, j, slice(a, a + 1))

    def pass_second(self, j):
        for first, over_d in zip(self.chunk(1, j), self.chunk(3, j)):
            first.wait_recv()
            over_d.start()

    def start(self, stage, j, arrays=slice(0, 3)):
        for copy in self.chunk(stage, j, arrays):
            copy.start()

    def arrived(self, stage, j, arrays=slice(0, 3)):
        for copy in self.chunk(stage, j, arrays):
            copy.wait_recv()

    def sent(self, stage, j, arrays=slice(0, 3)):
        for copy in self.chunk(stage, j, arrays):
            copy.wait_send()


EARLY_FORWARD = ((0, 15), (1, 18), (2, 20), (3, 22))
EARLY_SECOND = ((0, 19), (1, 21), (2, 23))
SLOT_SOURCE = (0, 0, 0, 1)


def normed_rows(wide, gain):
    inv_rms = lax.rsqrt(jnp.mean(wide * wide, axis=-1, keepdims=True) + NORM_EPS)
    return (wide * inv_rms * gain).astype(jnp.bfloat16)


def attention_kernel(x_hbm, gain_ref, freq_ref, wq_hbm, wk_hbm, wv_hbm, wo_ref, w1_ref, w3_ref, w2_ref,
                     o_hbm, kc_ref, vc_ref, ro_ref, r1_ref, r3_ref, r2_ref,
                     x_ref, wq_ref, wk_ref, wv_ref, o_ref, local_sems, cos_ref, sin_ref, a_sc, q_sc, wq_sc, wk_sc, wv_sc, kv_buf, m_sc, l_sc, acc_sc, send_sems, recv_sems, kv_send, kv_recv, wt_send, wt_recv):
    head_dim = 128
    half_dim = head_dim // 2
    chunk_len = x_ref.shape[0]
    heads = wq_ref.shape[0]
    chains = 2
    per_chain = heads // chains
    rows = per_chain * Q_ROWS
    q_blocks = chunk_len // Q_ROWS
    coef = head_dim ** -0.5 * LOG2E
    net = Links((w1_ref, w3_ref, w2_ref), (r1_ref, r3_ref, r2_ref), send_sems, recv_sems, w1_ref.shape[1] // TILE)
    y, c = net.y, net.c
    core_lower = lax.rem(c + y, 2)
    chip_lower = lax.rem(c // 2 + y, 2)
    other_chip = lax.rem(c + 2, 4)

    def kv_copy(n, hd):
        src, dst, to = ((0, 1, "x"), (0, 2, "d"), (1, 3, "d"), (0, 4, "y"), (4, 5, "x"), (4, 6, "d"), (5, 7, "d"))[n]
        return net.remote(kv_buf.at[src, hd], kv_buf.at[dst, hd], kv_send.at[n, hd], kv_recv.at[n, hd], to)

    def weight_copy(kind, stage):
        own, held = ((wk_hbm, wk_sc), (wv_hbm, wv_sc), (wq_hbm, wq_sc), (wo_ref, ro_ref))[kind]
        quarter = own.shape[-2] // 4
        sl = pl.ds(pl.multiple_of((other_chip if stage == 3 else c) * quarter, 64), quarter)
        src = own if stage == 0 else held
        pick = (lambda r: r.at[sl, :]) if kind == 3 else (lambda r: r.at[:, sl, :])
        return net.remote(pick(src), pick(held), wt_send.at[kind, stage], wt_recv.at[kind, stage], "yxdd"[stage])

    def weights_start(kinds, stage):
        for kind in kinds:
            weight_copy(kind, stage).start()

    def weights_arrived(kinds, stage):
        for kind in kinds:
            weight_copy(kind, stage).wait_recv()

    def row_slice(i):
        return pl.ds(pl.multiple_of(i * Q_ROWS, Q_ROWS), Q_ROWS)

    def rope(t, sl):
        return (t * cos_ref[sl, :] + pltpu.roll(t, half_dim, 1) * sin_ref[sl, :]).astype(jnp.bfloat16)

    def norm_x():
        def body(i, carry):
            sl = row_slice(i)
            row = (y * (7 - 2 * c) + c) * chunk_len + i * Q_ROWS + lax.broadcasted_iota(jnp.int32, (Q_ROWS, head_dim), 0)
            angles = row.astype(jnp.float32) * freq_ref[...][None, :]
            sine_tab = jnp.sin(angles)
            cos_ref[sl, :] = jnp.cos(angles)
            sin_ref[sl, :] = jnp.where(lax.broadcasted_iota(jnp.int32, (Q_ROWS, head_dim), 1) < half_dim, -sine_tab, sine_tab)
            a_sc[sl, :] = normed_rows(x_ref[sl, :].astype(jnp.float32), gain_ref[...].astype(jnp.float32)[None, :])
            return carry
        lax.fori_loop(0, q_blocks, body, 0)

    def make_kv(k_ref, v_ref, hd):
        def body(i, carry):
            sl = row_slice(i)
            w = jnp.concatenate([k_ref[0], v_ref[0]], axis=1)
            proj = jnp.dot(a_sc[sl, :], w, preferred_element_type=jnp.float32)
            kv_buf[0, hd, 0, sl, :] = rope(proj[:, :head_dim], sl)
            kv_buf[0, hd, 1, sl, :] = proj[:, head_dim:].astype(jnp.bfloat16)
            return carry
        lax.fori_loop(0, q_blocks, body, 0)

    def make_q(w_ref, hd):
        def body(i, carry):
            sl = row_slice(i)
            w = jnp.concatenate([w_ref[h] for h in range(heads)], axis=1)
            proj = jnp.dot(a_sc[sl, :], w, preferred_element_type=jnp.float32)
            for h in range(heads):
                cols = slice(h * head_dim, (h + 1) * head_dim)
                q_sc[hd, sl, cols] = rope(proj[:, cols], sl)
            return carry
        lax.fori_loop(0, q_blocks, body, 0)

    loads = [pltpu.make_async_copy(*pair, local_sems.at[n]) for n, pair in enumerate(((x_hbm, x_ref), (wk_hbm, wk_ref), (wv_hbm, wv_ref), (wq_hbm, wq_ref)))]
    for load in loads:
        load.start()
    net.barrier()
    weights_start((0, 1, 2), 0)
    loads[0].wait()
    norm_x()
    loads[1].wait()
    loads[2].wait()
    make_kv(wk_ref, wv_ref, 0)
    m_sc[...] = jnp.full_like(m_sc, MASK_VALUE)
    l_sc[...] = jnp.zeros_like(l_sc)
    acc_sc[...] = jnp.zeros_like(acc_sc)
    weights_arrived((0, 1), 0)
    weights_start((0, 1), 1)
    weights_start((0, 1), 2)
    kv_copy(1, 0).start()
    kv_copy(0, 0).start()
    kv_copy(3, 0).start()
    loads[3].wait()
    make_q(wq_ref, 0)

    def block(q_parts, state, start, slot, head, off, masked):
        k_blk = kv_buf[slot, head, 0, pl.ds(off, K_ROWS), :]
        v_blk = kv_buf[slot, head, 1, pl.ds(off, K_ROWS), :]
        for a in range(chains):
            s = lax.dot_general(q_parts[a], k_blk, (((1,), (1,)), ((), ())), preferred_element_type=jnp.float32)
            if masked:
                q_pos = start + lax.rem(lax.broadcasted_iota(jnp.int32, (rows, K_ROWS), 0), Q_ROWS)
                k_pos = off + lax.broadcasted_iota(jnp.int32, (rows, K_ROWS), 1)
                s = jnp.where(k_pos <= q_pos, s, MASK_VALUE)
            m_prev = m_sc[state, a]
            m_new = jnp.maximum(m_prev, jnp.max(s, axis=1, keepdims=True))
            alpha = jnp.exp2((m_prev - m_new) * coef)
            mc = m_new * coef
            sums = l_sc[state, a] * alpha
            p_tiles = []
            for j in range(K_ROWS // 128):
                p = jnp.exp2(s[:, j * 128:(j + 1) * 128] * coef - mc)
                sums = sums + p
                p_tiles.append(p.astype(jnp.bfloat16))
            l_sc[state, a] = sums
            m_sc[state, a] = m_new
            p_all = jnp.concatenate(p_tiles, axis=1)
            acc_sc[state, a] = acc_sc[state, a] * alpha + jnp.dot(p_all, v_blk, preferred_element_type=jnp.float32)

    def load_q(head, qb):
        sl = row_slice(qb)
        return [jnp.concatenate([q_sc[head, sl, (a * per_chain + h) * head_dim:(a * per_chain + h + 1) * head_dim] for h in range(per_chain)], axis=0) for a in range(chains)]

    per_piece = chunk_len // K_ROWS

    def step(s, carry):
        phase = s // q_blocks
        qb = lax.rem(s, q_blocks)
        is_last = phase // 4
        is_mid = (1 - is_last) * lax.rem(phase, 2)
        is_first = 1 - is_last - is_mid
        head = (1 - is_last) * (phase // 2) + is_last * (phase - 4)
        state = head * q_blocks + qb

        @pl.when(s == 0)
        def _():
            kv_copy(1, 0).wait_recv()

        @pl.when(s == 1)
        def _():
            weights_arrived((0, 1), 1)
            weights_start((0, 1), 3)

        @pl.when(s == 2)
        def _():
            weights_arrived((0, 1), 2)
            weights_arrived((0, 1), 3)
            make_kv(wk_sc, wv_sc, 1)
            weights_arrived((2,), 0)
            weights_start((2,), 1)
            weights_start((2,), 2)

        @pl.when(s == 3)
        def _():
            kv_copy(1, 1).start()
            kv_copy(0, 1).start()
            kv_copy(3, 1).start()
            weights_start((3,), 0)
            net.start(0, 0)
            net.start(0, 1)
            kv_copy(0, 0).wait_recv()
            kv_copy(2, 0).start()

        @pl.when(s == 4)
        def _():
            kv_copy(2, 0).wait_recv()

        @pl.when(s == 6)
        def _():
            weights_arrived((2,), 1)
            weights_start((2,), 3)
            kv_copy(3, 0).wait_recv()
            kv_copy(4, 0).start()
            kv_copy(5, 0).start()

        @pl.when(s == 7)
        def _():
            weights_arrived((2,), 2)
            weights_arrived((2,), 3)
            make_q(wq_sc, 1)

        @pl.when(s == 8)
        def _():
            kv_copy(1, 1).wait_recv()

        @pl.when(s == 9)
        def _():
            kv_copy(0, 1).wait_recv()
            kv_copy(2, 1).start()

        @pl.when(s == 10)
        def _():
            kv_copy(3, 1).wait_recv()
            kv_copy(4, 1).start()
            kv_copy(5, 1).start()

        @pl.when(s == 12)
        def _():
            kv_copy(2, 1).wait_recv()
            weights_arrived((3,), 0)
            weights_start((3,), 1)
            weights_start((3,), 2)

        @pl.when(s == 13)
        def _():
            kv_copy(4, 0).wait_recv()
            kv_copy(6, 0).start()

        @pl.when(s == 14)
        def _():
            kv_copy(4, 1).wait_recv()
            kv_copy(6, 1).start()

        @pl.when(s == 16)
        def _():
            for hd in range(2):
                kv_copy(5, hd).wait_recv()
                kv_copy(6, hd).wait_recv()
            weights_arrived((3,), 1)
            weights_start((3,), 3)

        for j, when in EARLY_FORWARD:
            @pl.when(s == when)
            def _(j=j):
                net.pass_on(j)
                if j + 2 < N_EARLY:
                    net.start(0, j + 2)
                elif j + 2 == N_EARLY:
                    net.start(0, N_EARLY, slice(0, PART))

        for j, when in EARLY_SECOND:
            @pl.when(s == when)
            def _(j=j):
                net.pass_second(j)

        q_parts = load_q(head, qb)
        start = qb * Q_ROWS
        diag = start // K_ROWS
        count = is_first * (diag + per_piece * core_lower) + is_mid * 2 * per_piece * chip_lower + is_last * 4 * per_piece * y
        kv_head = head + is_last * (1 - 2 * head)

        def inner(i, carry):
            in_core = (i >= diag).astype(jnp.int32)
            idx = i - is_first * in_core * diag
            slot = is_first * 2 * in_core + is_mid * (1 + 2 * (i // per_piece)) + is_last * (4 + i // per_piece)
            off = (is_first * (in_core * lax.rem(idx, per_piece) + (1 - in_core) * i) + (1 - is_first) * lax.rem(i, per_piece)) * K_ROWS
            block(q_parts, state, start, slot, kv_head, pl.multiple_of(off, K_ROWS), False)
            return carry

        lax.fori_loop(0, count, inner, 0)

        @pl.when(is_first == 1)
        def _():
            block(q_parts, state, start, 0, head, pl.multiple_of(diag * K_ROWS, K_ROWS), True)

        return carry

    lax.fori_loop(0, 6 * q_blocks, step, 0)

    def finish(state, carry):
        head = state // q_blocks
        sl = row_slice(lax.rem(state, q_blocks))
        for a in range(chains):
            total = jnp.sum(l_sc[state, a], axis=1, keepdims=True)
            out = (acc_sc[state, a] / total).astype(jnp.bfloat16)
            for h in range(per_chain):
                o_ref[head, sl, (a * per_chain + h) * head_dim:(a * per_chain + h + 1) * head_dim] = out[h * Q_ROWS:(h + 1) * Q_ROWS]
        return carry

    lax.fori_loop(0, 2 * q_blocks, finish, 0)

    stores = [pltpu.make_async_copy(o_ref, o_hbm, local_sems.at[0])]
    for e in range(2):
        late = c // 2
        owner = (1 - late) * (2 * c + e) + late * (7 - 2 * c - e)
        cross = lax.rem(late + y, 2)
        slot = 4 * cross + 2 * lax.rem(owner + c, 2) + lax.rem(owner // 2 + c // 2, 2)
        sl = pl.ds(e * chunk_len, chunk_len)
        stores.append(pltpu.make_async_copy(kv_buf.at[slot, cross, 0], kc_ref.at[sl, :], local_sems.at[1 + 2 * e]))
        stores.append(pltpu.make_async_copy(kv_buf.at[slot, cross, 1], vc_ref.at[sl, :], local_sems.at[2 + 2 * e]))
    for store in stores[::-1]:
        store.start()

    weights_arrived((3,), 2)
    weights_arrived((3,), 3)
    for store in stores:
        store.wait()
    for hd in range(2):
        for n in range(7):
            kv_copy(n, hd).wait_send()
    for kind in range(4):
        for stage in range(4):
            weight_copy(kind, stage).wait_send()
    forwarded = [j for j, _ in EARLY_FORWARD]
    second = [j for j, _ in EARLY_SECOND]
    for j in range(N_EARLY):
        if j not in forwarded:
            net.arrived(0, j)
        net.sent(0, j)
    net.arrived(0, N_EARLY, slice(0, PART))
    net.sent(0, N_EARLY, slice(0, PART))
    for j in forwarded:
        if j not in second:
            net.arrived(1, j)
        net.arrived(2, j)
        net.sent(1, j)
        net.sent(2, j)
    for j in second:
        net.arrived(3, j)
        net.sent(3, j)


def attention(x, gain, freq, wq, wk, wv, wo, w1, w3, w2):
    rows, dim = x.shape
    width = wq.shape[0] * 128
    states = 2 * rows // Q_ROWS
    m_rows = width // 128 // 2 * Q_ROWS
    vm = pl.BlockSpec(memory_space=pltpu.VMEM)
    hbm = pl.BlockSpec(memory_space=pl.ANY)
    bf16 = jnp.bfloat16
    n = N_EARLY + 1
    return pl.pallas_call(
        attention_kernel,
        in_specs=[hbm, vm, vm] + [hbm] * 7,
        out_specs=[hbm] * 7,
        out_shape=[
            jax.ShapeDtypeStruct((2, rows, width), bf16),
            jax.ShapeDtypeStruct((2 * rows, 128), bf16),
            jax.ShapeDtypeStruct((2 * rows, 128), bf16),
            jax.ShapeDtypeStruct(wo.shape, bf16),
            jax.ShapeDtypeStruct((N_CHUNKS - 1, 4, dim // 4, 4 * TILE), bf16),
            jax.ShapeDtypeStruct((N_CHUNKS - 1, 4, dim // 4, 4 * TILE), bf16),
            jax.ShapeDtypeStruct((N_CHUNKS - 1, 4, TILE, dim), bf16),
        ],
        scratch_shapes=[
            pltpu.VMEM((rows, dim), bf16),
            pltpu.VMEM(wq.shape, bf16),
            pltpu.VMEM(wk.shape, bf16),
            pltpu.VMEM(wv.shape, bf16),
            pltpu.VMEM((2, rows, width), bf16),
            pltpu.SemaphoreType.DMA((5,)),
            pltpu.VMEM((rows, 128), jnp.float32),
            pltpu.VMEM((rows, 128), jnp.float32),
            pltpu.VMEM((rows, dim), bf16),
            pltpu.VMEM((2, rows, width), bf16),
            pltpu.VMEM(wq.shape, bf16),
            pltpu.VMEM(wk.shape, bf16),
            pltpu.VMEM(wv.shape, bf16),
            pltpu.VMEM((8, 2, 2, rows, 128), bf16),
            pltpu.VMEM((states, 2, m_rows, 128), jnp.float32),
            pltpu.VMEM((states, 2, m_rows, 128), jnp.float32),
            pltpu.VMEM((states, 2, m_rows, 128), jnp.float32),
            pltpu.SemaphoreType.DMA((n, 4, 3)),
            pltpu.SemaphoreType.DMA((n, 4, 3)),
            pltpu.SemaphoreType.DMA((7, 2)),
            pltpu.SemaphoreType.DMA((7, 2)),
            pltpu.SemaphoreType.DMA((4, 4)),
            pltpu.SemaphoreType.DMA((4, 4)),
        ],
        compiler_params=pltpu.CompilerParams(collective_id=0, has_side_effects=True, vmem_limit_bytes=VMEM_LIMIT),
        cost_estimate=pl.CostEstimate(flops=16 * rows * 4096 * width, bytes_accessed=32 * 2**20, transcendentals=rows * 4096 * 12),
        name="attention",
    )(x, gain, freq, wq, wk, wv, wo, w1, w3, w2)


M_BLOCK = 1024
LATE_FORWARD = {3: (5,), 7: (6,), 11: (7,)}
LATE_SECOND = {3: (4,), 8: (5,), 12: (6,)}
END_SECOND = {15: (7,)}
LOAD_AFTER = 15
STEPS = 2 * N_CHUNKS - 1


def mlp_kernel(x_hbm, gain_ref, o_hbm, wo_hbm, ro_hbm, w1_ref, w3_ref, w2_ref, a1_ref, a3_ref, a2_ref, out_ref, hid_ref, r1_ref, r3_ref, r2_ref, e1_ref, e3_ref, e2_ref,
               w1_sc, w3_sc, w2_sc, x_ref, o_ref, wo_ref, ro_ref, first_sems, b_ref, acc_sc, hid_sc, load_sems, store_sems, send_sems, recv_sems):
    dim = x_ref.shape[1]
    width = 4 * TILE
    n_tiles = w1_ref.shape[1] // TILE
    net = Links((w1_ref, w3_ref, w2_ref), (r1_ref, r3_ref, r2_ref), send_sems, recv_sems, n_tiles)
    own_last = (n_tiles - 4) * TILE
    ends = (e1_ref, e3_ref, e2_ref)

    def own_loads(j, slot):
        off = min(j * width, own_last) if isinstance(j, int) else pl.multiple_of(jnp.minimum(j * width, own_last), TILE)
        sl = pl.ds(off, width)
        return [
            pltpu.make_async_copy(w1_ref.at[:, sl], w1_sc.at[slot], load_sems.at[slot, 0]),
            pltpu.make_async_copy(w3_ref.at[:, sl], w3_sc.at[slot], load_sems.at[slot, 1]),
            pltpu.make_async_copy(w2_ref.at[sl, :], w2_sc.at[slot], load_sems.at[slot, 2]),
        ]

    def other_loads(j, slot):
        copies = []
        depth = dim // 4
        for p in range(4):
            source = 2 * lax.rem(net.c // 2 + p % 2, 2) + lax.rem(net.c + p // 2, 2)
            deep = pl.ds(pl.multiple_of(source * depth, TILE), depth)
            sl = pl.ds(pl.multiple_of(source * TILE, TILE), TILE)
            copies.append(pltpu.make_async_copy(r1_ref.at[j, p], w1_sc.at[slot, deep, :], load_sems.at[slot, 0]))
            copies.append(pltpu.make_async_copy(r3_ref.at[j, p], w3_sc.at[slot, deep, :], load_sems.at[slot, 1]))
            copies.append(pltpu.make_async_copy(r2_ref.at[j, p], w2_sc.at[slot, sl, :], load_sems.at[slot, 2]))
        return copies

    def end_load(slot, a):
        w = pl.ds(0, e1_ref.shape[1])
        dst = w2_sc.at[slot, w, :] if a == 2 else (w1_sc, w3_sc)[a].at[slot, :, w]
        return pltpu.make_async_copy(ends[a], dst, load_sems.at[slot, a])

    def compute(slot, lane_keep):
        def rows_step(m, carry):
            sl = pl.ds(pl.multiple_of(m * M_BLOCK, M_BLOCK), M_BLOCK)
            b = b_ref[sl, :]
            gate = jnp.dot(b, w1_sc[slot], preferred_element_type=jnp.float32)
            up = jnp.dot(b, w3_sc[slot], preferred_element_type=jnp.float32)
            hidden = jax.nn.silu(gate) * up
            hidden = jnp.where(lane_keep > 0.5, hidden, 0.0).astype(jnp.bfloat16)
            acc_sc[sl, :] += jnp.dot(hidden, w2_sc[slot], preferred_element_type=jnp.float32)
            return carry

        lax.fori_loop(0, b_ref.shape[0] // M_BLOCK, rows_step, 0)

    firsts = [pltpu.make_async_copy(*pair, first_sems.at[n]) for n, pair in enumerate(((wo_hbm, wo_ref), (ro_hbm, ro_ref), (o_hbm, o_ref), (x_hbm, x_ref)))]
    for first in firsts:
        first.start()
    net.barrier()
    net.start(0, N_EARLY, slice(PART, 3))
    net.start(0, N_EARLY + 1)
    net.start(1, N_EARLY - 1)
    net.start(2, N_EARLY - 1)
    net.start(3, N_EARLY - 2)
    for copy in own_loads(0, 0):
        copy.start()

    def residual_rows(i, carry):
        sl = pl.ds(pl.multiple_of(i * Q_ROWS, Q_ROWS), Q_ROWS)
        attn = jnp.dot(o_ref[0, sl, :], wo_ref[...], preferred_element_type=jnp.float32)
        attn = attn + jnp.dot(o_ref[1, sl, :], ro_ref[...], preferred_element_type=jnp.float32)
        residual = (x_ref[sl, :].astype(jnp.float32) + attn).astype(jnp.bfloat16).astype(jnp.float32)
        acc_sc[sl, :] = residual
        b_ref[sl, :] = normed_rows(residual, gain_ref[...].astype(jnp.float32)[None, :])
        return carry

    for first in firsts:
        first.wait()
    lax.fori_loop(0, x_ref.shape[0] // Q_ROWS, residual_rows, 0)
    lane_tile = lax.broadcasted_iota(jnp.int32, (1, width), 1) // TILE

    def pass_on(s, forward, second):
        for when, chunks in forward.items():
            @pl.when(s == when)
            def _(chunks=chunks):
                for j in chunks:
                    net.pass_on(j, PART if j == N_EARLY else 0)
                    if j + 2 < N_CHUNKS - 1:
                        net.start(0, j + 2)
                    elif j + 2 == N_CHUNKS - 1:
                        for copy in net.last_chunk(0, ends):
                            copy.start()
        for when, chunks in second.items():
            @pl.when(s == when)
            def _(chunks=chunks):
                for j in chunks:
                    net.pass_second(j)

    def load_next(s, slot, after):
        for j in range(3, N_CHUNKS - 1):
            if (N_CHUNKS - 1 + j >= LOAD_AFTER) == after:
                @pl.when(s == N_CHUNKS - 1 + j)
                def _(j=j):
                    if j >= 4:
                        net.arrived(2, j)
                    net.arrived(3, j)

        if not after:
            @pl.when(s + 1 < N_CHUNKS)
            def _():
                for copy in own_loads(s + 1, 1 - slot):
                    copy.start()

        if not after:
            @pl.when(s == STEPS - 1)
            def _():
                for a in range(2):
                    net.last_chunk(2, ends, slice(a, a + 1))[0].wait_recv()
                    end_load(1 - slot, a).start()

        first, last = (LOAD_AFTER, STEPS - 1) if after else (N_CHUNKS - 1, LOAD_AFTER)

        @pl.when((s >= first) & (s < last))
        def _():
            for copy in other_loads(s + 1 - N_CHUNKS, 1 - slot):
                copy.start()

    def step(s, carry):
        slot = lax.rem(s, 2)
        pass_on(s, LATE_FORWARD, LATE_SECOND)
        load_next(s, slot, False)
        for copy in own_loads(0, slot):
            copy.wait()

        keep = 1.0 - (s == N_CHUNKS - 1).astype(jnp.float32) * (lane_tile == 0).astype(jnp.float32)
        compute(slot, keep)
        pass_on(s, {}, END_SECOND)

        @pl.when(s == STEPS - 2)
        def _():
            for a in range(2):
                net.last_chunk(0, ends, slice(a, a + 1))[0].wait_recv()
                net.last_chunk(2, ends, slice(a, a + 1))[0].start()

        load_next(s, slot, True)
        return carry

    lax.fori_loop(0, STEPS, step, 0)

    store_sum = pltpu.make_async_copy(acc_sc, out_ref, store_sems.at[0])
    store_sum.start()
    slot = STEPS % 2
    left = e1_ref.shape[1]
    net.last_chunk(0, ends, slice(2, 3))[0].wait_recv()
    net.last_chunk(2, ends, slice(2, 3))[0].start()
    for a in range(2):
        end_load(slot, a).wait()

    def hidden_rows(m, carry):
        sl = pl.ds(pl.multiple_of(m * M_BLOCK, M_BLOCK), M_BLOCK)
        gate = jnp.dot(b_ref[sl, :], w1_sc[slot, :, :left], preferred_element_type=jnp.float32)
        up = jnp.dot(b_ref[sl, :], w3_sc[slot, :, :left], preferred_element_type=jnp.float32)
        hid_sc[sl, :] = (jax.nn.silu(gate) * up).astype(jnp.bfloat16)
        return carry

    lax.fori_loop(0, x_ref.shape[0] // M_BLOCK, hidden_rows, 0)
    store_hidden = pltpu.make_async_copy(hid_sc, hid_ref, store_sems.at[1])
    store_hidden.start()
    net.last_chunk(2, ends, slice(2, 3))[0].wait_recv()
    store_sum.wait()
    store_hidden.wait()
    net.sent(0, N_EARLY, slice(PART, 3))
    for j in range(N_EARLY + 1, N_CHUNKS - 1):
        net.sent(0, j)
    for j in range(N_EARLY - 1, N_CHUNKS - 1):
        net.sent(1, j)
        net.sent(2, j)
    for j in range(N_EARLY - 2, N_CHUNKS - 1):
        net.sent(3, j)
    for stage in (0, 2):
        for copy in net.last_chunk(stage, ends):
            copy.wait_send()


def mlp(x, gain, o, wo, ro, w1, w3, w2, early):
    rows, dim = x.shape
    vm = pl.BlockSpec(memory_space=pltpu.VMEM)
    hbm = pl.BlockSpec(memory_space=pl.ANY)
    bf16 = jnp.bfloat16
    width = 4 * TILE
    left = w1.shape[1] % width
    n = N_CHUNKS
    return pl.pallas_call(
        mlp_kernel,
        in_specs=[hbm, vm] + [hbm] * 9,
        out_specs=[hbm] * 8,
        out_shape=[jax.ShapeDtypeStruct((rows, dim), jnp.float32), jax.ShapeDtypeStruct((rows, left), bf16)] + [jax.ShapeDtypeStruct(a.shape, bf16) for a in early] + [jax.ShapeDtypeStruct(s, bf16) for s in ((dim, left), (dim, left), (left, dim))],
        input_output_aliases={8: 2, 9: 3, 10: 4},
        scratch_shapes=[
            pltpu.VMEM((2, dim, width), bf16),
            pltpu.VMEM((2, dim, width), bf16),
            pltpu.VMEM((2, width, dim), bf16),
            pltpu.VMEM(x.shape, bf16),
            pltpu.VMEM(o.shape, bf16),
            pltpu.VMEM(wo.shape, bf16),
            pltpu.VMEM(ro.shape, bf16),
            pltpu.SemaphoreType.DMA((4,)),
            pltpu.VMEM((rows, dim), bf16),
            pltpu.VMEM((rows, dim), jnp.float32),
            pltpu.VMEM((rows, left), bf16),
            pltpu.SemaphoreType.DMA((2, 3)),
            pltpu.SemaphoreType.DMA((2,)),
            pltpu.SemaphoreType.DMA((n, 4, 3)),
            pltpu.SemaphoreType.DMA((n, 4, 3)),
        ],
        compiler_params=pltpu.CompilerParams(collective_id=1, has_side_effects=True, vmem_limit_bytes=VMEM_LIMIT),
        cost_estimate=pl.CostEstimate(flops=12 * rows * dim * w1.shape[1], bytes_accessed=12 * dim * w1.shape[1], transcendentals=2 * rows * w1.shape[1]),
        name="mlp",
    )(x, gain, o, wo, ro, w1, w3, w2, *early)


def last_kernel(sum_ref, hid_ref, w2_ref, kc_ref, vc_ref, out_ref, k_ref, v_ref):
    out_ref[...] = (sum_ref[...] + jnp.dot(hid_ref[...], w2_ref[...], preferred_element_type=jnp.float32)).astype(out_ref.dtype)
    k_ref[...] = kc_ref[...]
    v_ref[...] = vc_ref[...]


def last_product(total, hidden, w2, k_cache, v_cache):
    rows, dim = total.shape
    steps = rows // 512

    def by_rows(a):
        return pl.BlockSpec((a.shape[0] // steps, a.shape[1]), lambda i: (i, 0))

    out = jax.ShapeDtypeStruct((rows, dim), jnp.bfloat16)
    return pl.pallas_call(
        last_kernel,
        grid=(steps,),
        in_specs=[by_rows(total), by_rows(hidden), pl.BlockSpec(w2.shape, lambda i: (0, 0)), by_rows(k_cache), by_rows(v_cache)],
        out_specs=[by_rows(out), by_rows(k_cache), by_rows(v_cache)],
        out_shape=[out, jax.ShapeDtypeStruct(k_cache.shape, k_cache.dtype), jax.ShapeDtypeStruct(v_cache.shape, v_cache.dtype)],
        cost_estimate=pl.CostEstimate(flops=2 * rows * dim * w2.shape[0], bytes_accessed=6 * rows * dim, transcendentals=0),
        name="last_product",
    )(total, hidden, w2, k_cache, v_cache)

def solution(mesh):
    def layer_shard(x_loc, norm_attn, norm_mlp, w_query, w_key, w_value, w_out, w_gate, w_up, w_down):
        wq, wk, wv = (jnp.transpose(w, (1, 0, 2)) for w in (w_query, w_key, w_value))
        wo = w_out.reshape(-1, w_out.shape[2])
        o, k_cache, v_cache, wo_other, *early = attention(x_loc, norm_attn, rope_frequencies(w_query.shape[2]), wq, wk, wv, wo, w_gate, w_up, w_down)
        total, hidden, *_, last_w2 = mlp(x_loc, norm_mlp, o, wo, wo_other, w_gate, w_up, w_down, early)
        return tuple(last_product(total, hidden, last_w2, k_cache, v_cache))

    row_spec = P(("dp", "cp", "tp"), None)
    cache_spec = P(("dp", "cp"), "tp")
    head_spec = P(None, "tp", None)
    return jax.shard_map(
        layer_shard,
        mesh=mesh,
        in_specs=(row_spec, P(None), P(None), head_spec, head_spec, head_spec, P("tp", None, None), P(None, "tp"), P(None, "tp"), P("tp", None)),
        out_specs=(row_spec, cache_spec, cache_spec),
        check_vma=False,
    )
```
